8 devices in a mesh: stage: 4 (over z, y, x), data: 2 (over core).
Axes of the slice: x: 2, y: 2, z: 1, core: 2. Of those that a mesh axis runs over, the one named last changes fastest.
Arguments:
- x_in: bfloat16 [8, 4096, 768], P(None, 'data')
- targets: bfloat16 [8, 4096, 768], P(None, 'data')
- w1_bf: bfloat16 [4, 2, 1, 768, 3072], P('stage')
- w2_bf: bfloat16 [4, 2, 1, 3072, 768], P('stage')
- w_master: float32 [4, 2, 1, 4718592], P('stage', None, None, 'data')
- m_state: float32 [4, 2, 1, 4718592], P('stage', None, None, 'data')
- v_state: float32 [4, 2, 1, 4718592], P('stage', None, None, 'data')
Outputs:
- output 1: bfloat16 [4, 2, 1, 768, 3072], P('stage')
- output 2: bfloat16 [4, 2, 1, 3072, 768], P('stage')
- output 3: float32 [4, 2, 1, 4718592], P('stage', None, None, 'data')
- output 4: float32 [4, 2, 1, 4718592], P('stage', None, None, 'data')
- output 5: float32 [4, 2, 1, 4718592], P('stage', None, None, 'data')
- output 6: float32 [], replicated
All inputs are finite; a program needn't handle non-finite values.
Results may differ from the reference program's by a relative error of at most 0.001.
Values are sent between devices in bfloat16 or wider.
A program may use at most 1 GiB of HBM per device.

```python
import math
import jax
import jax.numpy as jnp
from jax import lax

STAGES = 4
DATA_WAYS = 2
MB_GROUPS = 2
TOK_DEV = 2048
VSTAGE_BLOCKS = 1
D_MODEL = 768
ADAM_STEP = 1000

N_MICRO = MB_GROUPS * STAGES
N_ROWS = DATA_WAYS * TOK_DEV
D_FF = 4 * D_MODEL
N_BLOCKS = 2 * STAGES * VSTAGE_BLOCKS
N_TOKENS = N_MICRO * N_ROWS
FLAT_LEN = 8 * D_MODEL * D_MODEL
N_PARAMS = N_BLOCKS * FLAT_LEN
BETA_ONE = 0.9
BETA_TWO = 0.999
ADAM_EPS = 1e-8
WEIGHT_DECAY = 0.1
TAU_CLIP = 0.3 * D_MODEL * math.sqrt(N_BLOCKS * (3.0 / N_TOKENS + 0.008))
LEARN_RATE = 0.1 / math.sqrt(4.0 * D_MODEL * N_BLOCKS)


def gelu_tanh(pre_act):
    return jax.nn.gelu(pre_act, approximate=True)


def moment_scale():
    scale_two = TAU_CLIP * math.sqrt(2.0 / (N_PARAMS * (1.0 + 1.0 / N_BLOCKS)))
    scale_one = scale_two / math.sqrt(N_BLOCKS)
    return jnp.concatenate([jnp.full((D_MODEL * D_FF,), scale_one, jnp.float32), jnp.full((D_FF * D_MODEL,), scale_two, jnp.float32)])


def setup_inputs(seed: int = 0) -> dict:
    key_list = jax.random.split(jax.random.key(seed), 6)
    act_shape = (N_MICRO, N_ROWS, D_MODEL)
    lead_dims = (STAGES, 2, VSTAGE_BLOCKS)
    x_in = jax.random.normal(key_list[0], act_shape, jnp.float32)
    targets = jax.random.normal(key_list[1], act_shape, jnp.float32)
    w_one = jax.random.normal(key_list[2], lead_dims + (D_MODEL, D_FF), jnp.float32) * D_MODEL ** -0.5
    w_two = jax.random.normal(key_list[3], lead_dims + (D_FF, D_MODEL), jnp.float32) * (D_FF * N_BLOCKS) ** -0.5
    w_master = jnp.concatenate([w_one.reshape(lead_dims + (-1,)), w_two.reshape(lead_dims + (-1,))], axis=-1)
    elem_scale = moment_scale()
    m_state = 0.5 * elem_scale * jax.random.normal(key_list[4], w_master.shape, jnp.float32)
    v_state = elem_scale * elem_scale * (0.25 + 0.5 * jax.random.uniform(key_list[5], w_master.shape, jnp.float32))
    return dict(x_in=x_in.astype(jnp.bfloat16), targets=targets.astype(jnp.bfloat16), w1_bf=w_one.astype(jnp.bfloat16), w2_bf=w_two.astype(jnp.bfloat16), w_master=w_master, m_state=m_state, v_state=v_state)


def block_forward(h_in, w_one, w_two):
    pre_act = jnp.dot(h_in, w_one, preferred_element_type=jnp.float32)
    act_bf = gelu_tanh(pre_act).astype(jnp.bfloat16)
    out_val = h_in.astype(jnp.float32) + jnp.dot(act_bf, w_two, preferred_element_type=jnp.float32)
    return out_val.astype(jnp.bfloat16)


def block_backward(h_in, grad_out, w_one, w_two):
    pre_act = jnp.dot(h_in, w_one, preferred_element_type=jnp.float32)
    act_val, gelu_pull = jax.vjp(gelu_tanh, pre_act)
    act_bf = act_val.astype(jnp.bfloat16)
    grad_act = jnp.dot(grad_out, w_two.T, preferred_element_type=jnp.float32)
    grad_pre = gelu_pull(grad_act)[0].astype(jnp.bfloat16)
    back_val = jnp.dot(grad_pre, w_one.T, preferred_element_type=jnp.float32)
    grad_in = (grad_out.astype(jnp.float32) + back_val).astype(jnp.bfloat16)
    grad_one = jnp.dot(h_in.T, grad_pre, preferred_element_type=jnp.float32)
    grad_two = jnp.dot(act_bf.T, grad_out, preferred_element_type=jnp.float32)
    return grad_in, grad_one, grad_two


def reference(x_in, targets, w1_bf, w2_bf, w_master, m_state, v_state):
    w_ones = jnp.swapaxes(w1_bf, 0, 1).reshape(N_BLOCKS, D_MODEL, D_FF)
    w_twos = jnp.swapaxes(w2_bf, 0, 1).reshape(N_BLOCKS, D_FF, D_MODEL)

    def fwd_step(h_in, weights):
        return block_forward(h_in, weights[0], weights[1]), h_in

    def bwd_step(grad_out, saved_item):
        grad_in, grad_one, grad_two = block_backward(saved_item[0], grad_out, saved_item[1], saved_item[2])
        return grad_in, (grad_one, grad_two)

    def micro_step(state_carry, mb_pair):
        acc_one, acc_two, loss_acc = state_carry
        h_out, block_inputs = lax.scan(fwd_step, mb_pair[0], (w_ones, w_twos))
        residual = h_out.astype(jnp.float32) - mb_pair[1].astype(jnp.float32)
        loss_acc = loss_acc + 0.5 * jnp.sum(residual * residual)
        grad_seed = (residual / N_TOKENS).astype(jnp.bfloat16)
        grad_pair = lax.scan(bwd_step, grad_seed, (block_inputs, w_ones, w_twos), reverse=True)[1]
        return (acc_one + grad_pair[0], acc_two + grad_pair[1], loss_acc), None

    start_carry = (jnp.zeros((N_BLOCKS, D_MODEL, D_FF), jnp.float32), jnp.zeros((N_BLOCKS, D_FF, D_MODEL), jnp.float32), jnp.zeros((), jnp.float32))
    acc_one, acc_two, loss_acc = lax.scan(micro_step, start_carry, (x_in, targets))[0]
    flat_dims = (2, STAGES, VSTAGE_BLOCKS, -1)
    grad_flat = jnp.swapaxes(jnp.concatenate([acc_one.reshape(flat_dims), acc_two.reshape(flat_dims)], axis=-1), 0, 1)
    grad_norm = jnp.sqrt(jnp.sum(grad_flat * grad_flat))
    clip_factor = jnp.minimum(1.0, TAU_CLIP / grad_norm)
    grad_clip = clip_factor * grad_flat
    m_new = BETA_ONE * m_state + (1.0 - BETA_ONE) * grad_clip
    v_new = BETA_TWO * v_state + (1.0 - BETA_TWO) * grad_clip * grad_clip
    m_hat = m_new / (1.0 - BETA_ONE ** ADAM_STEP)
    v_hat = v_new / (1.0 - BETA_TWO ** ADAM_STEP)
    w_new = w_master - LEARN_RATE * (m_hat / (jnp.sqrt(v_hat) + ADAM_EPS) + WEIGHT_DECAY * w_master)
    w_bf = w_new.astype(jnp.bfloat16)
    split_at = D_MODEL * D_FF
    w1_new = w_bf[..., :split_at].reshape(STAGES, 2, VSTAGE_BLOCKS, D_MODEL, D_FF)
    w2_new = w_bf[..., split_at:].reshape(STAGES, 2, VSTAGE_BLOCKS, D_FF, D_MODEL)
    return w1_new, w2_new, w_new, m_new, v_new, loss_acc / N_TOKENS
```

```python
import functools
import math
import jax
import jax.numpy as jnp
from jax import lax
from jax.experimental import pallas as pl
from jax.experimental.pallas import tpu as pltpu
from jax.sharding import PartitionSpec as P

BETA_ONE = 0.9
BETA_TWO = 0.999
ADAM_EPS = 1e-8
WEIGHT_DECAY = 0.1
ADAM_STEP = 1000
GELU_A = math.sqrt(2.0 / math.pi)
GELU_B = GELU_A * 0.044715
MESH = pl.DeviceIdType.MESH
ANY = pl.BlockSpec(memory_space=pl.ANY)
F32 = jnp.float32
BF16 = jnp.bfloat16

TILE = 512
PATH_PIECES = 3


def _dot_t(lhs, rhs):
    return lax.dot_general(lhs, rhs, (((1,), (1,)), ((), ())), preferred_element_type=F32)


def _dot(lhs, rhs):
    return jnp.dot(lhs, rhs, preferred_element_type=F32)


SEND_SLOT = -20
HOP_SLOT = {1: (-16, -13, -10), 2: (-12, -9, -6), 3: (-8, -5, -2)}
LOAD_SLOT = -1


def forward_kernel(n_blocks, tiles, x_hbm, w1_loc, w2_loc, wg1, wg2, saved, u_out, act, w1_buf, w2_buf, u_buf, acc,
                   x_sem, act_sem, u_sem, w_sem, ici_send, ici_recv, d2d_send, d2d_recv):
    me = lax.axis_index("stage")
    core = lax.axis_index("data")
    d_model, d_ff = w1_loc.shape[1], w1_loc.shape[2]
    n_rows = act.shape[0]
    n_piece = 4 * PATH_PIECES
    rows1, rows2 = d_model // n_piece, d_ff // n_piece

    def peer(flip):
        bit0, bit1 = lax.rem(me, 2), me // 2
        return (1 - bit0 + 2 * bit1) if flip == 1 else (bit0 + 2 * (1 - bit1))

    def rel_of(blk):
        own = lax.rem(blk, 4)
        a0, a1, b0, b1 = lax.rem(me, 2), me // 2, lax.rem(own, 2), own // 2
        return (a0 + b0 - 2 * a0 * b0) + 2 * (a1 + b1 - 2 * a1 * b1)

    def piece(j, path, of_core):
        return j * 4 + path * 2 + of_core

    def views(blk, idx):
        return (wg1.at[blk, pl.ds(pl.multiple_of(idx * rows1, 64), rows1), :],
                wg2.at[blk, pl.ds(pl.multiple_of(idx * rows2, 256), rows2), :])

    def local_views(blk, idx):
        half = blk // 4
        return (w1_loc.at[half, pl.ds(pl.multiple_of(idx * rows1, 64), rows1), :],
                w2_loc.at[half, pl.ds(pl.multiple_of(idx * rows2, 256), rows2), :])

    def ici_copies(blk, path, j, sources, flip):
        idx = piece(j, path, core)
        slot = path * PATH_PIECES + j
        return [pltpu.make_async_remote_copy(
            src_ref=src, dst_ref=dst, send_sem=ici_send.at[blk, slot, m], recv_sem=ici_recv.at[blk, slot, m],
            device_id=(peer(flip), core), device_id_type=MESH)
            for m, (src, dst) in enumerate(zip(sources, views(blk, idx)))]

    def d2d_copies(blk, path, j, of_core):
        idx = piece(j, path, of_core)
        slot = path * PATH_PIECES + j
        return [pltpu.make_async_remote_copy(
            src_ref=ref, dst_ref=ref, send_sem=d2d_send.at[blk, slot, m], recv_sem=d2d_recv.at[blk, slot, m],
            device_id=(me, 1 - core), device_id_type=MESH) for m, ref in enumerate(views(blk, idx))]

    def first_flip(path):
        return 1 if path == 0 else 2

    def own_send(blk):
        @pl.when(rel_of(blk) == 0)
        def _():
            for j in range(PATH_PIECES):
                for path in range(2):
                    for cp in ici_copies(blk, path, j, local_views(blk, piece(j, path, core)), first_flip(path)):
                        cp.start()

    def hop_event(blk, hop, j):
        rel = rel_of(blk)
        for path in range(2):
            at_rel = {1: (1, 2), 2: (3, 3), 3: (2, 1)}[hop][path]

            @pl.when(rel == at_rel)
            def _(path=path):
                flip = first_flip(path)
                if hop == 1:
                    flip = 3 - flip
                copies = ici_copies(blk, path, j, views(blk, piece(j, path, core)), flip)
                for cp in copies:
                    cp.wait_recv()
                if hop < 3:
                    for cp in copies:
                        cp.start()
                for cp in d2d_copies(blk, path, j, core):
                    cp.start()

    def weight_loads(blk, par, is_own):
        half = blk // 4
        src1, src2 = (w1_loc.at[half], w2_loc.at[half]) if is_own else (wg1.at[blk], wg2.at[blk])
        return [pltpu.make_async_copy(src1, w1_buf.at[par], w_sem.at[par, 0]),
                pltpu.make_async_copy(src2, w2_buf.at[par], w_sem.at[par, 1])]

    def load_event(blk):
        rel = rel_of(blk)
        par = lax.rem(blk, 2)

        @pl.when(rel == 0)
        def _():
            for cp in weight_loads(blk, par, True):
                cp.start()

        @pl.when(rel != 0)
        def _():
            for path in range(2):
                for j in range(PATH_PIECES):
                    for cp in d2d_copies(blk, path, j, 1 - core):
                        cp.wait_recv()
            for cp in weight_loads(blk, par, False):
                cp.start()

    def x_copy():
        return pltpu.make_async_copy(x_hbm.at[pl.ds(pl.multiple_of(me * n_rows, n_rows), n_rows), :], act, x_sem)

    def act_copy(slot, tile):
        rows = pl.ds(pl.multiple_of(tile * TILE, TILE), TILE)
        return pltpu.make_async_copy(act.at[rows, :], saved.at[slot, rows, :], act_sem.at[tile])

    def u_copy(blk, tile, par):
        rows = pl.ds(pl.multiple_of(tile * TILE, TILE), TILE)
        return pltpu.make_async_copy(u_buf.at[par], u_out.at[blk, rows, :], u_sem.at[par])

    barrier = pltpu.get_barrier_semaphore()
    for target in ((peer(1), core), (peer(2), core), (me, 1 - core)):
        pl.semaphore_signal(barrier, inc=1, device_id=target, device_id_type=MESH)
    x_copy().start()
    pl.semaphore_wait(barrier, 3)

    events = [(SEND_SLOT, own_send)]
    for hop in (3, 2, 1):
        for j in range(PATH_PIECES):
            events.append((HOP_SLOT[hop][j], functools.partial(lambda blk, hop, j: hop_event(blk, hop, j), hop=hop, j=j)))
    events.append((LOAD_SLOT, load_event))

    def comm_slot(blk, tile):
        for offset, fn in events:
            residue = offset % tiles
            ahead = (residue - offset) // tiles
            target = blk + ahead

            @pl.when((tile == residue) & (target >= 0) & (target < n_blocks))
            def _(fn=fn, target=target):
                fn(target)

    def compute(blk, tile):
        par = lax.rem(blk, 2)
        u_par = lax.rem(tile, 2)
        rows = pl.ds(pl.multiple_of(tile * TILE, TILE), TILE)

        @pl.when(tile == 0)
        def _():
            for cp in weight_loads(blk, par, True):
                cp.wait()

        @pl.when((blk == 0) & (tile == 0))
        def _():
            x_copy().wait()
            for t in range(tiles):
                act_copy(0, t).start()

        @pl.when((blk > 0) | (tile > 1))
        def _():
            u_copy(blk, tile, u_par).wait()

        act_copy(blk, tile).wait()
        x = act[rows, :]
        chunk = 256
        n_chunk = d_ff // chunk
        for f in range(n_chunk):
            cols = slice(f * chunk, (f + 1) * chunk)
            u = _dot(x, w1_buf[par, :, cols])
            u_buf[u_par, :, cols] = u
            inner = u * (GELU_A + GELU_B * (u * u))
            a = (u * (0.5 + 0.5 * jnp.tanh(inner))).astype(BF16)
            part = _dot(a, w2_buf[par, cols, :])
            if f == 0:
                acc[...] = part
            elif f < n_chunk - 1:
                acc[...] += part
            else:
                act[rows, :] = (x.astype(F32) + (acc[...] + part)).astype(BF16)
        u_copy(blk, tile, u_par).start()
        act_copy(blk + 1, tile).start()

    lead = -(SEND_SLOT // tiles)

    @pl.loop(0, (n_blocks + lead) * tiles)
    def _(step):
        blk = step // tiles - lead
        tile = lax.rem(step, tiles)
        comm_slot(blk, tile)

        @pl.when(blk >= 0)
        def _():
            compute(blk, tile)

    for par in range(2):
        u_copy(0, 0, par).wait()
    for t in range(tiles):
        act_copy(0, t).wait()

    @pl.loop(0, n_blocks)
    def _(blk):
        rel = rel_of(blk)
        for path in range(2):
            last = (2, 1)[path]

            @pl.when(rel != last)
            def _(path=path):
                for j in range(PATH_PIECES):
                    for cp in ici_copies(blk, path, j, views(blk, piece(j, path, core)), 1):
                        cp.wait_send()

        @pl.when(rel != 0)
        def _():
            for path in range(2):
                for j in range(PATH_PIECES):
                    for cp in d2d_copies(blk, path, j, core):
                        cp.wait_send()


def run_forward(x_flat, w1_loc, w2_loc, n_rows):
    n_half, d_model, d_ff = w1_loc.shape
    n_blocks = 4 * n_half
    tiles = n_rows // TILE
    slots = 2 * PATH_PIECES
    out_shape = [
        jax.ShapeDtypeStruct((n_blocks, d_model, d_ff), BF16),
        jax.ShapeDtypeStruct((n_blocks, d_ff, d_model), BF16),
        jax.ShapeDtypeStruct((n_blocks + 1, n_rows, d_model), BF16),
        jax.ShapeDtypeStruct((n_blocks, n_rows, d_ff), F32),
    ]
    return pl.pallas_call(
        functools.partial(forward_kernel, n_blocks, tiles),
        name="forward",
        out_shape=out_shape,
        in_specs=[ANY] * 3,
        out_specs=[ANY] * 4,
        scratch_shapes=[
            pltpu.VMEM((n_rows, d_model), BF16),
            pltpu.VMEM((2, d_model, d_ff), BF16),
            pltpu.VMEM((2, d_ff, d_model), BF16),
            pltpu.VMEM((2, TILE, d_ff), F32),
            pltpu.VMEM((TILE, d_model), F32),
            pltpu.SemaphoreType.DMA(()),
            pltpu.SemaphoreType.DMA((tiles,)),
            pltpu.SemaphoreType.DMA((2,)),
            pltpu.SemaphoreType.DMA((2, 2)),
            pltpu.SemaphoreType.DMA((n_blocks, slots, 2)),
            pltpu.SemaphoreType.DMA((n_blocks, slots, 2)),
            pltpu.SemaphoreType.DMA((n_blocks, slots, 2)),
            pltpu.SemaphoreType.DMA((n_blocks, slots, 2)),
        ],
        compiler_params=pltpu.CompilerParams(collective_id=0, has_side_effects=True, vmem_limit_bytes=60 * 2**20),
        cost_estimate=pl.CostEstimate(flops=4 * n_blocks * n_rows * d_model * d_ff, bytes_accessed=600 * 2**20, transcendentals=0),
    )(x_flat, w1_loc, w2_loc)


RING = 6
CHUNK = 512


def backward_kernel(top_block, n_blocks, tiles, g_hbm, saved, u_hbm, w1_loc, w2_loc, wg1, wg2, g_out, keep, send,
                    act, w1_buf, w2_buf, dw1, dw2, u_buf, x_buf, x_t, g_t, acc, q_buf,
                    g_sem, w_sem, u_sem, x_sem, dw_sem):
    me = lax.axis_index("stage")
    core = lax.axis_index("data")
    d_ff = dw1.shape[1]
    n_chunk = d_ff // CHUNK

    def rel_of(blk):
        own = lax.rem(blk, 4)
        a0, a1, b0, b1 = lax.rem(me, 2), me // 2, lax.rem(own, 2), own // 2
        return (a0 + b0 - 2 * a0 * b0) + 2 * (a1 + b1 - 2 * a1 * b1)

    def rows_of(tile):
        return pl.ds(pl.multiple_of(tile * TILE, TILE), TILE)

    def cols_of(f):
        return pl.ds(pl.multiple_of(f * CHUNK, CHUNK), CHUNK)

    def weight_loads(blk, par, is_own):
        half = blk // 4
        src1, src2 = (w1_loc.at[half], w2_loc.at[half]) if is_own else (wg1.at[blk], wg2.at[blk])
        return [pltpu.make_async_copy(src1, w1_buf.at[par], w_sem.at[par, 0]),
                pltpu.make_async_copy(src2, w2_buf.at[par], w_sem.at[par, 1])]

    def start_weights(blk, par):
        rel = rel_of(blk)

        @pl.when(rel == 0)
        def _():
            for cp in weight_loads(blk, par, True):
                cp.start()

        @pl.when(rel != 0)
        def _():
            for cp in weight_loads(blk, par, False):
                cp.start()

    def u_copy(step, slot):
        blk = top_block - step // (tiles * n_chunk)
        tile = lax.rem(step // n_chunk, tiles)
        f = lax.rem(step, n_chunk)
        return pltpu.make_async_copy(u_hbm.at[blk, rows_of(tile), cols_of(f)], u_buf.at[slot], u_sem.at[slot])

    def x_copy(blk, tile, par):
        return pltpu.make_async_copy(saved.at[blk, rows_of(tile), :], x_buf.at[par], x_sem.at[par])

    def g_in_copy():
        return pltpu.make_async_copy(g_hbm, act, g_sem)

    def dw_copies(blk, f, swap):
        rel = rel_of(blk)
        one, two = (send, keep) if swap else (keep, send)
        return [pltpu.make_async_copy(dw1.at[:, cols_of(f)], one.at[rel, :, cols_of(f)], dw_sem.at[f, 0]),
                pltpu.make_async_copy(dw2.at[:, cols_of(f)], two.at[rel, :, cols_of(f)], dw_sem.at[f, 1])]

    total = n_blocks * tiles * n_chunk

    g_in_copy().start()
    start_weights(top_block, 0)
    x_copy(top_block, 0, 0).start()
    for step in range(RING - 2):
        u_copy(step, step).start()
    g_in_copy().wait()
    for cp in weight_loads(top_block, 0, True):
        cp.wait()
    q_buf[0] = _dot_t(act[pl.ds(0, TILE), :], w2_buf[0, pl.ds(0, CHUNK), :])

    @pl.loop(0, n_blocks * tiles)
    def _(bt):
        i = bt // tiles
        tile = lax.rem(bt, tiles)
        blk = top_block - i
        par = lax.rem(i, 2)
        rows = rows_of(tile)
        x_par = lax.rem(tile, 2)

        @pl.when((tile == 1) & (i + 1 < n_blocks))
        def _():
            start_weights(blk - 1, 1 - par)

        x_copy(blk, tile, x_par).wait()

        @pl.when(bt + 1 < n_blocks * tiles)
        def _():
            x_copy(top_block - (bt + 1) // tiles, lax.rem(bt + 1, tiles), 1 - x_par).start()

        x_t[...] = x_buf[x_par].T
        g_t[...] = act[rows, :].T
        acc[...] = act[rows, :].astype(F32)

        def chunk_prep(f, step):
            @pl.when(step + RING - 2 < total)
            def _():
                u_copy(step + RING - 2, lax.rem(step + RING - 2, RING)).start()
            u_copy(step, lax.rem(step, RING)).wait()

            @pl.when((tile == 0) & (i > 0))
            def _():
                for cp in dw_copies(blk, f, False):
                    cp.wait()

            @pl.when(tile == 0)
            def _():
                dw1[:, cols_of(f)] = jnp.zeros((dw1.shape[0], CHUNK), F32)
                dw2[:, cols_of(f)] = jnp.zeros((dw2.shape[0], CHUNK), F32)

        def chunk_main(f, step, q_par, next_g, next_w2):
            cols = cols_of(f)
            q_buf[1 - q_par] = _dot_t(next_g, next_w2)
            u = u_buf[lax.rem(step, RING)]
            u2 = u * u
            th = jnp.tanh(u * (GELU_A + GELU_B * u2))
            cdf = 0.5 + 0.5 * th
            a = (u * cdf).astype(BF16)
            slope = cdf + (u * (0.5 * GELU_A + 1.5 * GELU_B * u2)) * (1.0 - th * th)
            r = (q_buf[q_par] * slope).astype(BF16)
            dw1[:, cols] += _dot(x_t[...], r)
            dw2[:, cols] += _dot(g_t[...], a)
            acc[...] += _dot_t(r, w1_buf[par, :, cols])

        def chunk_done(f):
            @pl.when((tile == tiles - 1) & (core == 0))
            def _():
                for cp in dw_copies(blk, f, False):
                    cp.start()

            @pl.when((tile == tiles - 1) & (core == 1))
            def _():
                for cp in dw_copies(blk, f, True):
                    cp.start()

        @pl.loop(0, n_chunk // 2)
        def _(pair):
            f0 = pair * 2
            step = bt * n_chunk + f0
            last = f0 + 2 == n_chunk
            end_block = last & (tile == tiles - 1)
            chunk_prep(f0, step)
            chunk_prep(f0 + 1, step + 1)

            @pl.when(end_block & (i + 1 < n_blocks))
            def _():
                for cp in weight_loads(blk, 1 - par, True):
                    cp.wait()

            next_rows = rows_of(jnp.where(last, lax.rem(tile + 1, tiles), tile))
            next_f = jnp.where(last, 0, f0 + 2)
            next_par = jnp.where(end_block, 1 - par, par)
            g_now = act[rows, :]
            chunk_main(f0, step, 0, g_now, w2_buf[par, cols_of(f0 + 1), :])
            chunk_main(f0 + 1, step + 1, 1, act[next_rows, :], w2_buf[next_par, cols_of(next_f), :])
            chunk_done(f0)
            chunk_done(f0 + 1)

        act[rows, :] = acc[...].astype(BF16)

    for f in range(n_chunk):
        for cp in dw_copies(top_block, f, False):
            cp.wait()
    out = pltpu.make_async_copy(act, g_out, g_sem)
    out.start()
    out.wait()


def run_backward(top_block, n_blocks, grad, saved, u_all, w1_loc, w2_loc, wg1, wg2):
    n_rows, d_model = grad.shape
    d_ff = w1_loc.shape[2]
    tiles = n_rows // TILE
    return pl.pallas_call(
        functools.partial(backward_kernel, top_block, n_blocks, tiles),
        name=f"backward_{top_block}",
        out_shape=[
            jax.ShapeDtypeStruct((n_rows, d_model), BF16),
            jax.ShapeDtypeStruct((n_blocks, d_model, d_ff), F32),
            jax.ShapeDtypeStruct((n_blocks, d_model, d_ff), F32),
        ],
        in_specs=[ANY] * 7,
        out_specs=[ANY] * 3,
        scratch_shapes=[
            pltpu.VMEM((n_rows, d_model), BF16),
            pltpu.VMEM((2, d_model, d_ff), BF16),
            pltpu.VMEM((2, d_ff, d_model), BF16),
            pltpu.VMEM((d_model, d_ff), F32),
            pltpu.VMEM((d_model, d_ff), F32),
            pltpu.VMEM((RING, TILE, CHUNK), F32),
            pltpu.VMEM((2, TILE, d_model), BF16),
            pltpu.VMEM((d_model, TILE), BF16),
            pltpu.VMEM((d_model, TILE), BF16),
            pltpu.VMEM((TILE, d_model), F32),
            pltpu.VMEM((2, TILE, CHUNK), F32),
            pltpu.SemaphoreType.DMA(()),
            pltpu.SemaphoreType.DMA((2, 2)),
            pltpu.SemaphoreType.DMA((RING,)),
            pltpu.SemaphoreType.DMA((2,)),
            pltpu.SemaphoreType.DMA((d_ff // CHUNK, 2)),
        ],
        compiler_params=pltpu.CompilerParams(vmem_limit_bytes=67043328),
        cost_estimate=pl.CostEstimate(flops=8 * n_blocks * n_rows * d_model * d_ff, bytes_accessed=400 * 2**20, transcendentals=0),
    )(grad, saved, u_all, w1_loc, w2_loc, wg1, wg2)


def adam_update(w_old, m_old, v_old, grad_val, clip_factor, learn_rate):
    grad_clip = clip_factor * grad_val
    m_new = BETA_ONE * m_old + (1.0 - BETA_ONE) * grad_clip
    v_new = BETA_TWO * v_old + (1.0 - BETA_TWO) * grad_clip * grad_clip
    m_hat = m_new / (1.0 - BETA_ONE ** ADAM_STEP)
    v_hat = v_new / (1.0 - BETA_TWO ** ADAM_STEP)
    w_new = w_old - learn_rate * (m_hat / (jnp.sqrt(v_hat) + ADAM_EPS) + WEIGHT_DECAY * w_old)
    return w_new, m_new, v_new


def solution(mesh):
    n_stage = mesh.shape["stage"]
    n_data = mesh.shape["data"]
    axes = ("stage", "data")

    def device(stage, core):
        return stage * n_data + core

    sibling = [(device(s, c), device(s, 1 - c)) for s in range(n_stage) for c in range(n_data)]

    def across(flip):
        return [(device(s, c), device(s ^ flip, c)) for s in range(n_stage) for c in range(n_data)]

    def reduce_group(keep, send):
        got = lax.ppermute(send, axes, sibling)
        own = keep[0] + got[0]
        for flip in range(1, n_stage):
            part = (keep[flip] + got[flip]).astype(BF16)
            own = own + lax.ppermute(part, axes, across(flip)).astype(F32)
        return own

    def device_step(x_loc, t_loc, w1_loc, w2_loc, wm_loc, m_loc, v_loc):
        n_micro, n_tok, d_model = x_loc.shape
        d_ff = w1_loc.shape[4]
        n_tokens = n_micro * n_tok * n_data
        n_blocks = 2 * n_stage
        n_rows = n_micro * n_tok // n_stage
        tau_clip = 0.3 * d_model * math.sqrt(n_blocks * (3.0 / n_tokens + 0.008))
        learn_rate = 0.1 / math.sqrt(4.0 * d_model * n_blocks)
        stage_idx = lax.axis_index("stage")
        core = lax.axis_index("data")
        x_flat = x_loc.reshape(n_micro * n_tok, d_model)
        w1 = w1_loc.reshape(2, d_model, d_ff)
        w2 = w2_loc.reshape(2, d_ff, d_model)
        wg1, wg2, saved, u_all = run_forward(x_flat, w1, w2, n_rows)
        target = lax.dynamic_slice_in_dim(t_loc.reshape(n_micro * n_tok, d_model), stage_idx * n_rows, n_rows, 0)
        residual = saved[n_blocks].astype(F32) - target.astype(F32)
        loss_acc = 0.5 * jnp.sum(residual * residual)
        seed = (residual / n_tokens).astype(BF16)
        grad, keep_hi, send_hi = run_backward(7, 4, seed, saved, u_all, w1, w2, wg1, wg2)
        own_hi = reduce_group(keep_hi, send_hi)
        grad, keep_lo, send_lo = run_backward(3, 4, grad, saved, u_all, w1, w2, wg1, wg2)
        own_lo = reduce_group(keep_lo, send_lo)
        own = jnp.stack([own_lo, own_hi])
        sq_sum = jnp.sum(own * own)
        flat = jnp.where(core == 0, own.reshape(2, -1), jnp.swapaxes(own, 1, 2).reshape(2, -1))
        grad_shard = flat[:, None]
        grad_norm = jnp.sqrt(lax.psum(sq_sum, axes))
        clip_factor = jnp.minimum(1.0, tau_clip / grad_norm)
        w_new, m_new, v_new = adam_update(wm_loc[0], m_loc[0], v_loc[0], grad_shard, clip_factor, learn_rate)
        w_half = w_new.astype(BF16)
        w_other = lax.ppermute(w_half, axes, sibling)
        w1_new = jnp.where(core == 0, w_half, w_other).reshape(1, 2, 1, d_model, d_ff)
        w2_new = jnp.where(core == 0, w_other, w_half).reshape(1, 2, 1, d_ff, d_model)
        mean_loss = lax.psum(loss_acc, axes) / n_tokens
        return w1_new, w2_new, w_new[None], m_new[None], v_new[None], mean_loss

    act_spec = P(None, "data", None)
    flat_spec = P("stage", None, None, "data")
    return jax.shard_map(device_step, mesh=mesh, in_specs=(act_spec, act_spec, P("stage"), P("stage"), flat_spec, flat_spec, flat_spec), out_specs=(P("stage"), P("stage"), flat_spec, flat_spec, flat_spec, P()), check_vma=False)
```

```python
import functools
import math
import jax
import jax.numpy as jnp
from jax import lax
from jax.experimental import pallas as pl
from jax.experimental.pallas import tpu as pltpu
from jax.sharding import PartitionSpec as P

BETA_ONE = 0.9
BETA_TWO = 0.999
ADAM_EPS = 1e-8
WEIGHT_DECAY = 0.1
ADAM_STEP = 1000
GELU_A = math.sqrt(2.0 / math.pi)
GELU_B = GELU_A * 0.044715
MESH = pl.DeviceIdType.MESH
ANY = pl.BlockSpec(memory_space=pl.ANY)
F32 = jnp.float32
BF16 = jnp.bfloat16

TILE = 512
PATH_PIECES = 4


def _dot_t(lhs, rhs):
    return lax.dot_general(lhs, rhs, (((1,), (1,)), ((), ())), preferred_element_type=F32)


def _dot(lhs, rhs):
    return jnp.dot(lhs, rhs, preferred_element_type=F32)


SEND_SLOT = (-45, -30, -28, -20)
HOP_SLOT = {1: (-27, -20, -18, -14), 2: (-18, -14, -8, -6), 3: (-12, -9, -2, -2)}
LOAD_SLOT = -1


def forward_kernel(n_blocks, tiles, x_hbm, w1_loc, w2_loc, wg1, wg2, saved, u_out, act, w1_buf, w2_buf, u_buf, acc,
                   x_sem, act_sem, u_sem, w_sem, ici_send, ici_recv, d2d_send, d2d_recv):
    me = lax.axis_index("stage")
    core = lax.axis_index("data")
    d_model, d_ff = w1_loc.shape[1], w1_loc.shape[2]
    n_rows = act.shape[0]
    n_piece = 4 * PATH_PIECES
    rows1, rows2 = d_model // n_piece, d_ff // n_piece

    def peer(flip):
        bit0, bit1 = lax.rem(me, 2), me // 2
        return (1 - bit0 + 2 * bit1) if flip == 1 else (bit0 + 2 * (1 - bit1))

    def rel_of(blk):
        own = lax.rem(blk, 4)
        a0, a1, b0, b1 = lax.rem(me, 2), me // 2, lax.rem(own, 2), own // 2
        return (a0 + b0 - 2 * a0 * b0) + 2 * (a1 + b1 - 2 * a1 * b1)

    def piece(j, path, of_core):
        return j * 4 + path * 2 + of_core

    def views(blk, idx):
        return (wg1.at[blk, pl.ds(pl.multiple_of(idx * rows1, 16), rows1), :],
                wg2.at[blk, pl.ds(pl.multiple_of(idx * rows2, 64), rows2), :])

    def local_views(blk, idx):
        half = blk // 4
        return (w1_loc.at[half, pl.ds(pl.multiple_of(idx * rows1, 16), rows1), :],
                w2_loc.at[half, pl.ds(pl.multiple_of(idx * rows2, 64), rows2), :])

    def ici_copies(blk, path, j, sources, flip):
        idx = piece(j, path, core)
        slot = path * PATH_PIECES + j
        return [pltpu.make_async_remote_copy(
            src_ref=src, dst_ref=dst, send_sem=ici_send.at[blk, slot, m], recv_sem=ici_recv.at[blk, slot, m],
            device_id=(peer(flip), core), device_id_type=MESH)
            for m, (src, dst) in enumerate(zip(sources, views(blk, idx)))]

    def d2d_copies(blk, path, j, of_core):
        idx = piece(j, path, of_core)
        slot = path * PATH_PIECES + j
        return [pltpu.make_async_remote_copy(
            src_ref=ref, dst_ref=ref, send_sem=d2d_send.at[blk, slot, m], recv_sem=d2d_recv.at[blk, slot, m],
            device_id=(me, 1 - core), device_id_type=MESH) for m, ref in enumerate(views(blk, idx))]

    def first_flip(path):
        return 1 if path == 0 else 2

    def own_send(blk, j):
        @pl.when(rel_of(blk) == 0)
        def _():
            for path in range(2):
                for cp in ici_copies(blk, path, j, local_views(blk, piece(j, path, core)), first_flip(path)):
                    cp.start()

    def hop_event(blk, hop, j):
        rel = rel_of(blk)
        for path in range(2):
            at_rel = {1: (1, 2), 2: (3, 3), 3: (2, 1)}[hop][path]

            @pl.when(rel == at_rel)
            def _(path=path):
                flip = first_flip(path)
                if hop == 1:
                    flip = 3 - flip
                copies = ici_copies(blk, path, j, views(blk, piece(j, path, core)), flip)
                for cp in copies:
                    cp.wait_recv()
                if hop < 3:
                    for cp in copies:
                        cp.start()
                for cp in d2d_copies(blk, path, j, core):
                    cp.start()

    def weight_loads(blk, par, is_own):
        half = blk // 4
        src1, src2 = (w1_loc.at[half], w2_loc.at[half]) if is_own else (wg1.at[blk], wg2.at[blk])
        return [pltpu.make_async_copy(src1, w1_buf.at[par], w_sem.at[par, 0]),
                pltpu.make_async_copy(src2, w2_buf.at[par], w_sem.at[par, 1])]

    def load_event(blk):
        rel = rel_of(blk)
        par = lax.rem(blk, 2)

        @pl.when(rel == 0)
        def _():
            for cp in weight_loads(blk, par, True):
                cp.start()

        @pl.when(rel != 0)
        def _():
            for path in range(2):
                for j in range(PATH_PIECES):
                    for cp in d2d_copies(blk, path, j, 1 - core):
                        cp.wait_recv()
            for cp in weight_loads(blk, par, False):
                cp.start()

    def x_copy():
        return pltpu.make_async_copy(x_hbm.at[pl.ds(pl.multiple_of(me * n_rows, n_rows), n_rows), :], act, x_sem)

    def act_copy(slot, tile):
        rows = pl.ds(pl.multiple_of(tile * TILE, TILE), TILE)
        return pltpu.make_async_copy(act.at[rows, :], saved.at[slot, rows, :], act_sem.at[tile])

    def u_copy(blk, tile, par):
        rows = pl.ds(pl.multiple_of(tile * TILE, TILE), TILE)
        return pltpu.make_async_copy(u_buf.at[par], u_out.at[blk, rows, :], u_sem.at[par])

    barrier = pltpu.get_barrier_semaphore()
    for target in ((peer(1), core), (peer(2), core), (me, 1 - core)):
        pl.semaphore_signal(barrier, inc=1, device_id=target, device_id_type=MESH)
    x_copy().start()
    pl.semaphore_wait(barrier, 3)

    events = []
    for hop in (3, 2, 1):
        for j in range(PATH_PIECES):
            events.append((HOP_SLOT[hop][j], functools.partial(lambda blk, hop, j: hop_event(blk, hop, j), hop=hop, j=j)))
    for j in range(PATH_PIECES):
        events.append((SEND_SLOT[j], functools.partial(lambda blk, j: own_send(blk, j), j=j)))
    events.append((LOAD_SLOT, load_event))

    def comm_slot(blk, tile):
        for offset, fn in events:
            residue = offset % tiles
            ahead = (residue - offset) // tiles
            target = blk + ahead

            @pl.when((tile == residue) & (target >= 0) & (target < n_blocks))
            def _(fn=fn, target=target):
                fn(target)

    def compute(blk, tile):
        par = lax.rem(blk, 2)
        u_par = lax.rem(tile, 2)
        rows = pl.ds(pl.multiple_of(tile * TILE, TILE), TILE)

        @pl.when(tile == 0)
        def _():
            for cp in weight_loads(blk, par, True):
                cp.wait()

        @pl.when((blk == 0) & (tile == 0))
        def _():
            x_copy().wait()
            for t in range(tiles):
                act_copy(0, t).start()

        @pl.when((blk > 0) | (tile > 1))
        def _():
            u_copy(blk, tile, u_par).wait()

        act_copy(blk, tile).wait()
        x = act[rows, :]
        chunk = 256
        n_chunk = d_ff // chunk
        for f in range(n_chunk):
            cols = slice(f * chunk, (f + 1) * chunk)
            u = _dot(x, w1_buf[par, :, cols])
            u_buf[u_par, :, cols] = u
            inner = u * (GELU_A + GELU_B * (u * u))
            a = (u * (0.5 + 0.5 * jnp.tanh(inner))).astype(BF16)
            part = _dot(a, w2_buf[par, cols, :])
            if f == 0:
                acc[...] = part
            elif f < n_chunk - 1:
                acc[...] += part
            else:
                act[rows, :] = (x.astype(F32) + (acc[...] + part)).astype(BF16)
        u_copy(blk, tile, u_par).start()
        act_copy(blk + 1, tile).start()

    lead = -(min(SEND_SLOT) // tiles)

    @pl.loop(0, (n_blocks + lead) * tiles)
    def _(step):
        blk = step // tiles - lead
        tile = lax.rem(step, tiles)
        comm_slot(blk, tile)

        @pl.when(blk >= 0)
        def _():
            compute(blk, tile)

    for par in range(2):
        u_copy(0, 0, par).wait()
    for t in range(tiles):
        act_copy(0, t).wait()

    @pl.loop(0, n_blocks)
    def _(blk):
        rel = rel_of(blk)
        for path in range(2):
            last = (2, 1)[path]

            @pl.when(rel != last)
            def _(path=path):
                for j in range(PATH_PIECES):
                    for cp in ici_copies(blk, path, j, views(blk, piece(j, path, core)), 1):
                        cp.wait_send()

        @pl.when(rel != 0)
        def _():
            for path in range(2):
                for j in range(PATH_PIECES):
                    for cp in d2d_copies(blk, path, j, core):
                        cp.wait_send()


def run_forward(x_flat, w1_loc, w2_loc, n_rows):
    n_half, d_model, d_ff = w1_loc.shape
    n_blocks = 4 * n_half
    tiles = n_rows // TILE
    slots = 2 * PATH_PIECES
    out_shape = [
        jax.ShapeDtypeStruct((n_blocks, d_model, d_ff), BF16),
        jax.ShapeDtypeStruct((n_blocks, d_ff, d_model), BF16),
        jax.ShapeDtypeStruct((n_blocks + 1, n_rows, d_model), BF16),
        jax.ShapeDtypeStruct((n_blocks, n_rows, d_ff), F32),
    ]
    return pl.pallas_call(
        functools.partial(forward_kernel, n_blocks, tiles),
        name="forward",
        out_shape=out_shape,
        in_specs=[ANY] * 3,
        out_specs=[ANY] * 4,
        scratch_shapes=[
            pltpu.VMEM((n_rows, d_model), BF16),
            pltpu.VMEM((2, d_model, d_ff), BF16),
            pltpu.VMEM((2, d_ff, d_model), BF16),
            pltpu.VMEM((2, TILE, d_ff), F32),
            pltpu.VMEM((TILE, d_model), F32),
            pltpu.SemaphoreType.DMA(()),
            pltpu.SemaphoreType.DMA((tiles,)),
            pltpu.SemaphoreType.DMA((2,)),
            pltpu.SemaphoreType.DMA((2, 2)),
            pltpu.SemaphoreType.DMA((n_blocks, slots, 2)),
            pltpu.SemaphoreType.DMA((n_blocks, slots, 2)),
            pltpu.SemaphoreType.DMA((n_blocks, slots, 2)),
            pltpu.SemaphoreType.DMA((n_blocks, slots, 2)),
        ],
        compiler_params=pltpu.CompilerParams(collective_id=0, has_side_effects=True, vmem_limit_bytes=60 * 2**20),
        cost_estimate=pl.CostEstimate(flops=4 * n_blocks * n_rows * d_model * d_ff, bytes_accessed=600 * 2**20, transcendentals=0),
    )(x_flat, w1_loc, w2_loc)


RING = 4
CHUNK = 512
PIECE = 256


def _relation(me, blk):
    own = lax.rem(blk, 4)
    a0, a1, b0, b1 = lax.rem(me, 2), me // 2, lax.rem(own, 2), own // 2
    return (a0 + b0 - 2 * a0 * b0) + 2 * (a1 + b1 - 2 * a1 * b1)


def _weight_loads(sources, buffers, sems, blk, par, is_own):
    w1_loc, w2_loc, wg1, wg2 = sources
    half = blk // 4
    src1, src2 = (w1_loc.at[half], w2_loc.at[half]) if is_own else (wg1.at[blk], wg2.at[blk])
    return [pltpu.make_async_copy(src1, buffers[0].at[par], sems.at[par, 0]),
            pltpu.make_async_copy(src2, buffers[1].at[par], sems.at[par, 1])]


def _start_weights(me, sources, buffers, sems, blk, par):
    rel = _relation(me, blk)

    @pl.when(rel == 0)
    def _():
        for cp in _weight_loads(sources, buffers, sems, blk, par, True):
            cp.start()

    @pl.when(rel != 0)
    def _():
        for cp in _weight_loads(sources, buffers, sems, blk, par, False):
            cp.start()


def _tile_rows(tile):
    return pl.ds(pl.multiple_of(tile * TILE, TILE), TILE)


def _sibling_barrier(me, core):
    barrier = pltpu.get_barrier_semaphore()
    pl.semaphore_signal(barrier, inc=1, device_id=(me, 1 - core), device_id_type=MESH)
    pl.semaphore_wait(barrier, 1)


def _gelu_grad(u):
    cube = GELU_B * (u * u)
    th = jnp.tanh(u * (GELU_A + cube))
    cdf = 0.5 + 0.5 * th
    a = u * cdf
    return a, cdf + (a * (3.0 - 3.0 * th)) * (cube + GELU_A / 3.0)


def backward_kernel(top_block, n_blocks, tiles, g_hbm, saved, u_hbm, w1_loc, w2_loc, wg1, wg2, g_out, keep, sib, own, part1, part2, part3,
                    act, w1_buf, w2_buf, dw, u_buf, x_buf, x_t, g_t, acc, q_buf, k_buf, s_buf, o_buf,
                    g_sem, w_sem, u_sem, x_sem, keep_sem, send_sem, recv_sem, load_sem, out_sem):
    me = lax.axis_index("stage")
    core = lax.axis_index("data")
    d_model, d_ff = dw.shape[1], dw.shape[2]
    n_chunk = d_ff // CHUNK
    n_piece = d_ff // PIECE
    sources, buffers = (w1_loc, w2_loc, wg1, wg2), (w1_buf, w2_buf)
    total = n_blocks * tiles * n_chunk

    def cols_of(f):
        return pl.ds(pl.multiple_of(f * CHUNK, CHUNK), CHUNK)

    def u_copy(step):
        blk = top_block - step // (tiles * n_chunk)
        tile = lax.rem(step // n_chunk, tiles)
        f = lax.rem(step, n_chunk)
        slot = lax.rem(step, RING)
        return pltpu.make_async_copy(u_hbm.at[blk, _tile_rows(tile), cols_of(f)], u_buf.at[slot], u_sem.at[slot])

    def x_copy(bt):
        par = lax.rem(bt, 2)
        return pltpu.make_async_copy(saved.at[top_block - bt // tiles, _tile_rows(lax.rem(bt, tiles)), :], x_buf.at[par], x_sem.at[par])

    def g_in_copy():
        return pltpu.make_async_copy(g_hbm, act, g_sem)

    def keep_copy(i, f):
        return pltpu.make_async_copy(dw.at[core, :, cols_of(f)], keep.at[i, :, cols_of(f)], keep_sem.at[f])

    def send_copy(i, f):
        return pltpu.make_async_remote_copy(
            src_ref=dw.at[1 - core, :, cols_of(f)], dst_ref=sib.at[i, :, cols_of(f)], send_sem=send_sem.at[f],
            recv_sem=recv_sem.at[i, f], device_id=(me, 1 - core), device_id_type=MESH)

    def piece_cols(c):
        return pl.ds(pl.multiple_of(c * PIECE, PIECE), PIECE)

    def piece_loads(i, c):
        par = lax.rem(c, 2)
        return [pltpu.make_async_copy(keep.at[i, :, piece_cols(c)], k_buf.at[par], load_sem.at[par, 0]),
                pltpu.make_async_copy(sib.at[i, :, piece_cols(c)], s_buf.at[par], load_sem.at[par, 1])]

    def own_out(c):
        par = lax.rem(c, 2)
        return pltpu.make_async_copy(k_buf.at[par], own.at[:, piece_cols(c)], out_sem.at[par])

    def part_out(rel, c):
        par = lax.rem(c, 2)
        return pltpu.make_async_copy(o_buf.at[par], (part1, part2, part3)[rel - 1].at[:, piece_cols(c)], out_sem.at[par])

    def wait_out(i, c):
        rel = _relation(me, top_block - i)

        @pl.when(rel == 0)
        def _():
            own_out(c).wait()

        @pl.when(rel != 0)
        def _():
            part_out(1, c).wait()

    def piece_load(i, c):
        @pl.when(c >= 2)
        def _():
            wait_out(i, c)

        @pl.when((c < 2) & (i > 0))
        def _():
            wait_out(i - 1, c)

        @pl.when(lax.rem(c, 2) == 0)
        def _():
            send_copy(i, c // 2).wait_recv()
        for cp in piece_loads(i, c):
            cp.start()

    def piece_sum(i, c):
        par = lax.rem(c, 2)
        rel = _relation(me, top_block - i)
        for cp in piece_loads(i, c):
            cp.wait()

        @pl.when(rel == 0)
        def _():
            k_buf[par] = k_buf[par] + s_buf[par]
            own_out(c).start()

        @pl.when(rel != 0)
        def _():
            o_buf[par] = (k_buf[par] + s_buf[par]).astype(BF16)
            for other in range(1, 4):
                @pl.when(rel == other)
                def _(other=other):
                    part_out(other, c).start()

    g_in_copy().start()
    _start_weights(me, sources, buffers, w_sem, top_block, 0)
    x_copy(0).start()
    x_copy(1).start()
    for step in range(RING - 2):
        u_copy(step).start()
    _sibling_barrier(me, core)
    g_in_copy().wait()
    x_copy(0).wait()
    x_t[0] = x_buf[0].T
    g_t[0] = act[pl.ds(0, TILE), :].T
    for cp in _weight_loads(sources, buffers, w_sem, top_block, 0, True):
        cp.wait()
    q_buf[0] = _dot_t(act[pl.ds(0, TILE), :], w2_buf[0, pl.ds(0, CHUNK), :])

    @pl.loop(0, n_blocks * tiles)
    def _(bt):
        i = bt // tiles
        tile = lax.rem(bt, tiles)
        blk = top_block - i
        par = lax.rem(i, 2)
        t_par = lax.rem(bt, 2)
        rows = _tile_rows(tile)
        next_rows = _tile_rows(lax.rem(tile + 1, tiles))

        @pl.when((tile == 1) & (i + 1 < n_blocks))
        def _():
            _start_weights(me, sources, buffers, w_sem, blk - 1, 1 - par)

        @pl.when(bt + 1 < n_blocks * tiles)
        def _():
            x_copy(bt + 1).wait()

        @pl.when(bt + 2 < n_blocks * tiles)
        def _():
            x_copy(bt + 2).start()

        @pl.when((i > 0) & (tile >= 2))
        def _():
            piece_sum(i - 1, 2 * tile - 4)
            piece_sum(i - 1, 2 * tile - 3)

        @pl.when((i > 0) & (tile >= 1) & (tile < tiles - 1))
        def _():
            piece_load(i - 1, 2 * tile - 2)
            piece_load(i - 1, 2 * tile - 1)

        acc[...] = act[rows, :].astype(F32)

        def chunk_prep(f, step):
            @pl.when(step + RING - 2 < total)
            def _():
                u_copy(step + RING - 2).start()
            u_copy(step).wait()

            @pl.when((tile == 0) & (i > 0))
            def _():
                keep_copy(i, f).wait()
                send_copy(i, f).wait_send()

            @pl.when(tile == 0)
            def _():
                dw[0, :, cols_of(f)] = jnp.zeros((d_model, CHUNK), F32)
                dw[1, :, cols_of(f)] = jnp.zeros((d_model, CHUNK), F32)

        def chunk_main(f, step, q_par, next_g, next_w2):
            cols = cols_of(f)
            q_buf[1 - q_par] = _dot_t(next_g, next_w2)
            a, slope = _gelu_grad(u_buf[lax.rem(step, RING)])
            r = (q_buf[q_par] * slope).astype(BF16)
            dw[0, :, cols] += _dot(x_t[t_par], r)
            dw[1, :, cols] += _dot(g_t[t_par], a.astype(BF16))
            acc[...] += _dot_t(r, w1_buf[par, :, cols])

        @pl.loop(0, n_chunk // 2)
        def _(pair):
            f0 = pair * 2
            step = bt * n_chunk + f0
            last = f0 + 2 == n_chunk
            end_block = last & (tile == tiles - 1)
            chunk_prep(f0, step)
            chunk_prep(f0 + 1, step + 1)

            @pl.when(end_block & (i + 1 < n_blocks))
            def _():
                for cp in _weight_loads(sources, buffers, w_sem, blk, 1 - par, True):
                    cp.wait()

            q_rows = _tile_rows(jnp.where(last, lax.rem(tile + 1, tiles), tile))
            next_f = jnp.where(last, 0, f0 + 2)
            next_par = jnp.where(end_block, 1 - par, par)
            third = pl.ds(pl.multiple_of(pair * 256, 256), 256)
            chunk_main(f0, step, 0, act[rows, :], w2_buf[par, cols_of(f0 + 1), :])
            x_t[1 - t_par, third, :] = x_buf[1 - t_par, :, third].T
            g_t[1 - t_par, third, :] = act[next_rows, third].T
            chunk_main(f0 + 1, step + 1, 1, act[q_rows, :], w2_buf[next_par, cols_of(next_f), :])

            @pl.when(tile == tiles - 1)
            def _():
                for f in (f0, f0 + 1):
                    keep_copy(i, f).start()
                    send_copy(i, f).start()

        act[rows, :] = acc[...].astype(BF16)

    out = pltpu.make_async_copy(act, g_out, g_sem)
    out.start()
    final = n_blocks - 1
    for f in range(n_chunk):
        keep_copy(final, f).wait()
    for c in range(n_piece + 1):
        if c < n_piece:
            piece_load(final, jnp.int32(c))
        if c > 0:
            piece_sum(final, jnp.int32(c - 1))
    for c in (n_piece - 2, n_piece - 1):
        wait_out(final, jnp.int32(c))
    for f in range(n_chunk):
        send_copy(final, f).wait_send()
    out.wait()


def run_backward(top_block, n_blocks, grad, saved, u_all, weights):
    n_rows, d_model = grad.shape
    d_ff = weights[0].shape[2]
    tiles = n_rows // TILE
    n_chunk = d_ff // CHUNK
    return pl.pallas_call(
        functools.partial(backward_kernel, top_block, n_blocks, tiles),
        name="backward",
        out_shape=[
            jax.ShapeDtypeStruct((n_rows, d_model), BF16),
            jax.ShapeDtypeStruct((n_blocks, d_model, d_ff), F32),
            jax.ShapeDtypeStruct((n_blocks, d_model, d_ff), F32),
            jax.ShapeDtypeStruct((d_model, d_ff), F32),
        ] + [jax.ShapeDtypeStruct((d_model, d_ff), BF16)] * 3,
        in_specs=[ANY] * 7,
        out_specs=[ANY] * 7,
        scratch_shapes=[
            pltpu.VMEM((n_rows, d_model), BF16),
            pltpu.VMEM((2, d_model, d_ff), BF16),
            pltpu.VMEM((2, d_ff, d_model), BF16),
            pltpu.VMEM((2, d_model, d_ff), F32),
            pltpu.VMEM((RING, TILE, CHUNK), F32),
            pltpu.VMEM((2, TILE, d_model), BF16),
            pltpu.VMEM((2, d_model, TILE), BF16),
            pltpu.VMEM((2, d_model, TILE), BF16),
            pltpu.VMEM((TILE, d_model), F32),
            pltpu.VMEM((2, TILE, CHUNK), F32),
            pltpu.VMEM((2, d_model, PIECE), F32),
            pltpu.VMEM((2, d_model, PIECE), F32),
            pltpu.VMEM((2, d_model, PIECE), BF16),
            pltpu.SemaphoreType.DMA(()),
            pltpu.SemaphoreType.DMA((2, 2)),
            pltpu.SemaphoreType.DMA((RING,)),
            pltpu.SemaphoreType.DMA((2,)),
            pltpu.SemaphoreType.DMA((n_chunk,)),
            pltpu.SemaphoreType.DMA((n_chunk,)),
            pltpu.SemaphoreType.DMA((n_blocks, n_chunk)),
            pltpu.SemaphoreType.DMA((2, 2)),
            pltpu.SemaphoreType.DMA((2,)),
        ],
        compiler_params=pltpu.CompilerParams(collective_id=1, has_side_effects=True, vmem_limit_bytes=67043328),
        cost_estimate=pl.CostEstimate(flops=8 * n_blocks * n_rows * d_model * d_ff, bytes_accessed=400 * 2**20, transcendentals=0),
    )(grad, saved, u_all, *weights)


def chain_kernel(top_block, tiles, g_hbm, u_hbm, w1_loc, w2_loc, wg1, wg2, g_all, r_all, a_all,
                 act, w1_buf, w2_buf, u_buf, r_buf, a_buf, acc, g_sem, w_sem, u_sem, r_sem, a_sem, s_sem):
    me = lax.axis_index("stage")
    d_ff = u_buf.shape[2]
    n_blocks = top_block + 1
    sources, buffers = (w1_loc, w2_loc, wg1, wg2), (w1_buf, w2_buf)
    steps = n_blocks * tiles

    def u_copy(bt):
        par = lax.rem(bt, 2)
        return pltpu.make_async_copy(u_hbm.at[top_block - bt // tiles, _tile_rows(lax.rem(bt, tiles)), :], u_buf.at[par], u_sem.at[par])

    def out_copies(bt):
        par = lax.rem(bt, 2)
        blk, rows = top_block - bt // tiles, _tile_rows(lax.rem(bt, tiles))
        return [pltpu.make_async_copy(r_buf.at[par], r_all.at[blk, rows, :], r_sem.at[par]),
                pltpu.make_async_copy(a_buf.at[par], a_all.at[blk, rows, :], a_sem.at[par])]

    def g_save(bt):
        rows = _tile_rows(lax.rem(bt, tiles))
        return pltpu.make_async_copy(act.at[rows, :], g_all.at[top_block - bt // tiles, rows, :], s_sem)

    g_in = pltpu.make_async_copy(g_hbm, act, g_sem)
    g_in.start()
    _start_weights(me, sources, buffers, w_sem, top_block, 0)
    u_copy(0).start()
    g_in.wait()

    @pl.loop(0, steps)
    def _(bt):
        i = bt // tiles
        tile = lax.rem(bt, tiles)
        blk = top_block - i
        par = lax.rem(i, 2)
        b_par = lax.rem(bt, 2)
        rows = _tile_rows(tile)

        @pl.when(tile == 0)
        def _():
            for cp in _weight_loads(sources, buffers, w_sem, blk, par, True):
                cp.wait()

            @pl.when(i + 1 < n_blocks)
            def _():
                _start_weights(me, sources, buffers, w_sem, blk - 1, 1 - par)

        @pl.when(bt + 1 < steps)
        def _():
            u_copy(bt + 1).start()

        g_save(bt).start()
        u_copy(bt).wait()

        @pl.when(bt >= 2)
        def _():
            for cp in out_copies(bt - 2):
                cp.wait()

        def body(with_input_grad):
            g = act[rows, :]
            n_chunk = d_ff // CHUNK
            for f in range(n_chunk):
                cols = slice(f * CHUNK, (f + 1) * CHUNK)
                q = _dot_t(g, w2_buf[par, cols, :])
                a, slope = _gelu_grad(u_buf[b_par, :, cols])
                r = (q * slope).astype(BF16)
                a_buf[b_par, :, cols] = a.astype(BF16)
                r_buf[b_par, :, cols] = r
                if with_input_grad:
                    part = _dot_t(r, w1_buf[par, :, cols])
                    if f == 0:
                        acc[...] = part
                    else:
                        acc[...] += part

        @pl.when(blk > 0)
        def _():
            body(True)

        @pl.when(blk == 0)
        def _():
            body(False)

        for cp in out_copies(bt):
            cp.start()
        g_save(bt).wait()

        @pl.when(blk > 0)
        def _():
            act[rows, :] = (act[rows, :].astype(F32) + acc[...]).astype(BF16)

    for bt in (steps - 2, steps - 1):
        for cp in out_copies(jnp.int32(bt)):
            cp.wait()


def run_chain(top_block, grad, u_all, weights):
    n_rows, d_model = grad.shape
    d_ff = weights[0].shape[2]
    tiles = n_rows // TILE
    n_blocks = top_block + 1
    return pl.pallas_call(
        functools.partial(chain_kernel, top_block, tiles),
        name="chain",
        out_shape=[
            jax.ShapeDtypeStruct((n_blocks, n_rows, d_model), BF16),
            jax.ShapeDtypeStruct((n_blocks, n_rows, d_ff), BF16),
            jax.ShapeDtypeStruct((n_blocks, n_rows, d_ff), BF16),
        ],
        in_specs=[ANY] * 6,
        out_specs=[ANY] * 3,
        scratch_shapes=[
            pltpu.VMEM((n_rows, d_model), BF16),
            pltpu.VMEM((2, d_model, d_ff), BF16),
            pltpu.VMEM((2, d_ff, d_model), BF16),
            pltpu.VMEM((2, TILE, d_ff), F32),
            pltpu.VMEM((2, TILE, d_ff), BF16),
            pltpu.VMEM((2, TILE, d_ff), BF16),
            pltpu.VMEM((TILE, d_model), F32),
            pltpu.SemaphoreType.DMA(()),
            pltpu.SemaphoreType.DMA((2, 2)),
            pltpu.SemaphoreType.DMA((2,)),
            pltpu.SemaphoreType.DMA((2,)),
            pltpu.SemaphoreType.DMA((2,)),
            pltpu.SemaphoreType.DMA(()),
        ],
        compiler_params=pltpu.CompilerParams(vmem_limit_bytes=62 * 2**20),
        cost_estimate=pl.CostEstimate(flops=4 * n_blocks * n_rows * d_model * d_ff, bytes_accessed=400 * 2**20, transcendentals=0),
    )(grad, u_all, *weights)


DW_ROWS = 1024


def weight_grad_kernel(first_col, saved, g_all, r_all, a_all, own, part1, part2, part3,
                       x_buf, g_buf, r_buf, a_buf, dw, sib, o_buf, in_sem, send_sem, recv_sem, out_sem):
    me = lax.axis_index("stage")
    core = lax.axis_index("data")
    width = dw.shape[3]
    row_steps = saved.shape[1] // DW_ROWS
    steps = 4 * row_steps
    cols = pl.ds(first_col, width)

    def owner_at(n):
        return jnp.where(n == 0, 3, jnp.where(n == 3, 0, n))

    def block_at(n):
        rel = owner_at(n)
        bit0 = lax.rem(lax.rem(me, 2) + lax.rem(rel, 2), 2)
        bit1 = lax.rem(me // 2 + rel // 2, 2)
        return bit0 + 2 * bit1

    def loads(step):
        par = lax.rem(step, 2)
        blk = block_at(step // row_steps)
        rows = pl.ds(pl.multiple_of(lax.rem(step, row_steps) * DW_ROWS, DW_ROWS), DW_ROWS)
        return [pltpu.make_async_copy(saved.at[blk, rows, :], x_buf.at[par], in_sem.at[par, 0]),
                pltpu.make_async_copy(g_all.at[blk, rows, :], g_buf.at[par], in_sem.at[par, 1]),
                pltpu.make_async_copy(r_all.at[blk, rows, cols], r_buf.at[par], in_sem.at[par, 2]),
                pltpu.make_async_copy(a_all.at[blk, rows, cols], a_buf.at[par], in_sem.at[par, 3])]

    def send_copy(n):
        par = lax.rem(n, 2)
        return pltpu.make_async_remote_copy(
            src_ref=dw.at[par, 1 - core], dst_ref=sib.at[n], send_sem=send_sem.at[par], recv_sem=recv_sem.at[n],
            device_id=(me, 1 - core), device_id_type=MESH)

    def part_copy(which):
        return pltpu.make_async_copy(o_buf, (part3, part1, part2)[which], out_sem)

    for cp in loads(0):
        cp.start()
    _sibling_barrier(me, core)

    @pl.loop(0, steps)
    def _(step):
        n = step // row_steps
        k = lax.rem(step, row_steps)
        par = lax.rem(step, 2)
        d_par = lax.rem(n, 2)

        @pl.when(step + 1 < steps)
        def _():
            for cp in loads(step + 1):
                cp.start()

        @pl.when((k == 0) & (n >= 2))
        def _():
            send_copy(n).wait_send()
        for which in range(3):
            @pl.when((k == 1) & (n == which + 1))
            def _(which=which):
                if which > 0:
                    part_copy(which - 1).wait()
                send_copy(jnp.int32(which)).wait_recv()
                o_buf[...] = (dw[which % 2, core] + sib[which]).astype(BF16)
                part_copy(which).start()
        for cp in loads(step):
            cp.wait()
        x_t = x_buf[par].T
        g_t = g_buf[par].T
        first = k == 0
        d1 = _dot(x_t, r_buf[par])
        d2 = _dot(g_t, a_buf[par])
        dw[d_par, 0] = jnp.where(first, 0.0, dw[d_par, 0]) + d1
        dw[d_par, 1] = jnp.where(first, 0.0, dw[d_par, 1]) + d2

        @pl.when(k == row_steps - 1)
        def _():
            send_copy(n).start()

    part_copy(2).wait()
    last = jnp.int32(3)
    send_copy(last).wait_recv()
    sib[3] = dw[1, core] + sib[3]
    done = pltpu.make_async_copy(sib.at[3], own, out_sem)
    done.start()
    done.wait()
    for n in (2, 3):
        send_copy(jnp.int32(n)).wait_send()


def run_weight_grad(first_col, width, ident, saved, g_all, r_all, a_all):
    n_rows, d_model = saved.shape[1:]
    return pl.pallas_call(
        functools.partial(weight_grad_kernel, first_col),
        name=f"weight_grad_{first_col}",
        out_shape=[jax.ShapeDtypeStruct((d_model, width), F32)] + [jax.ShapeDtypeStruct((d_model, width), BF16)] * 3,
        in_specs=[ANY] * 4,
        out_specs=[ANY] * 4,
        scratch_shapes=[
            pltpu.VMEM((2, DW_ROWS, d_model), BF16),
            pltpu.VMEM((2, DW_ROWS, d_model), BF16),
            pltpu.VMEM((2, DW_ROWS, width), BF16),
            pltpu.VMEM((2, DW_ROWS, width), BF16),
            pltpu.VMEM((2, 2, d_model, width), F32),
            pltpu.VMEM((4, d_model, width), F32),
            pltpu.VMEM((d_model, width), BF16),
            pltpu.SemaphoreType.DMA((2, 4)),
            pltpu.SemaphoreType.DMA((2,)),
            pltpu.SemaphoreType.DMA((4,)),
            pltpu.SemaphoreType.DMA(()),
        ],
        compiler_params=pltpu.CompilerParams(collective_id=ident, has_side_effects=True, vmem_limit_bytes=62 * 2**20),
        cost_estimate=pl.CostEstimate(flops=16 * n_rows * d_model * width, bytes_accessed=100 * 2**20, transcendentals=0),
    )(saved, g_all, r_all, a_all)


COMBINE_ROWS = 96


def combine_kernel(own, got1, got2, got3, *refs):
    total, squares = refs[-2:]
    step = pl.program_id(0)
    val = (own[...] + got1[...].astype(F32)) + (got2[...].astype(F32) + got3[...].astype(F32))
    total[0] = val
    part = jnp.sum((val * val).reshape(-1, 8, val.shape[1]), axis=0)
    folded = part[:, :128]
    for j in range(1, val.shape[1] // 128):
        folded = folded + part[:, j * 128:(j + 1) * 128]
    squares[...] = jnp.where(step == 0, 0.0, squares[...]) + folded


def run_combine(shape, half, first_col, own, got, total=None):
    d_model, width = own.shape
    block = (COMBINE_ROWS, width)
    spec = pl.BlockSpec(block, lambda i: (i, 0))
    earlier = [] if total is None else [total]
    return pl.pallas_call(
        combine_kernel,
        name="combine",
        grid=(d_model // COMBINE_ROWS,),
        out_shape=[jax.ShapeDtypeStruct(shape, F32), jax.ShapeDtypeStruct((8, 128), F32)],
        in_specs=[spec] * 4 + [ANY] * len(earlier),
        out_specs=[pl.BlockSpec((1,) + block, lambda i: (half, i, first_col // width)), pl.BlockSpec((8, 128), lambda i: (0, 0))],
        input_output_aliases={4: 0} if earlier else {},
        compiler_params=pltpu.CompilerParams(dimension_semantics=("arbitrary",)),
        cost_estimate=pl.CostEstimate(flops=10**9, bytes_accessed=20 * 2**20, transcendentals=0),
    )(own, *got, *earlier)


def scalars_kernel(tau_clip, squares, loss, clip_out, loss_out, mine, gathered, send_sem, recv_sem):
    stage = lax.axis_index("stage")
    core = lax.axis_index("data")
    n_dev = gathered.shape[0]
    here = stage * 2 + core
    barrier = pltpu.get_barrier_semaphore()
    for k in range(1, n_dev):
        other = lax.rem(here + k, n_dev)
        pl.semaphore_signal(barrier, inc=1, device_id=(other // 2, lax.rem(other, 2)), device_id_type=MESH)
    mine[0] = squares[...]
    mine[1] = loss[...]
    gathered[here] = mine[...]
    pl.semaphore_wait(barrier, n_dev - 1)

    def copy(k, slot):
        other = lax.rem(here + k, n_dev)
        return pltpu.make_async_remote_copy(
            src_ref=mine, dst_ref=gathered.at[slot], send_sem=send_sem.at[k], recv_sem=recv_sem.at[k],
            device_id=(other // 2, lax.rem(other, 2)), device_id_type=MESH)

    for k in range(1, n_dev):
        copy(k, here).start()
    for k in range(1, n_dev):
        copy(k, lax.rem(here + n_dev - k, n_dev)).wait_recv()
    sums = jnp.sum(gathered[...], axis=0)
    squared = jnp.sum(jnp.sum(sums[0], axis=0, keepdims=True), axis=1, keepdims=True)
    lost = jnp.sum(jnp.sum(sums[1], axis=0, keepdims=True), axis=1, keepdims=True)
    norm = jnp.sqrt(jnp.broadcast_to(squared, (8, 128)))
    clip_out[...] = jnp.minimum(1.0, tau_clip / norm)
    loss_out[...] = jnp.broadcast_to(lost, (8, 128))
    for k in range(1, n_dev):
        copy(k, here).wait_send()


def run_scalars(tau_clip, squares, loss):
    vmem = pl.BlockSpec(memory_space=pltpu.VMEM)
    return pl.pallas_call(
        functools.partial(scalars_kernel, tau_clip),
        name="scalars",
        out_shape=[jax.ShapeDtypeStruct((8, 128), F32)] * 2,
        in_specs=[vmem] * 2,
        out_specs=[vmem] * 2,
        scratch_shapes=[
            pltpu.VMEM((2, 8, 128), F32),
            pltpu.VMEM((8, 2, 8, 128), F32),
            pltpu.SemaphoreType.DMA((8,)),
            pltpu.SemaphoreType.DMA((8,)),
        ],
        compiler_params=pltpu.CompilerParams(collective_id=7, has_side_effects=True),
    )(squares, loss)


FLAT_ROWS = 1536


def update_kernel(learn_rate, grad, clip, w_old, m_old, v_old, w_new, m_new, v_new, w1_half, w2_half,
                  g_one, g_two, flat, wide, n_one, n_two, g_sem, n_sem):
    step = pl.program_id(0)
    core = lax.axis_index("data")
    d_model, d_ff = grad.shape[1], grad.shape[2]
    rows1, rows2 = FLAT_ROWS * 128 // d_ff, FLAT_ROWS * 128 // d_model
    chunks = d_model // rows1
    steps = 2 * chunks

    def g_copy(n, of_core):
        par = lax.rem(n, 2)
        half, chunk = n // chunks, lax.rem(n, chunks)
        if of_core == 0:
            return pltpu.make_async_copy(grad.at[half, pl.ds(pl.multiple_of(chunk * rows1, rows1), rows1), :], g_one.at[par], g_sem.at[par])
        return pltpu.make_async_copy(grad.at[half, :, pl.ds(pl.multiple_of(chunk * rows2, rows2), rows2)], g_two.at[par], g_sem.at[par])

    def n_copy(n, of_core):
        par = lax.rem(n, 2)
        half, chunk = n // chunks, lax.rem(n, chunks)
        if of_core == 0:
            return pltpu.make_async_copy(n_one.at[par], w1_half.at[half, pl.ds(pl.multiple_of(chunk * rows1, rows1), rows1), :], n_sem.at[par])
        return pltpu.make_async_copy(n_two.at[par], w2_half.at[half, pl.ds(pl.multiple_of(chunk * rows2, rows2), rows2), :], n_sem.at[par])

    par = lax.rem(step, 2)
    for of_core in range(2):
        @pl.when(core == of_core)
        def _(of_core=of_core):
            @pl.when(step == 0)
            def _():
                g_copy(step, of_core).start()

            @pl.when(step + 1 < steps)
            def _():
                g_copy(step + 1, of_core).start()
            g_copy(step, of_core).wait()
            if of_core == 0:
                val = g_one[par]
                per_row = d_ff // 128
            else:
                val = g_two[par].T
                per_row = d_model // 128
            for j in range(per_row):
                flat[pl.ds(j, val.shape[0], per_row), :] = val[:, j * 128:(j + 1) * 128]

    grad_clip = jnp.broadcast_to(clip[0:1, :], (FLAT_ROWS, 128)) * flat[...]
    m_val = BETA_ONE * m_old[...] + (1.0 - BETA_ONE) * grad_clip
    v_val = BETA_TWO * v_old[...] + (1.0 - BETA_TWO) * grad_clip * grad_clip
    m_hat = m_val * (1.0 / (1.0 - BETA_ONE ** ADAM_STEP))
    v_hat = v_val * (1.0 / (1.0 - BETA_TWO ** ADAM_STEP))
    w_val = w_old[...]
    w_val = w_val - learn_rate * (m_hat / (jnp.sqrt(v_hat) + ADAM_EPS) + WEIGHT_DECAY * w_val)
    m_new[...] = m_val
    v_new[...] = v_val
    w_new[...] = w_val
    wide[...] = w_val

    for of_core in range(2):
        @pl.when(core == of_core)
        def _(of_core=of_core):
            @pl.when(step >= 2)
            def _():
                n_copy(step - 2, of_core).wait()
            buf, per_row = (n_one, d_ff // 128) if of_core == 0 else (n_two, d_model // 128)
            for j in range(per_row):
                buf[par, :, j * 128:(j + 1) * 128] = wide[pl.ds(j, buf.shape[1], per_row), :].astype(BF16)
            n_copy(step, of_core).start()

            @pl.when(step == steps - 1)
            def _():
                n_copy(step - 1, of_core).wait()
                n_copy(step, of_core).wait()


def run_update(learn_rate, grad, clip, w_old, m_old, v_old):
    _, d_model, d_ff = grad.shape
    rows1, rows2 = FLAT_ROWS * 128 // d_ff, FLAT_ROWS * 128 // d_model
    steps = w_old.shape[0] // FLAT_ROWS
    flat_spec = pl.BlockSpec((FLAT_ROWS, 128), lambda i: (i, 0))
    flat_shape = jax.ShapeDtypeStruct(w_old.shape, F32)
    return pl.pallas_call(
        functools.partial(update_kernel, learn_rate),
        name="update",
        grid=(steps,),
        out_shape=[flat_shape] * 3 + [jax.ShapeDtypeStruct((2, d_model, d_ff), BF16), jax.ShapeDtypeStruct((2, d_ff, d_model), BF16)],
        in_specs=[ANY, pl.BlockSpec((8, 128), lambda i: (0, 0))] + [flat_spec] * 3,
        out_specs=[flat_spec] * 3 + [ANY, ANY],
        scratch_shapes=[
            pltpu.VMEM((2, rows1, d_ff), F32),
            pltpu.VMEM((2, d_model, rows2), F32),
            pltpu.VMEM((FLAT_ROWS, 128), F32),
            pltpu.VMEM((FLAT_ROWS, 128), F32),
            pltpu.VMEM((2, rows1, d_ff), BF16),
            pltpu.VMEM((2, rows2, d_model), BF16),
            pltpu.SemaphoreType.DMA((2,)),
            pltpu.SemaphoreType.DMA((2,)),
        ],
        compiler_params=pltpu.CompilerParams(dimension_semantics=("arbitrary",), vmem_limit_bytes=40 * 2**20),
        cost_estimate=pl.CostEstimate(flops=10**9, bytes_accessed=150 * 2**20, transcendentals=0),
    )(grad, clip, w_old, m_old, v_old)


GROUPS = ((0, 1024), (1024, 1024), (2048, 512), (2560, 512))


def solution(mesh):
    n_stage = mesh.shape["stage"]
    n_data = mesh.shape["data"]
    axes = ("stage", "data")

    def device(stage, core):
        return stage * n_data + core

    def from_core(core):
        return [(device(s, core), device(s, 1 - core)) for s in range(n_stage)]

    def across(flip):
        return [(device(s, c), device(s ^ flip, c)) for s in range(n_stage) for c in range(n_data)]

    def exchange(parts):
        return [lax.ppermute(part, axes, across(flip)) for flip, part in enumerate(parts, start=1)]

    def device_step(x_loc, t_loc, w1_loc, w2_loc, wm_loc, m_loc, v_loc):
        n_micro, n_tok, d_model = x_loc.shape
        d_ff = w1_loc.shape[4]
        n_tokens = n_micro * n_tok * n_data
        n_blocks = 2 * n_stage
        n_rows = n_micro * n_tok // n_stage
        tau_clip = 0.3 * d_model * math.sqrt(n_blocks * (3.0 / n_tokens + 0.008))
        learn_rate = 0.1 / math.sqrt(4.0 * d_model * n_blocks)
        stage_idx = lax.axis_index("stage")
        core = lax.axis_index("data")
        w1 = w1_loc.reshape(2, d_model, d_ff)
        w2 = w2_loc.reshape(2, d_ff, d_model)
        wg1, wg2, saved, u_all = run_forward(x_loc.reshape(n_micro * n_tok, d_model), w1, w2, n_rows)
        weights = (w1, w2, wg1, wg2)
        target = lax.dynamic_slice_in_dim(t_loc.reshape(n_micro * n_tok, d_model), stage_idx * n_rows, n_rows, 0)
        residual = saved[n_blocks].astype(F32) - target.astype(F32)
        loss_acc = 0.5 * jnp.sum((residual * residual).reshape(-1, 8, d_model // 128, 128), axis=(0, 2))
        seed = (residual / n_tokens).astype(BF16)
        grad, _, _, own_hi, *parts_hi = run_backward(7, 4, seed, saved, u_all, weights)
        got_hi = exchange(parts_hi)
        g_all, r_all, a_all = run_chain(3, grad, u_all, weights)
        low = []
        for ident, (first, width) in enumerate(GROUPS):
            own, *parts = run_weight_grad(first, width, 2 + ident, saved, g_all, r_all, a_all)
            low.append((first, own, exchange(parts)))
        shape = (2, d_model, d_ff)
        total, squares = run_combine(shape, 1, 0, own_hi, got_hi)
        for first, own, got in low:
            total, more = run_combine(shape, 0, first, own, got, total)
            squares = squares + more
        clip, loss_all = run_scalars(tau_clip, squares, loss_acc)
        flat = [val.reshape(-1, 128) for val in (wm_loc, m_loc, v_loc)]
        w_new, m_new, v_new, w1_half, w2_half = run_update(learn_rate, total, clip, *flat)
        w1_got = lax.ppermute(w1_half, axes, from_core(0))
        w2_got = lax.ppermute(w2_half, axes, from_core(1))
        w1_new = jnp.where(core == 0, w1_half, w1_got).reshape(w1_loc.shape)
        w2_new = jnp.where(core == 1, w2_half, w2_got).reshape(w2_loc.shape)
        mean_loss = loss_all[0, 0] / n_tokens
        return w1_new, w2_new, w_new.reshape(wm_loc.shape), m_new.reshape(wm_loc.shape), v_new.reshape(wm_loc.shape), mean_loss

    act_spec = P(None, "data", None)
    flat_spec = P("stage", None, None, "data")
    return jax.shard_map(device_step, mesh=mesh, in_specs=(act_spec, act_spec, P("stage"), P("stage"), flat_spec, flat_spec, flat_spec), out_specs=(P("stage"), P("stage"), flat_spec, flat_spec, flat_spec, P()), check_vma=False)
```

```python
import functools
import math
import jax
import jax.numpy as jnp
from jax import lax
from jax.experimental import pallas as pl
from jax.experimental.pallas import tpu as pltpu
from jax.sharding import PartitionSpec as P

BETA_ONE = 0.9
BETA_TWO = 0.999
ADAM_EPS = 1e-8
WEIGHT_DECAY = 0.1
ADAM_STEP = 1000
GELU_A = math.sqrt(2.0 / math.pi)
GELU_B = GELU_A * 0.044715
MESH = pl.DeviceIdType.MESH
ANY = pl.BlockSpec(memory_space=pl.ANY)
F32 = jnp.float32
BF16 = jnp.bfloat16

TILE = 512
PATH_PIECES = 4


def _dot_t(lhs, rhs):
    return lax.dot_general(lhs, rhs, (((1,), (1,)), ((), ())), preferred_element_type=F32)


def _dot(lhs, rhs):
    return jnp.dot(lhs, rhs, preferred_element_type=F32)


SEND_SLOT = (-45, -30, -28, -20)
HOP_SLOT = {1: (-27, -20, -18, -14), 2: (-18, -14, -8, -6), 3: (-12, -9, -2, -2)}
LOAD_SLOT = -1


def forward_kernel(n_blocks, tiles, n_tokens, x_hbm, t_hbm, w1_loc, w2_loc, wg1, wg2, saved, u_out, seed, loss,
                   act, w1_buf, w2_buf, u_buf, acc, t_buf, s_buf,
                   x_sem, act_sem, u_sem, w_sem, t_sem, s_sem, ici_send, ici_recv, d2d_send, d2d_recv):
    me = lax.axis_index("stage")
    core = lax.axis_index("data")
    d_model, d_ff = w1_loc.shape[1], w1_loc.shape[2]
    n_rows = act.shape[0]
    n_piece = 4 * PATH_PIECES
    rows1, rows2 = d_model // n_piece, d_ff // n_piece

    def peer(flip):
        bit0, bit1 = lax.rem(me, 2), me // 2
        return (1 - bit0 + 2 * bit1) if flip == 1 else (bit0 + 2 * (1 - bit1))

    def rel_of(blk):
        own = lax.rem(blk, 4)
        a0, a1, b0, b1 = lax.rem(me, 2), me // 2, lax.rem(own, 2), own // 2
        return (a0 + b0 - 2 * a0 * b0) + 2 * (a1 + b1 - 2 * a1 * b1)

    def piece(j, path, of_core):
        return j * 4 + path * 2 + of_core

    def views(blk, idx):
        return (wg1.at[blk, pl.ds(pl.multiple_of(idx * rows1, 16), rows1), :],
                wg2.at[blk, pl.ds(pl.multiple_of(idx * rows2, 64), rows2), :])

    def local_views(blk, idx):
        half = blk // 4
        return (w1_loc.at[half, pl.ds(pl.multiple_of(idx * rows1, 16), rows1), :],
                w2_loc.at[half, pl.ds(pl.multiple_of(idx * rows2, 64), rows2), :])

    def ici_copies(blk, path, j, sources, flip):
        idx = piece(j, path, core)
        slot = path * PATH_PIECES + j
        return [pltpu.make_async_remote_copy(
            src_ref=src, dst_ref=dst, send_sem=ici_send.at[blk, slot, m], recv_sem=ici_recv.at[blk, slot, m],
            device_id=(peer(flip), core), device_id_type=MESH)
            for m, (src, dst) in enumerate(zip(sources, views(blk, idx)))]

    def d2d_copies(blk, path, j, of_core):
        idx = piece(j, path, of_core)
        slot = path * PATH_PIECES + j
        return [pltpu.make_async_remote_copy(
            src_ref=ref, dst_ref=ref, send_sem=d2d_send.at[blk, slot, m], recv_sem=d2d_recv.at[blk, slot, m],
            device_id=(me, 1 - core), device_id_type=MESH) for m, ref in enumerate(views(blk, idx))]

    def first_flip(path):
        return 1 if path == 0 else 2

    def own_send(blk, j):
        @pl.when(rel_of(blk) == 0)
        def _():
            for path in range(2):
                for cp in ici_copies(blk, path, j, local_views(blk, piece(j, path, core)), first_flip(path)):
                    cp.start()

    def hop_event(blk, hop, j):
        rel = rel_of(blk)
        for path in range(2):
            at_rel = {1: (1, 2), 2: (3, 3), 3: (2, 1)}[hop][path]

            @pl.when(rel == at_rel)
            def _(path=path):
                flip = first_flip(path)
                if hop == 1:
                    flip = 3 - flip
                copies = ici_copies(blk, path, j, views(blk, piece(j, path, core)), flip)
                for cp in copies:
                    cp.wait_recv()
                if hop < 3:
                    for cp in copies:
                        cp.start()
                for cp in d2d_copies(blk, path, j, core):
                    cp.start()

    def weight_loads(blk, par, is_own):
        half = blk // 4
        src1, src2 = (w1_loc.at[half], w2_loc.at[half]) if is_own else (wg1.at[blk], wg2.at[blk])
        return [pltpu.make_async_copy(src1, w1_buf.at[par], w_sem.at[par, 0]),
                pltpu.make_async_copy(src2, w2_buf.at[par], w_sem.at[par, 1])]

    def load_event(blk):
        rel = rel_of(blk)
        par = lax.rem(blk, 2)

        @pl.when(rel == 0)
        def _():
            for cp in weight_loads(blk, par, True):
                cp.start()

        @pl.when(rel != 0)
        def _():
            for path in range(2):
                for j in range(PATH_PIECES):
                    for cp in d2d_copies(blk, path, j, 1 - core):
                        cp.wait_recv()
            for cp in weight_loads(blk, par, False):
                cp.start()

    def x_copy():
        return pltpu.make_async_copy(x_hbm.at[pl.ds(pl.multiple_of(me * n_rows, n_rows), n_rows), :], act, x_sem)

    def act_copy(slot, tile):
        rows = pl.ds(pl.multiple_of(tile * TILE, TILE), TILE)
        return pltpu.make_async_copy(act.at[rows, :], saved.at[slot, rows, :], act_sem.at[tile])

    def t_copy(tile):
        return pltpu.make_async_copy(t_hbm.at[pl.ds(pl.multiple_of(me * n_rows + tile * TILE, TILE), TILE), :], t_buf, t_sem)

    def seed_copy(tile):
        return pltpu.make_async_copy(s_buf, seed.at[pl.ds(pl.multiple_of(tile * TILE, TILE), TILE), :], s_sem)

    def u_copy(blk, tile, par):
        rows = pl.ds(pl.multiple_of(tile * TILE, TILE), TILE)
        return pltpu.make_async_copy(u_buf.at[par], u_out.at[blk, rows, :], u_sem.at[par])

    barrier = pltpu.get_barrier_semaphore()
    for target in ((peer(1), core), (peer(2), core), (me, 1 - core)):
        pl.semaphore_signal(barrier, inc=1, device_id=target, device_id_type=MESH)
    x_copy().start()
    pl.semaphore_wait(barrier, 3)

    events = []
    for hop in (3, 2, 1):
        for j in range(PATH_PIECES):
            events.append((HOP_SLOT[hop][j], functools.partial(lambda blk, hop, j: hop_event(blk, hop, j), hop=hop, j=j)))
    for j in range(PATH_PIECES):
        events.append((SEND_SLOT[j], functools.partial(lambda blk, j: own_send(blk, j), j=j)))
    events.append((LOAD_SLOT, load_event))

    def comm_slot(blk, tile):
        for offset, fn in events:
            residue = offset % tiles
            ahead = (residue - offset) // tiles
            target = blk + ahead

            @pl.when((tile == residue) & (target >= 0) & (target < n_blocks))
            def _(fn=fn, target=target):
                fn(target)

    def compute(blk, tile):
        par = lax.rem(blk, 2)
        u_par = lax.rem(tile, 2)
        rows = pl.ds(pl.multiple_of(tile * TILE, TILE), TILE)

        @pl.when(tile == 0)
        def _():
            for cp in weight_loads(blk, par, True):
                cp.wait()

        @pl.when((blk == 0) & (tile == 0))
        def _():
            x_copy().wait()
            for t in range(tiles):
                act_copy(0, t).start()

        @pl.when((blk > 0) | (tile > 1))
        def _():
            u_copy(blk, tile, u_par).wait()

        @pl.when(blk == n_blocks - 1)
        def _():
            t_copy(tile).start()

        act_copy(blk, tile).wait()
        x = act[rows, :]
        chunk = 256
        n_chunk = d_ff // chunk
        for f in range(n_chunk):
            cols = slice(f * chunk, (f + 1) * chunk)
            u = _dot(x, w1_buf[par, :, cols])
            u_buf[u_par, :, cols] = u
            inner = u * (GELU_A + GELU_B * (u * u))
            a = (u * (0.5 + 0.5 * jnp.tanh(inner))).astype(BF16)
            part = _dot(a, w2_buf[par, cols, :])
            if f == 0:
                acc[...] = part
            elif f < n_chunk - 1:
                acc[...] += part
            else:
                act[rows, :] = (x.astype(F32) + (acc[...] + part)).astype(BF16)
        u_copy(blk, tile, u_par).start()

        @pl.when(blk < n_blocks - 1)
        def _():
            act_copy(blk + 1, tile).start()

        @pl.when(blk == n_blocks - 1)
        def _():
            t_copy(tile).wait()

            @pl.when(tile > 0)
            def _():
                seed_copy(tile - 1).wait()
            residual = act[rows, :].astype(F32) - t_buf[...].astype(F32)
            s_buf[...] = (residual / n_tokens).astype(BF16)
            squares = jnp.sum((residual * residual).reshape(TILE // 8, 8, residual.shape[1]), axis=0)
            folded = squares[:, :128]
            for j in range(1, residual.shape[1] // 128):
                folded = folded + squares[:, j * 128:(j + 1) * 128]
            loss[...] += 0.5 * folded
            seed_copy(tile).start()

    lead = -(min(SEND_SLOT) // tiles)
    loss[...] = jnp.zeros_like(loss)

    @pl.loop(0, (n_blocks + lead) * tiles)
    def _(step):
        blk = step // tiles - lead
        tile = lax.rem(step, tiles)
        comm_slot(blk, tile)

        @pl.when(blk >= 0)
        def _():
            compute(blk, tile)

    for par in range(2):
        u_copy(0, 0, par).wait()
    seed_copy(0).wait()

    @pl.loop(0, n_blocks)
    def _(blk):
        rel = rel_of(blk)
        for path in range(2):
            last = (2, 1)[path]

            @pl.when(rel != last)
            def _(path=path):
                for j in range(PATH_PIECES):
                    for cp in ici_copies(blk, path, j, views(blk, piece(j, path, core)), 1):
                        cp.wait_send()

        @pl.when(rel != 0)
        def _():
            for path in range(2):
                for j in range(PATH_PIECES):
                    for cp in d2d_copies(blk, path, j, core):
                        cp.wait_send()


def run_forward(n_tokens, x_flat, t_flat, w1_loc, w2_loc, n_rows):
    n_half, d_model, d_ff = w1_loc.shape
    n_blocks = 4 * n_half
    tiles = n_rows // TILE
    slots = 2 * PATH_PIECES
    out_shape = [
        jax.ShapeDtypeStruct((n_blocks, d_model, d_ff), BF16),
        jax.ShapeDtypeStruct((n_blocks, d_ff, d_model), BF16),
        jax.ShapeDtypeStruct((n_blocks, n_rows, d_model), BF16),
        jax.ShapeDtypeStruct((n_blocks, n_rows, d_ff), F32),
        jax.ShapeDtypeStruct((n_rows, d_model), BF16),
        jax.ShapeDtypeStruct((8, 128), F32),
    ]
    return pl.pallas_call(
        functools.partial(forward_kernel, n_blocks, tiles, n_tokens),
        name="forward",
        out_shape=out_shape,
        in_specs=[ANY] * 4,
        out_specs=[ANY] * 5 + [pl.BlockSpec(memory_space=pltpu.VMEM)],
        scratch_shapes=[
            pltpu.VMEM((n_rows, d_model), BF16),
            pltpu.VMEM((2, d_model, d_ff), BF16),
            pltpu.VMEM((2, d_ff, d_model), BF16),
            pltpu.VMEM((2, TILE, d_ff), F32),
            pltpu.VMEM((TILE, d_model), F32),
            pltpu.VMEM((TILE, d_model), BF16),
            pltpu.VMEM((TILE, d_model), BF16),
            pltpu.SemaphoreType.DMA(()),
            pltpu.SemaphoreType.DMA((tiles,)),
            pltpu.SemaphoreType.DMA((2,)),
            pltpu.SemaphoreType.DMA((2, 2)),
            pltpu.SemaphoreType.DMA(()),
            pltpu.SemaphoreType.DMA(()),
            pltpu.SemaphoreType.DMA((n_blocks, slots, 2)),
            pltpu.SemaphoreType.DMA((n_blocks, slots, 2)),
            pltpu.SemaphoreType.DMA((n_blocks, slots, 2)),
            pltpu.SemaphoreType.DMA((n_blocks, slots, 2)),
        ],
        compiler_params=pltpu.CompilerParams(collective_id=0, has_side_effects=True, vmem_limit_bytes=60 * 2**20),
        cost_estimate=pl.CostEstimate(flops=4 * n_blocks * n_rows * d_model * d_ff, bytes_accessed=600 * 2**20, transcendentals=0),
    )(x_flat, t_flat, w1_loc, w2_loc)


RING = 4
CHUNK = 512
PIECE = 256


def _relation(me, blk):
    own = lax.rem(blk, 4)
    a0, a1, b0, b1 = lax.rem(me, 2), me // 2, lax.rem(own, 2), own // 2
    return (a0 + b0 - 2 * a0 * b0) + 2 * (a1 + b1 - 2 * a1 * b1)


def _weight_loads(sources, buffers, sems, blk, par, is_own):
    w1_loc, w2_loc, wg1, wg2 = sources
    half = blk // 4
    src1, src2 = (w1_loc.at[half], w2_loc.at[half]) if is_own else (wg1.at[blk], wg2.at[blk])
    return [pltpu.make_async_copy(src1, buffers[0].at[par], sems.at[par, 0]),
            pltpu.make_async_copy(src2, buffers[1].at[par], sems.at[par, 1])]


def _start_weights(me, sources, buffers, sems, blk, par):
    rel = _relation(me, blk)

    @pl.when(rel == 0)
    def _():
        for cp in _weight_loads(sources, buffers, sems, blk, par, True):
            cp.start()

    @pl.when(rel != 0)
    def _():
        for cp in _weight_loads(sources, buffers, sems, blk, par, False):
            cp.start()


def _tile_rows(tile):
    return pl.ds(pl.multiple_of(tile * TILE, TILE), TILE)


def _sibling_barrier(me, core):
    barrier = pltpu.get_barrier_semaphore()
    pl.semaphore_signal(barrier, inc=1, device_id=(me, 1 - core), device_id_type=MESH)
    pl.semaphore_wait(barrier, 1)


def _gelu_grad(u):
    cube = GELU_B * (u * u)
    th = jnp.tanh(u * (GELU_A + cube))
    cdf = 0.5 + 0.5 * th
    a = u * cdf
    return a, cdf + (a * (3.0 - 3.0 * th)) * (cube + GELU_A / 3.0)


def backward_kernel(top_block, n_blocks, tiles, g_hbm, saved, u_hbm, w1_loc, w2_loc, wg1, wg2, g_out, local, sib, own, part1, part2, part3,
                    act, w1_buf, w2_buf, dw, u_buf, x_buf, x_t, g_t, acc, q_buf, k_buf, s_buf, o_buf,
                    g_sem, w_sem, u_sem, x_sem, keep_sem, send_sem, recv_sem, load_sem, out_sem):
    me = lax.axis_index("stage")
    core = lax.axis_index("data")
    d_model, d_ff = dw.shape[1], dw.shape[2]
    n_chunk = d_ff // CHUNK
    n_piece = d_ff // PIECE
    sources, buffers = (w1_loc, w2_loc, wg1, wg2), (w1_buf, w2_buf)
    total = n_blocks * tiles * n_chunk

    def cols_of(f):
        return pl.ds(pl.multiple_of(f * CHUNK, CHUNK), CHUNK)

    def u_copy(step):
        blk = top_block - step // (tiles * n_chunk)
        tile = lax.rem(step // n_chunk, tiles)
        f = lax.rem(step, n_chunk)
        slot = lax.rem(step, RING)
        return pltpu.make_async_copy(u_hbm.at[blk, _tile_rows(tile), cols_of(f)], u_buf.at[slot], u_sem.at[slot])

    def x_copy(bt):
        par = lax.rem(bt, 2)
        return pltpu.make_async_copy(saved.at[top_block - bt // tiles, _tile_rows(lax.rem(bt, tiles)), :], x_buf.at[par], x_sem.at[par])

    def g_in_copy():
        return pltpu.make_async_copy(g_hbm, act, g_sem)

    def local_copies(i, f):
        return [pltpu.make_async_copy(dw.at[m, :, cols_of(f)], local.at[i, m, :, cols_of(f)], keep_sem.at[f, m]) for m in range(2)]

    def send_copy(i, f):
        return pltpu.make_async_remote_copy(
            src_ref=local.at[i, 1 - core, :, cols_of(f)], dst_ref=sib.at[i, :, cols_of(f)], send_sem=send_sem.at[i, f],
            recv_sem=recv_sem.at[i, f], device_id=(me, 1 - core), device_id_type=MESH)

    def piece_cols(c):
        return pl.ds(pl.multiple_of(c * PIECE, PIECE), PIECE)

    def piece_loads(i, c):
        par = lax.rem(c, 2)
        return [pltpu.make_async_copy(local.at[i, core, :, piece_cols(c)], k_buf.at[par], load_sem.at[par, 0]),
                pltpu.make_async_copy(sib.at[i, :, piece_cols(c)], s_buf.at[par], load_sem.at[par, 1])]

    def own_out(c):
        par = lax.rem(c, 2)
        return pltpu.make_async_copy(k_buf.at[par], own.at[:, piece_cols(c)], out_sem.at[par])

    def part_out(rel, c):
        par = lax.rem(c, 2)
        return pltpu.make_async_copy(o_buf.at[par], (part1, part2, part3)[rel - 1].at[:, piece_cols(c)], out_sem.at[par])

    def wait_out(i, c):
        rel = _relation(me, top_block - i)

        @pl.when(rel == 0)
        def _():
            own_out(c).wait()

        @pl.when(rel != 0)
        def _():
            part_out(1, c).wait()

    def piece_load(i, c):
        @pl.when(c >= 2)
        def _():
            wait_out(i, c)

        @pl.when((c < 2) & (i > 0))
        def _():
            wait_out(i - 1, c)

        @pl.when(lax.rem(c, 2) == 0)
        def _():
            send_copy(i, c // 2).wait_recv()
        for cp in piece_loads(i, c):
            cp.start()

    def piece_sum(i, c):
        par = lax.rem(c, 2)
        rel = _relation(me, top_block - i)
        for cp in piece_loads(i, c):
            cp.wait()

        @pl.when(rel == 0)
        def _():
            k_buf[par] = k_buf[par] + s_buf[par]
            own_out(c).start()

        @pl.when(rel != 0)
        def _():
            o_buf[par] = (k_buf[par] + s_buf[par]).astype(BF16)
            for other in range(1, 4):
                @pl.when(rel == other)
                def _(other=other):
                    part_out(other, c).start()

    g_in_copy().start()
    _start_weights(me, sources, buffers, w_sem, top_block, 0)
    x_copy(0).start()
    x_copy(1).start()
    for step in range(RING - 2):
        u_copy(step).start()
    _sibling_barrier(me, core)
    g_in_copy().wait()
    x_copy(0).wait()
    x_t[0] = x_buf[0].T
    g_t[0] = act[pl.ds(0, TILE), :].T
    for cp in _weight_loads(sources, buffers, w_sem, top_block, 0, True):
        cp.wait()
    q_buf[0] = _dot_t(act[pl.ds(0, TILE), :], w2_buf[0, pl.ds(0, CHUNK), :])

    @pl.loop(0, n_blocks * tiles)
    def _(bt):
        i = bt // tiles
        tile = lax.rem(bt, tiles)
        blk = top_block - i
        par = lax.rem(i, 2)
        t_par = lax.rem(bt, 2)
        rows = _tile_rows(tile)
        next_rows = _tile_rows(lax.rem(tile + 1, tiles))

        @pl.when((tile == 1) & (i + 1 < n_blocks))
        def _():
            _start_weights(me, sources, buffers, w_sem, blk - 1, 1 - par)

        @pl.when(bt + 1 < n_blocks * tiles)
        def _():
            x_copy(bt + 1).wait()

        @pl.when(bt + 2 < n_blocks * tiles)
        def _():
            x_copy(bt + 2).start()

        @pl.when((i > 0) & (tile >= 2))
        def _():
            piece_sum(i - 1, 2 * tile - 4)
            piece_sum(i - 1, 2 * tile - 3)

        @pl.when((i > 0) & (tile >= 1) & (tile < tiles - 1))
        def _():
            piece_load(i - 1, 2 * tile - 2)
            piece_load(i - 1, 2 * tile - 1)

        acc[...] = act[rows, :].astype(F32)

        def chunk_prep(f, step):
            @pl.when(step + RING - 2 < total)
            def _():
                u_copy(step + RING - 2).start()
            u_copy(step).wait()

            @pl.when((tile == 0) & (i > 0))
            def _():
                for cp in local_copies(i - 1, f):
                    cp.wait()
                send_copy(i - 1, f).start()

            @pl.when(tile == 0)
            def _():
                dw[0, :, cols_of(f)] = jnp.zeros((d_model, CHUNK), F32)
                dw[1, :, cols_of(f)] = jnp.zeros((d_model, CHUNK), F32)

        def chunk_main(f, step, q_par, next_g, next_w2):
            cols = cols_of(f)
            q_buf[1 - q_par] = _dot_t(next_g, next_w2)
            a, slope = _gelu_grad(u_buf[lax.rem(step, RING)])
            r = (q_buf[q_par] * slope).astype(BF16)
            dw[0, :, cols] += _dot(x_t[t_par], r)
            dw[1, :, cols] += _dot(g_t[t_par], a.astype(BF16))
            acc[...] += _dot_t(r, w1_buf[par, :, cols])

        @pl.loop(0, n_chunk // 2)
        def _(pair):
            f0 = pair * 2
            step = bt * n_chunk + f0
            last = f0 + 2 == n_chunk
            end_block = last & (tile == tiles - 1)
            chunk_prep(f0, step)
            chunk_prep(f0 + 1, step + 1)

            @pl.when(end_block & (i + 1 < n_blocks))
            def _():
                for cp in _weight_loads(sources, buffers, w_sem, blk, 1 - par, True):
                    cp.wait()

            q_rows = _tile_rows(jnp.where(last, lax.rem(tile + 1, tiles), tile))
            next_f = jnp.where(last, 0, f0 + 2)
            next_par = jnp.where(end_block, 1 - par, par)
            third = pl.ds(pl.multiple_of(pair * 256, 256), 256)
            chunk_main(f0, step, 0, act[rows, :], w2_buf[par, cols_of(f0 + 1), :])
            x_t[1 - t_par, third, :] = x_buf[1 - t_par, :, third].T
            g_t[1 - t_par, third, :] = act[next_rows, third].T
            chunk_main(f0 + 1, step + 1, 1, act[q_rows, :], w2_buf[next_par, cols_of(next_f), :])

            @pl.when(tile == tiles - 1)
            def _():
                for f in (f0, f0 + 1):
                    for cp in local_copies(i, f):
                        cp.start()

        act[rows, :] = acc[...].astype(BF16)

    out = pltpu.make_async_copy(act, g_out, g_sem)
    out.start()
    final = n_blocks - 1
    for f in range(n_chunk):
        for cp in local_copies(final, f):
            cp.wait()
        send_copy(final, f).start()
    for c in range(n_piece + 1):
        if c < n_piece:
            piece_load(final, jnp.int32(c))
        if c > 0:
            piece_sum(final, jnp.int32(c - 1))
    for c in (n_piece - 2, n_piece - 1):
        wait_out(final, jnp.int32(c))
    for i in range(n_blocks):
        for f in range(n_chunk):
            send_copy(i, f).wait_send()
    out.wait()


def run_backward(top_block, n_blocks, grad, saved, u_all, weights):
    n_rows, d_model = grad.shape
    d_ff = weights[0].shape[2]
    tiles = n_rows // TILE
    n_chunk = d_ff // CHUNK
    return pl.pallas_call(
        functools.partial(backward_kernel, top_block, n_blocks, tiles),
        name="backward",
        out_shape=[
            jax.ShapeDtypeStruct((n_rows, d_model), BF16),
            jax.ShapeDtypeStruct((n_blocks, 2, d_model, d_ff), F32),
            jax.ShapeDtypeStruct((n_blocks, d_model, d_ff), F32),
            jax.ShapeDtypeStruct((d_model, d_ff), F32),
        ] + [jax.ShapeDtypeStruct((d_model, d_ff), BF16)] * 3,
        in_specs=[ANY] * 7,
        out_specs=[ANY] * 7,
        scratch_shapes=[
            pltpu.VMEM((n_rows, d_model), BF16),
            pltpu.VMEM((2, d_model, d_ff), BF16),
            pltpu.VMEM((2, d_ff, d_model), BF16),
            pltpu.VMEM((2, d_model, d_ff), F32),
            pltpu.VMEM((RING, TILE, CHUNK), F32),
            pltpu.VMEM((2, TILE, d_model), BF16),
            pltpu.VMEM((2, d_model, TILE), BF16),
            pltpu.VMEM((2, d_model, TILE), BF16),
            pltpu.VMEM((TILE, d_model), F32),
            pltpu.VMEM((2, TILE, CHUNK), F32),
            pltpu.VMEM((2, d_model, PIECE), F32),
            pltpu.VMEM((2, d_model, PIECE), F32),
            pltpu.VMEM((2, d_model, PIECE), BF16),
            pltpu.SemaphoreType.DMA(()),
            pltpu.SemaphoreType.DMA((2, 2)),
            pltpu.SemaphoreType.DMA((RING,)),
            pltpu.SemaphoreType.DMA((2,)),
            pltpu.SemaphoreType.DMA((n_chunk, 2)),
            pltpu.SemaphoreType.DMA((n_blocks, n_chunk)),
            pltpu.SemaphoreType.DMA((n_blocks, n_chunk)),
            pltpu.SemaphoreType.DMA((2, 2)),
            pltpu.SemaphoreType.DMA((2,)),
        ],
        compiler_params=pltpu.CompilerParams(collective_id=1, has_side_effects=True, vmem_limit_bytes=67043328),
        cost_estimate=pl.CostEstimate(flops=8 * n_blocks * n_rows * d_model * d_ff, bytes_accessed=400 * 2**20, transcendentals=0),
    )(grad, saved, u_all, *weights)


def chain_kernel(top_block, tiles, g_hbm, u_hbm, w1_loc, w2_loc, wg1, wg2, g_all, r_all, a_all,
                 act, w1_buf, w2_buf, u_buf, r_buf, a_buf, acc, q_buf, g_sem, w_sem, u_sem, r_sem, a_sem, s_sem):
    me = lax.axis_index("stage")
    d_ff = u_buf.shape[2]
    n_blocks = top_block + 1
    sources, buffers = (w1_loc, w2_loc, wg1, wg2), (w1_buf, w2_buf)
    steps = n_blocks * tiles

    def u_copy(bt):
        par = lax.rem(bt, 2)
        return pltpu.make_async_copy(u_hbm.at[top_block - bt // tiles, _tile_rows(lax.rem(bt, tiles)), :], u_buf.at[par], u_sem.at[par])

    def out_copies(bt):
        par = lax.rem(bt, 2)
        blk, rows = top_block - bt // tiles, _tile_rows(lax.rem(bt, tiles))
        return [pltpu.make_async_copy(r_buf.at[par], r_all.at[blk, rows, :], r_sem.at[par]),
                pltpu.make_async_copy(a_buf.at[par], a_all.at[blk, rows, :], a_sem.at[par])]

    def g_save(bt):
        rows = _tile_rows(lax.rem(bt, tiles))
        return pltpu.make_async_copy(act.at[rows, :], g_all.at[top_block - bt // tiles, rows, :], s_sem)

    g_in = pltpu.make_async_copy(g_hbm, act, g_sem)
    g_in.start()
    _start_weights(me, sources, buffers, w_sem, top_block, 0)
    u_copy(0).start()
    g_in.wait()

    @pl.loop(0, steps)
    def _(bt):
        i = bt // tiles
        tile = lax.rem(bt, tiles)
        blk = top_block - i
        par = lax.rem(i, 2)
        b_par = lax.rem(bt, 2)
        rows = _tile_rows(tile)

        @pl.when(tile == 0)
        def _():
            for cp in _weight_loads(sources, buffers, w_sem, blk, par, True):
                cp.wait()

            @pl.when(i + 1 < n_blocks)
            def _():
                _start_weights(me, sources, buffers, w_sem, blk - 1, 1 - par)

        @pl.when(bt + 1 < steps)
        def _():
            u_copy(bt + 1).start()

        g_save(bt).start()
        u_copy(bt).wait()

        @pl.when(bt >= 2)
        def _():
            for cp in out_copies(bt - 2):
                cp.wait()

        def body(with_input_grad):
            n_chunk = d_ff // CHUNK
            q_buf[0] = _dot_t(act[rows, :], w2_buf[par, :CHUNK, :])
            for f in range(n_chunk):
                cols = slice(f * CHUNK, (f + 1) * CHUNK)
                if f + 1 < n_chunk:
                    q_buf[(f + 1) % 2] = _dot_t(act[rows, :], w2_buf[par, (f + 1) * CHUNK:(f + 2) * CHUNK, :])
                a, slope = _gelu_grad(u_buf[b_par, :, cols])
                r = (q_buf[f % 2] * slope).astype(BF16)
                a_buf[b_par, :, cols] = a.astype(BF16)
                r_buf[b_par, :, cols] = r
                if with_input_grad:
                    part = _dot_t(r, w1_buf[par, :, cols])
                    if f == 0:
                        acc[...] = part
                    else:
                        acc[...] += part

        @pl.when(blk > 0)
        def _():
            body(True)

        @pl.when(blk == 0)
        def _():
            body(False)

        for cp in out_copies(bt):
            cp.start()
        g_save(bt).wait()

        @pl.when(blk > 0)
        def _():
            act[rows, :] = (act[rows, :].astype(F32) + acc[...]).astype(BF16)

    for bt in (steps - 2, steps - 1):
        for cp in out_copies(jnp.int32(bt)):
            cp.wait()


def run_chain(top_block, grad, u_all, weights):
    n_rows, d_model = grad.shape
    d_ff = weights[0].shape[2]
    tiles = n_rows // TILE
    n_blocks = top_block + 1
    return pl.pallas_call(
        functools.partial(chain_kernel, top_block, tiles),
        name="chain",
        out_shape=[
            jax.ShapeDtypeStruct((n_blocks, n_rows, d_model), BF16),
            jax.ShapeDtypeStruct((n_blocks, n_rows, d_ff), BF16),
            jax.ShapeDtypeStruct((n_blocks, n_rows, d_ff), BF16),
        ],
        in_specs=[ANY] * 6,
        out_specs=[ANY] * 3,
        scratch_shapes=[
            pltpu.VMEM((n_rows, d_model), BF16),
            pltpu.VMEM((2, d_model, d_ff), BF16),
            pltpu.VMEM((2, d_ff, d_model), BF16),
            pltpu.VMEM((2, TILE, d_ff), F32),
            pltpu.VMEM((2, TILE, d_ff), BF16),
            pltpu.VMEM((2, TILE, d_ff), BF16),
            pltpu.VMEM((TILE, d_model), F32),
            pltpu.VMEM((2, TILE, CHUNK), F32),
            pltpu.SemaphoreType.DMA(()),
            pltpu.SemaphoreType.DMA((2, 2)),
            pltpu.SemaphoreType.DMA((2,)),
            pltpu.SemaphoreType.DMA((2,)),
            pltpu.SemaphoreType.DMA((2,)),
            pltpu.SemaphoreType.DMA(()),
        ],
        compiler_params=pltpu.CompilerParams(vmem_limit_bytes=62 * 2**20),
        cost_estimate=pl.CostEstimate(flops=4 * n_blocks * n_rows * d_model * d_ff, bytes_accessed=400 * 2**20, transcendentals=0),
    )(grad, u_all, *weights)


DW_ROWS = 1024


def weight_grad_kernel(first_col, saved, g_all, r_all, a_all, own, part1, part2, part3,
                       x_buf, g_buf, r_buf, a_buf, dw, sib, o_buf, in_sem, send_sem, recv_sem, out_sem):
    me = lax.axis_index("stage")
    core = lax.axis_index("data")
    width = dw.shape[3]
    row_steps = saved.shape[1] // DW_ROWS
    steps = 4 * row_steps
    cols = pl.ds(first_col, width)

    def owner_at(n):
        return jnp.where(n == 0, 3, jnp.where(n == 3, 0, n))

    def block_at(n):
        rel = owner_at(n)
        bit0 = lax.rem(lax.rem(me, 2) + lax.rem(rel, 2), 2)
        bit1 = lax.rem(me // 2 + rel // 2, 2)
        return bit0 + 2 * bit1

    def loads(step):
        par = lax.rem(step, 2)
        blk = block_at(step // row_steps)
        rows = pl.ds(pl.multiple_of(lax.rem(step, row_steps) * DW_ROWS, DW_ROWS), DW_ROWS)
        return [pltpu.make_async_copy(saved.at[blk, rows, :], x_buf.at[par], in_sem.at[par, 0]),
                pltpu.make_async_copy(g_all.at[blk, rows, :], g_buf.at[par], in_sem.at[par, 1]),
                pltpu.make_async_copy(r_all.at[blk, rows, cols], r_buf.at[par], in_sem.at[par, 2]),
                pltpu.make_async_copy(a_all.at[blk, rows, cols], a_buf.at[par], in_sem.at[par, 3])]

    def send_copy(n):
        par = lax.rem(n, 2)
        return pltpu.make_async_remote_copy(
            src_ref=dw.at[par, 1 - core], dst_ref=sib.at[n], send_sem=send_sem.at[par], recv_sem=recv_sem.at[n],
            device_id=(me, 1 - core), device_id_type=MESH)

    def part_copy(which):
        return pltpu.make_async_copy(o_buf, (part3, part1, part2)[which], out_sem)

    for cp in loads(0):
        cp.start()
    _sibling_barrier(me, core)

    @pl.loop(0, steps)
    def _(step):
        n = step // row_steps
        k = lax.rem(step, row_steps)
        par = lax.rem(step, 2)
        d_par = lax.rem(n, 2)

        @pl.when(step + 1 < steps)
        def _():
            for cp in loads(step + 1):
                cp.start()

        @pl.when((k == 0) & (n >= 2))
        def _():
            send_copy(n).wait_send()
        for which in range(3):
            @pl.when((k == row_steps - 1) & (n == which + 1))
            def _(which=which):
                if which > 0:
                    part_copy(which - 1).wait()
                send_copy(jnp.int32(which)).wait_recv()
                o_buf[...] = (dw[which % 2, core] + sib[which]).astype(BF16)
                part_copy(which).start()
        for cp in loads(step):
            cp.wait()
        x_t = x_buf[par].T
        g_t = g_buf[par].T
        first = k == 0
        d1 = _dot(x_t, r_buf[par])
        d2 = _dot(g_t, a_buf[par])
        dw[d_par, 0] = jnp.where(first, 0.0, dw[d_par, 0]) + d1
        dw[d_par, 1] = jnp.where(first, 0.0, dw[d_par, 1]) + d2

        @pl.when(k == row_steps - 1)
        def _():
            send_copy(n).start()

    part_copy(2).wait()
    last = jnp.int32(3)
    send_copy(last).wait_recv()
    sib[3] = dw[1, core] + sib[3]
    done = pltpu.make_async_copy(sib.at[3], own, out_sem)
    done.start()
    done.wait()
    for n in (2, 3):
        send_copy(jnp.int32(n)).wait_send()


def run_weight_grad(first_col, width, ident, saved, g_all, r_all, a_all):
    n_rows, d_model = saved.shape[1:]
    return pl.pallas_call(
        functools.partial(weight_grad_kernel, first_col),
        name=f"weight_grad_{first_col}",
        out_shape=[jax.ShapeDtypeStruct((d_model, width), F32)] + [jax.ShapeDtypeStruct((d_model, width), BF16)] * 3,
        in_specs=[ANY] * 4,
        out_specs=[ANY] * 4,
        scratch_shapes=[
            pltpu.VMEM((2, DW_ROWS, d_model), BF16),
            pltpu.VMEM((2, DW_ROWS, d_model), BF16),
            pltpu.VMEM((2, DW_ROWS, width), BF16),
            pltpu.VMEM((2, DW_ROWS, width), BF16),
            pltpu.VMEM((2, 2, d_model, width), F32),
            pltpu.VMEM((4, d_model, width), F32),
            pltpu.VMEM((d_model, width), BF16),
            pltpu.SemaphoreType.DMA((2, 4)),
            pltpu.SemaphoreType.DMA((2,)),
            pltpu.SemaphoreType.DMA((4,)),
            pltpu.SemaphoreType.DMA(()),
        ],
        compiler_params=pltpu.CompilerParams(collective_id=ident, has_side_effects=True, vmem_limit_bytes=62 * 2**20),
        cost_estimate=pl.CostEstimate(flops=16 * n_rows * d_model * width, bytes_accessed=100 * 2**20, transcendentals=0),
    )(saved, g_all, r_all, a_all)


COMBINE_ROWS = 64


def combine_kernel(tau_clip, n_groups, *refs):
    groups = [refs[4 * g:4 * g + 4] for g in range(n_groups)]
    loss, total, clip_out, loss_out, mine, gathered, send_sem, recv_sem = refs[4 * n_groups:]
    step = pl.program_id(0)
    here = lax.axis_index("stage") * 2 + lax.axis_index("data")
    n_dev = gathered.shape[0]
    barrier = pltpu.get_barrier_semaphore()

    @pl.when(step == 0)
    def _():
        for k in range(1, n_dev):
            other = lax.rem(here + k, n_dev)
            pl.semaphore_signal(barrier, inc=1, device_id=(other // 2, lax.rem(other, 2)), device_id_type=MESH)
        mine[0] = jnp.zeros((8, 128), F32)
        mine[1] = loss[...]

    first = 0
    squares = mine[0]
    for g, (own, got1, got2, got3) in enumerate(groups):
        width = own.shape[1]
        val = (own[...] + got1[...].astype(F32)) + (got2[...].astype(F32) + got3[...].astype(F32))
        if g == 0:
            total[1] = val
        else:
            total[0, :, first:first + width] = val
            first += width
        part = jnp.sum((val * val).reshape(COMBINE_ROWS // 8, 8, width), axis=0)
        for j in range(width // 128):
            squares = squares + part[:, j * 128:(j + 1) * 128]
    mine[0] = squares

    def copy(k, slot):
        other = lax.rem(here + k, n_dev)
        return pltpu.make_async_remote_copy(
            src_ref=mine, dst_ref=gathered.at[slot], send_sem=send_sem.at[k], recv_sem=recv_sem.at[k],
            device_id=(other // 2, lax.rem(other, 2)), device_id_type=MESH)

    @pl.when(step == pl.num_programs(0) - 1)
    def _():
        gathered[here] = mine[...]
        pl.semaphore_wait(barrier, n_dev - 1)
        for k in range(1, n_dev):
            copy(k, here).start()
        for k in range(1, n_dev):
            copy(k, lax.rem(here + n_dev - k, n_dev)).wait_recv()
        sums = jnp.sum(gathered[...], axis=0)
        squared = jnp.sum(jnp.sum(sums[0], axis=0, keepdims=True), axis=1, keepdims=True)
        lost = jnp.sum(jnp.sum(sums[1], axis=0, keepdims=True), axis=1, keepdims=True)
        norm = jnp.sqrt(jnp.broadcast_to(squared, (8, 128)))
        clip_out[...] = jnp.minimum(1.0, tau_clip / norm)
        loss_out[...] = jnp.broadcast_to(lost, (8, 128))
        for k in range(1, n_dev):
            copy(k, here).wait_send()


def run_combine(tau_clip, groups, loss):
    d_model, d_ff = groups[0][0].shape
    specs = [pl.BlockSpec((COMBINE_ROWS, val.shape[1]), lambda i: (i, 0)) for group in groups for val in group]
    lanes = pl.BlockSpec((8, 128), lambda i: (0, 0))
    return pl.pallas_call(
        functools.partial(combine_kernel, tau_clip, len(groups)),
        name="combine",
        grid=(d_model // COMBINE_ROWS,),
        out_shape=[jax.ShapeDtypeStruct((2, d_model, d_ff), F32)] + [jax.ShapeDtypeStruct((8, 128), F32)] * 2,
        in_specs=specs + [lanes],
        out_specs=[pl.BlockSpec((2, COMBINE_ROWS, d_ff), lambda i: (0, i, 0)), lanes, lanes],
        scratch_shapes=[
            pltpu.VMEM((2, 8, 128), F32),
            pltpu.VMEM((8, 2, 8, 128), F32),
            pltpu.SemaphoreType.DMA((8,)),
            pltpu.SemaphoreType.DMA((8,)),
        ],
        compiler_params=pltpu.CompilerParams(collective_id=7, has_side_effects=True, dimension_semantics=("arbitrary",), vmem_limit_bytes=40 * 2**20),
    )(*[val for group in groups for val in group], loss)


FLAT_ROWS = 1536


def update_kernel(learn_rate, grad, clip, w_old, m_old, v_old, w_new, m_new, v_new, w1_half, w2_half,
                  g_one, g_two, flat, wide, n_one, n_two, g_sem, n_sem):
    step = pl.program_id(0)
    core = lax.axis_index("data")
    d_model, d_ff = grad.shape[1], grad.shape[2]
    rows1, rows2 = FLAT_ROWS * 128 // d_ff, FLAT_ROWS * 128 // d_model
    chunks = d_model // rows1
    steps = 2 * chunks

    def g_copy(n, of_core):
        par = lax.rem(n, 2)
        half, chunk = n // chunks, lax.rem(n, chunks)
        if of_core == 0:
            return pltpu.make_async_copy(grad.at[half, pl.ds(pl.multiple_of(chunk * rows1, rows1), rows1), :], g_one.at[par], g_sem.at[par])
        return pltpu.make_async_copy(grad.at[half, :, pl.ds(pl.multiple_of(chunk * rows2, rows2), rows2)], g_two.at[par], g_sem.at[par])

    def n_copy(n, of_core):
        par = lax.rem(n, 2)
        half, chunk = n // chunks, lax.rem(n, chunks)
        if of_core == 0:
            return pltpu.make_async_copy(n_one.at[par], w1_half.at[half, pl.ds(pl.multiple_of(chunk * rows1, rows1), rows1), :], n_sem.at[par])
        return pltpu.make_async_copy(n_two.at[par], w2_half.at[half, pl.ds(pl.multiple_of(chunk * rows2, rows2), rows2), :], n_sem.at[par])

    par = lax.rem(step, 2)
    for of_core in range(2):
        @pl.when(core == of_core)
        def _(of_core=of_core):
            @pl.when(step == 0)
            def _():
                g_copy(step, of_core).start()

            @pl.when(step + 1 < steps)
            def _():
                g_copy(step + 1, of_core).start()
            g_copy(step, of_core).wait()
            if of_core == 0:
                val = g_one[par]
                per_row = d_ff // 128
            else:
                val = g_two[par].T
                per_row = d_model // 128
            for j in range(per_row):
                flat[pl.ds(j, val.shape[0], per_row), :] = val[:, j * 128:(j + 1) * 128]

    grad_clip = jnp.broadcast_to(clip[0:1, :], (FLAT_ROWS, 128)) * flat[...]
    m_val = BETA_ONE * m_old[...] + (1.0 - BETA_ONE) * grad_clip
    v_val = BETA_TWO * v_old[...] + (1.0 - BETA_TWO) * grad_clip * grad_clip
    m_hat = m_val * (1.0 / (1.0 - BETA_ONE ** ADAM_STEP))
    v_hat = v_val * (1.0 / (1.0 - BETA_TWO ** ADAM_STEP))
    w_val = w_old[...]
    w_val = w_val - learn_rate * (m_hat / (jnp.sqrt(v_hat) + ADAM_EPS) + WEIGHT_DECAY * w_val)
    m_new[...] = m_val
    v_new[...] = v_val
    w_new[...] = w_val
    wide[...] = w_val

    for of_core in range(2):
        @pl.when(core == of_core)
        def _(of_core=of_core):
            @pl.when(step >= 2)
            def _():
                n_copy(step - 2, of_core).wait()
            buf, per_row = (n_one, d_ff // 128) if of_core == 0 else (n_two, d_model // 128)
            for j in range(per_row):
                buf[par, :, j * 128:(j + 1) * 128] = wide[pl.ds(j, buf.shape[1], per_row), :].astype(BF16)
            n_copy(step, of_core).start()

            @pl.when(step == steps - 1)
            def _():
                n_copy(step - 1, of_core).wait()
                n_copy(step, of_core).wait()


def run_update(learn_rate, grad, clip, w_old, m_old, v_old):
    _, d_model, d_ff = grad.shape
    rows1, rows2 = FLAT_ROWS * 128 // d_ff, FLAT_ROWS * 128 // d_model
    steps = w_old.shape[0] // FLAT_ROWS
    flat_spec = pl.BlockSpec((FLAT_ROWS, 128), lambda i: (i, 0))
    flat_shape = jax.ShapeDtypeStruct(w_old.shape, F32)
    return pl.pallas_call(
        functools.partial(update_kernel, learn_rate),
        name="update",
        grid=(steps,),
        out_shape=[flat_shape] * 3 + [jax.ShapeDtypeStruct((2, d_model, d_ff), BF16), jax.ShapeDtypeStruct((2, d_ff, d_model), BF16)],
        in_specs=[ANY, pl.BlockSpec((8, 128), lambda i: (0, 0))] + [flat_spec] * 3,
        out_specs=[flat_spec] * 3 + [ANY, ANY],
        scratch_shapes=[
            pltpu.VMEM((2, rows1, d_ff), F32),
            pltpu.VMEM((2, d_model, rows2), F32),
            pltpu.VMEM((FLAT_ROWS, 128), F32),
            pltpu.VMEM((FLAT_ROWS, 128), F32),
            pltpu.VMEM((2, rows1, d_ff), BF16),
            pltpu.VMEM((2, rows2, d_model), BF16),
            pltpu.SemaphoreType.DMA((2,)),
            pltpu.SemaphoreType.DMA((2,)),
        ],
        compiler_params=pltpu.CompilerParams(dimension_semantics=("arbitrary",), vmem_limit_bytes=40 * 2**20),
        cost_estimate=pl.CostEstimate(flops=10**9, bytes_accessed=150 * 2**20, transcendentals=0),
    )(grad, clip, w_old, m_old, v_old)


def merge_kernel(w1_half, w2_half, w1_got, w2_got, w1_new, w2_new, buf1, buf2, in_sem, out_sem):
    del w1_half, w2_half
    core = lax.axis_index("data")
    for of_core, got, new, buf in ((1, w1_got, w1_new, buf1), (0, w2_got, w2_new, buf2)):
        parts = [(half, slot) for half in range(2) for slot in range(MERGE_PARTS)]
        rows = buf.shape[1]

        @pl.when(core == of_core)
        def _(parts=parts, rows=rows, got=got, new=new, buf=buf):
            ins, outs = [], []
            for n, (half, slot) in enumerate(parts):
                where = pl.ds(slot * rows, rows)
                ins.append(pltpu.make_async_copy(got.at[half, where, :], buf.at[n], in_sem.at[n]))
                outs.append(pltpu.make_async_copy(buf.at[n], new.at[half, where, :], out_sem.at[n]))
            for cp in ins:
                cp.start()
            for cp_in, cp_out in zip(ins, outs):
                cp_in.wait()
                cp_out.start()
            for cp in outs:
                cp.wait()


MERGE_PARTS = 4


def run_merge(w1_half, w2_half, w1_got, w2_got):
    _, d_model, d_ff = w1_half.shape
    n = 2 * MERGE_PARTS
    return pl.pallas_call(
        merge_kernel,
        name="merge",
        out_shape=[jax.ShapeDtypeStruct(w1_half.shape, BF16), jax.ShapeDtypeStruct(w2_half.shape, BF16)],
        in_specs=[ANY] * 4,
        out_specs=[ANY] * 2,
        input_output_aliases={0: 0, 1: 1},
        scratch_shapes=[
            pltpu.VMEM((n, d_model // MERGE_PARTS, d_ff), BF16),
            pltpu.VMEM((n, d_ff // MERGE_PARTS, d_model), BF16),
            pltpu.SemaphoreType.DMA((n,)),
            pltpu.SemaphoreType.DMA((n,)),
        ],
        compiler_params=pltpu.CompilerParams(vmem_limit_bytes=40 * 2**20),
    )(w1_half, w2_half, w1_got, w2_got)


GROUPS = ((0, 1024), (1024, 1024), (2048, 512), (2560, 512))


def solution(mesh):
    n_stage = mesh.shape["stage"]
    n_data = mesh.shape["data"]
    axes = ("stage", "data")

    def device(stage, core):
        return stage * n_data + core

    def from_core(core):
        return [(device(s, core), device(s, 1 - core)) for s in range(n_stage)]

    def across(flip):
        return [(device(s, c), device(s ^ flip, c)) for s in range(n_stage) for c in range(n_data)]

    def exchange(parts):
        return [lax.ppermute(part, axes, across(flip)) for flip, part in enumerate(parts, start=1)]

    def device_step(x_loc, t_loc, w1_loc, w2_loc, wm_loc, m_loc, v_loc):
        n_micro, n_tok, d_model = x_loc.shape
        d_ff = w1_loc.shape[4]
        n_tokens = n_micro * n_tok * n_data
        n_blocks = 2 * n_stage
        n_rows = n_micro * n_tok // n_stage
        tau_clip = 0.3 * d_model * math.sqrt(n_blocks * (3.0 / n_tokens + 0.008))
        learn_rate = 0.1 / math.sqrt(4.0 * d_model * n_blocks)
        w1 = w1_loc.reshape(2, d_model, d_ff)
        w2 = w2_loc.reshape(2, d_ff, d_model)
        flat_rows = (n_micro * n_tok, d_model)
        wg1, wg2, saved, u_all, seed, loss_acc = run_forward(n_tokens, x_loc.reshape(flat_rows), t_loc.reshape(flat_rows), w1, w2, n_rows)
        weights = (w1, w2, wg1, wg2)
        grad, _, _, own_hi, *parts_hi = run_backward(7, 4, seed, saved, u_all, weights)
        groups = [[own_hi] + exchange(parts_hi)]
        g_all, r_all, a_all = run_chain(3, grad, u_all, weights)
        for ident, (first, width) in enumerate(GROUPS):
            own, *parts = run_weight_grad(first, width, 2 + ident, saved, g_all, r_all, a_all)
            groups.append([own] + exchange(parts))
        total, clip, loss_all = run_combine(tau_clip, groups, loss_acc)
        flat = [val.reshape(-1, 128) for val in (wm_loc, m_loc, v_loc)]
        w_new, m_new, v_new, w1_half, w2_half = run_update(learn_rate, total, clip, *flat)
        w1_got = lax.ppermute(w1_half, axes, from_core(0))
        w2_got = lax.ppermute(w2_half, axes, from_core(1))
        w1_new, w2_new = run_merge(w1_half, w2_half, w1_got, w2_got)
        mean_loss = loss_all[0, 0] / n_tokens
        return w1_new.reshape(w1_loc.shape), w2_new.reshape(w2_loc.shape), w_new.reshape(wm_loc.shape), m_new.reshape(wm_loc.shape), v_new.reshape(wm_loc.shape), mean_loss

    act_spec = P(None, "data", None)
    flat_spec = P("stage", None, None, "data")
    return jax.shard_map(device_step, mesh=mesh, in_specs=(act_spec, act_spec, P("stage"), P("stage"), flat_spec, flat_spec, flat_spec), out_specs=(P("stage"), P("stage"), flat_spec, flat_spec, flat_spec, P()), check_vma=False)
```

```python
import functools
import math
import jax
import jax.numpy as jnp
from jax import lax
from jax.experimental import pallas as pl
from jax.experimental.pallas import tpu as pltpu
from jax.sharding import PartitionSpec as P


BETA_ONE = 0.9
BETA_TWO = 0.999
ADAM_EPS = 1e-8
WEIGHT_DECAY = 0.1
ADAM_STEP = 1000
GELU_A = math.sqrt(2.0 / math.pi)
GELU_B = GELU_A * 0.044715
MESH = pl.DeviceIdType.MESH
ANY = pl.BlockSpec(memory_space=pl.ANY)
F32 = jnp.float32
BF16 = jnp.bfloat16

TILE = 512
PATH_PIECES = 4


def _dot_t(lhs, rhs):
    return lax.dot_general(lhs, rhs, (((1,), (1,)), ((), ())), preferred_element_type=F32)


def _dot(lhs, rhs):
    return jnp.dot(lhs, rhs, preferred_element_type=F32)


SEND_SLOT = (-45, -30, -28, -20)
HOP_SLOT = {1: (-27, -20, -18, -14), 2: (-18, -14, -8, -6), 3: (-12, -9, -2, -2)}
LOAD_SLOT = -1


def forward_kernel(n_blocks, tiles, n_tokens, x_hbm, t_hbm, w1_loc, w2_loc, wg1, wg2, saved, u_out, seed, loss,
                   act, w1_buf, w2_buf, u_buf, acc, t_buf, s_buf,
                   x_sem, act_sem, u_sem, w_sem, t_sem, s_sem, ici_send, ici_recv, d2d_send, d2d_recv):
    me = lax.axis_index("stage")
    core = lax.axis_index("data")
    d_model, d_ff = w1_loc.shape[1], w1_loc.shape[2]
    n_rows = act.shape[0]
    n_piece = 4 * PATH_PIECES
    rows1, rows2 = d_model // n_piece, d_ff // n_piece

    def peer(flip):
        bit0, bit1 = lax.rem(me, 2), me // 2
        return (1 - bit0 + 2 * bit1) if flip == 1 else (bit0 + 2 * (1 - bit1))

    def rel_of(blk):
        own = lax.rem(blk, 4)
        a0, a1, b0, b1 = lax.rem(me, 2), me // 2, lax.rem(own, 2), own // 2
        return (a0 + b0 - 2 * a0 * b0) + 2 * (a1 + b1 - 2 * a1 * b1)

    def piece(j, path, of_core):
        return j * 4 + path * 2 + of_core

    def views(blk, idx):
        return (wg1.at[blk, pl.ds(pl.multiple_of(idx * rows1, 16), rows1), :],
                wg2.at[blk, pl.ds(pl.multiple_of(idx * rows2, 64), rows2), :])

    def local_views(blk, idx):
        half = blk // 4
        return (w1_loc.at[half, pl.ds(pl.multiple_of(idx * rows1, 16), rows1), :],
                w2_loc.at[half, pl.ds(pl.multiple_of(idx * rows2, 64), rows2), :])

    def ici_copies(blk, path, j, sources, flip):
        idx = piece(j, path, core)
        slot = path * PATH_PIECES + j
        return [pltpu.make_async_remote_copy(
            src_ref=src, dst_ref=dst, send_sem=ici_send.at[blk, slot, m], recv_sem=ici_recv.at[blk, slot, m],
            device_id=(peer(flip), core), device_id_type=MESH)
            for m, (src, dst) in enumerate(zip(sources, views(blk, idx)))]

    def d2d_copies(blk, path, j, of_core):
        idx = piece(j, path, of_core)
        slot = path * PATH_PIECES + j
        return [pltpu.make_async_remote_copy(
            src_ref=ref, dst_ref=ref, send_sem=d2d_send.at[blk, slot, m], recv_sem=d2d_recv.at[blk, slot, m],
            device_id=(me, 1 - core), device_id_type=MESH) for m, ref in enumerate(views(blk, idx))]

    def first_flip(path):
        return 1 if path == 0 else 2

    def own_send(blk, j):
        @pl.when(rel_of(blk) == 0)
        def _():
            for path in range(2):
                for cp in ici_copies(blk, path, j, local_views(blk, piece(j, path, core)), first_flip(path)):
                    cp.start()

    def hop_event(blk, hop, j):
        rel = rel_of(blk)
        for path in range(2):
            at_rel = {1: (1, 2), 2: (3, 3), 3: (2, 1)}[hop][path]

            @pl.when(rel == at_rel)
            def _(path=path):
                flip = first_flip(path)
                if hop == 1:
                    flip = 3 - flip
                copies = ici_copies(blk, path, j, views(blk, piece(j, path, core)), flip)
                for cp in copies:
                    cp.wait_recv()
                if hop < 3:
                    for cp in copies:
                        cp.start()
                for cp in d2d_copies(blk, path, j, core):
                    cp.start()

    def weight_loads(blk, par, is_own):
        half = blk // 4
        src1, src2 = (w1_loc.at[half], w2_loc.at[half]) if is_own else (wg1.at[blk], wg2.at[blk])
        return [pltpu.make_async_copy(src1, w1_buf.at[par], w_sem.at[par, 0]),
                pltpu.make_async_copy(src2, w2_buf.at[par], w_sem.at[par, 1])]

    def load_event(blk):
        rel = rel_of(blk)
        par = lax.rem(blk, 2)

        @pl.when(rel == 0)
        def _():
            for cp in weight_loads(blk, par, True):
                cp.start()

        @pl.when(rel != 0)
        def _():
            for path in range(2):
                for j in range(PATH_PIECES):
                    for cp in d2d_copies(blk, path, j, 1 - core):
                        cp.wait_recv()
            for cp in weight_loads(blk, par, False):
                cp.start()

    def x_copy():
        return pltpu.make_async_copy(x_hbm.at[pl.ds(pl.multiple_of(me * n_rows, n_rows), n_rows), :], act, x_sem)

    def act_copy(slot, tile):
        rows = pl.ds(pl.multiple_of(tile * TILE, TILE), TILE)
        return pltpu.make_async_copy(act.at[rows, :], saved.at[slot, rows, :], act_sem.at[tile])

    def t_copy(tile):
        return pltpu.make_async_copy(t_hbm.at[pl.ds(pl.multiple_of(me * n_rows + tile * TILE, TILE), TILE), :], t_buf, t_sem)

    def seed_copy(tile):
        return pltpu.make_async_copy(s_buf, seed.at[pl.ds(pl.multiple_of(tile * TILE, TILE), TILE), :], s_sem)

    def u_copy(blk, tile, par):
        rows = pl.ds(pl.multiple_of(tile * TILE, TILE), TILE)
        return pltpu.make_async_copy(u_buf.at[par], u_out.at[blk, rows, :], u_sem.at[par])

    barrier = pltpu.get_barrier_semaphore()
    for target in ((peer(1), core), (peer(2), core), (me, 1 - core)):
        pl.semaphore_signal(barrier, inc=1, device_id=target, device_id_type=MESH)
    x_copy().start()
    pl.semaphore_wait(barrier, 3)

    events = []
    for hop in (3, 2, 1):
        for j in range(PATH_PIECES):
            events.append((HOP_SLOT[hop][j], functools.partial(lambda blk, hop, j: hop_event(blk, hop, j), hop=hop, j=j)))
    for j in range(PATH_PIECES):
        events.append((SEND_SLOT[j], functools.partial(lambda blk, j: own_send(blk, j), j=j)))
    events.append((LOAD_SLOT, load_event))

    def comm_slot(blk, tile):
        for offset, fn in events:
            residue = offset % tiles
            ahead = (residue - offset) // tiles
            target = blk + ahead

            @pl.when((tile == residue) & (target >= 0) & (target < n_blocks))
            def _(fn=fn, target=target):
                fn(target)

    def compute(blk, tile):
        par = lax.rem(blk, 2)
        u_par = lax.rem(tile, 2)
        rows = pl.ds(pl.multiple_of(tile * TILE, TILE), TILE)

        @pl.when(tile == 0)
        def _():
            for cp in weight_loads(blk, par, True):
                cp.wait()

        @pl.when((blk == 0) & (tile == 0))
        def _():
            x_copy().wait()
            for t in range(tiles):
                act_copy(0, t).start()

        @pl.when((blk > 0) | (tile > 1))
        def _():
            u_copy(blk, tile, u_par).wait()

        @pl.when(blk == n_blocks - 1)
        def _():
            t_copy(tile).start()

        act_copy(blk, tile).wait()
        x = act[rows, :]
        chunk = 256
        n_chunk = d_ff // chunk
        for f in range(n_chunk):
            cols = slice(f * chunk, (f + 1) * chunk)
            u = _dot(x, w1_buf[par, :, cols])
            u_buf[u_par, :, cols] = u
            inner = u * (GELU_A + GELU_B * (u * u))
            a = (u * (0.5 + 0.5 * jnp.tanh(inner))).astype(BF16)
            part = _dot(a, w2_buf[par, cols, :])
            if f == 0:
                acc[...] = part
            elif f < n_chunk - 1:
                acc[...] += part
            else:
                act[rows, :] = (x.astype(F32) + (acc[...] + part)).astype(BF16)
        u_copy(blk, tile, u_par).start()

        @pl.when(blk < n_blocks - 1)
        def _():
            act_copy(blk + 1, tile).start()

        @pl.when(blk == n_blocks - 1)
        def _():
            t_copy(tile).wait()

            @pl.when(tile > 0)
            def _():
                seed_copy(tile - 1).wait()

            residual = act[rows, :].astype(F32) - t_buf[...].astype(F32)
            s_buf[...] = (residual / n_tokens).astype(BF16)
            squares = jnp.sum((residual * residual).reshape(TILE // 8, 8, residual.shape[1]), axis=0)
            folded = squares[:, :128]
            for j in range(1, residual.shape[1] // 128):
                folded = folded + squares[:, j * 128:(j + 1) * 128]
            loss[...] += 0.5 * folded
            seed_copy(tile).start()

    lead = -(min(SEND_SLOT) // tiles)
    loss[...] = jnp.zeros_like(loss)

    @pl.loop(0, (n_blocks + lead) * tiles)
    def _(step):
        blk = step // tiles - lead
        tile = lax.rem(step, tiles)
        comm_slot(blk, tile)

        @pl.when(blk >= 0)
        def _():
            compute(blk, tile)

    for par in range(2):
        u_copy(0, 0, par).wait()
    seed_copy(0).wait()

    @pl.loop(0, n_blocks)
    def _(blk):
        rel = rel_of(blk)
        for path in range(2):
            last = (2, 1)[path]

            @pl.when(rel != last)
            def _(path=path):
                for j in range(PATH_PIECES):
                    for cp in ici_copies(blk, path, j, views(blk, piece(j, path, core)), 1):
                        cp.wait_send()

        @pl.when(rel != 0)
        def _():
            for path in range(2):
                for j in range(PATH_PIECES):
                    for cp in d2d_copies(blk, path, j, core):
                        cp.wait_send()


def run_forward(n_tokens, x_flat, t_flat, w1_loc, w2_loc, n_rows):
    n_half, d_model, d_ff = w1_loc.shape
    n_blocks = 4 * n_half
    tiles = n_rows // TILE
    slots = 2 * PATH_PIECES
    out_shape = [
        jax.ShapeDtypeStruct((n_blocks, d_model, d_ff), BF16),
        jax.ShapeDtypeStruct((n_blocks, d_ff, d_model), BF16),
        jax.ShapeDtypeStruct((n_blocks, n_rows, d_model), BF16),
        jax.ShapeDtypeStruct((n_blocks, n_rows, d_ff), F32),
        jax.ShapeDtypeStruct((n_rows, d_model), BF16),
        jax.ShapeDtypeStruct((8, 128), F32),
    ]
    return pl.pallas_call(
        functools.partial(forward_kernel, n_blocks, tiles, n_tokens),
        name="forward",
        out_shape=out_shape,
        in_specs=[ANY] * 4,
        out_specs=[ANY] * 5 + [pl.BlockSpec(memory_space=pltpu.VMEM)],
        scratch_shapes=[
            pltpu.VMEM((n_rows, d_model), BF16),
            pltpu.VMEM((2, d_model, d_ff), BF16),
            pltpu.VMEM((2, d_ff, d_model), BF16),
            pltpu.VMEM((2, TILE, d_ff), F32),
            pltpu.VMEM((TILE, d_model), F32),
            pltpu.VMEM((TILE, d_model), BF16),
            pltpu.VMEM((TILE, d_model), BF16),
            pltpu.SemaphoreType.DMA(()),
            pltpu.SemaphoreType.DMA((tiles,)),
            pltpu.SemaphoreType.DMA((2,)),
            pltpu.SemaphoreType.DMA((2, 2)),
            pltpu.SemaphoreType.DMA(()),
            pltpu.SemaphoreType.DMA(()),
            pltpu.SemaphoreType.DMA((n_blocks, slots, 2)),
            pltpu.SemaphoreType.DMA((n_blocks, slots, 2)),
            pltpu.SemaphoreType.DMA((n_blocks, slots, 2)),
            pltpu.SemaphoreType.DMA((n_blocks, slots, 2)),
        ],
        compiler_params=pltpu.CompilerParams(collective_id=0, has_side_effects=True, vmem_limit_bytes=60 * 2**20),
        cost_estimate=pl.CostEstimate(flops=4 * n_blocks * n_rows * d_model * d_ff, bytes_accessed=600 * 2**20, transcendentals=0),
    )(x_flat, t_flat, w1_loc, w2_loc)


RING = 5
CHUNK = 512
PIECE = 256


def _relation(me, blk):
    own = lax.rem(blk, 4)
    a0, a1, b0, b1 = lax.rem(me, 2), me // 2, lax.rem(own, 2), own // 2
    return (a0 + b0 - 2 * a0 * b0) + 2 * (a1 + b1 - 2 * a1 * b1)


def _weight_loads(sources, buffers, sems, blk, par, is_own):
    w1_loc, w2_loc, wg1, wg2 = sources
    half = blk // 4
    src1, src2 = (w1_loc.at[half], w2_loc.at[half]) if is_own else (wg1.at[blk], wg2.at[blk])
    return [pltpu.make_async_copy(src1, buffers[0].at[par], sems.at[par, 0]),
            pltpu.make_async_copy(src2, buffers[1].at[par], sems.at[par, 1])]


def _start_weights(me, sources, buffers, sems, blk, par):
    rel = _relation(me, blk)

    @pl.when(rel == 0)
    def _():
        for cp in _weight_loads(sources, buffers, sems, blk, par, True):
            cp.start()

    @pl.when(rel != 0)
    def _():
        for cp in _weight_loads(sources, buffers, sems, blk, par, False):
            cp.start()


def _tile_rows(tile):
    return pl.ds(pl.multiple_of(tile * TILE, TILE), TILE)


def _sibling_barrier(me, core):
    barrier = pltpu.get_barrier_semaphore()
    pl.semaphore_signal(barrier, inc=1, device_id=(me, 1 - core), device_id_type=MESH)
    pl.semaphore_wait(barrier, 1)


def _gelu_grad(u):
    cube = GELU_B * (u * u)
    th = jnp.tanh(u * (GELU_A + cube))
    cdf = 0.5 + 0.5 * th
    a = u * cdf
    return a, cdf + (a * (3.0 - 3.0 * th)) * (cube + GELU_A / 3.0)


def backward_kernel(top_block, n_blocks, tiles, g_hbm, saved, u_hbm, w1_loc, w2_loc, wg1, wg2, g_out, local, sib, own, part1, part2, part3,
                    act, w1_buf, w2_buf, dw, u_buf, x_buf, x_t, g_t, acc, q_buf, k_buf, s_buf, o_buf,
                    g_sem, w_sem, u_sem, x_sem, keep_sem, send_sem, recv_sem, load_sem, out_sem):
    me = lax.axis_index("stage")
    core = lax.axis_index("data")
    d_model, d_ff = dw.shape[1], dw.shape[2]
    n_chunk = d_ff // CHUNK
    n_piece = d_ff // PIECE
    sources, buffers = (w1_loc, w2_loc, wg1, wg2), (w1_buf, w2_buf)
    total = n_blocks * tiles * n_chunk
    final = n_blocks - 1

    def cols_of(f):
        return pl.ds(pl.multiple_of(f * CHUNK, CHUNK), CHUNK)

    def u_copy(step):
        blk = top_block - step // (tiles * n_chunk)
        tile = lax.rem(step // n_chunk, tiles)
        f = lax.rem(step, n_chunk)
        slot = lax.rem(step, RING)
        return pltpu.make_async_copy(u_hbm.at[blk, _tile_rows(tile), cols_of(f)], u_buf.at[slot], u_sem.at[slot])

    def x_copy(bt):
        par = lax.rem(bt, 2)
        return pltpu.make_async_copy(saved.at[top_block - bt // tiles, _tile_rows(lax.rem(bt, tiles)), :], x_buf.at[par], x_sem.at[par])

    def g_in_copy():
        return pltpu.make_async_copy(g_hbm, act, g_sem)

    def local_copies(i, f):
        return [pltpu.make_async_copy(dw.at[m, :, cols_of(f)], local.at[i, m, :, cols_of(f)], keep_sem.at[f, m]) for m in range(2)]

    def send_copy(i, f, src=None):
        return pltpu.make_async_remote_copy(
            src_ref=local.at[i, 1 - core, :, cols_of(f)] if src is None else src, dst_ref=sib.at[i, :, cols_of(f)],
            send_sem=send_sem.at[i, f], recv_sem=recv_sem.at[i, f], device_id=(me, 1 - core), device_id_type=MESH)

    def piece_cols(c):
        return pl.ds(pl.multiple_of(c * PIECE, PIECE), PIECE)

    def sib_load(i, c):
        par = lax.rem(c, 2)
        return pltpu.make_async_copy(sib.at[i, :, piece_cols(c)], s_buf.at[par], load_sem.at[par, 1])

    def piece_loads(i, c):
        par = lax.rem(c, 2)
        return [pltpu.make_async_copy(local.at[i, core, :, piece_cols(c)], k_buf.at[par], load_sem.at[par, 0]), sib_load(i, c)]

    def own_out(c):
        par = lax.rem(c, 2)
        return pltpu.make_async_copy(k_buf.at[par], own.at[:, piece_cols(c)], out_sem.at[par])

    def part_out(rel, c):
        par = lax.rem(c, 2)
        return pltpu.make_async_copy(o_buf.at[par], (part1, part2, part3)[rel - 1].at[:, piece_cols(c)], out_sem.at[par])

    def wait_out(i, c):
        rel = _relation(me, top_block - i)

        @pl.when(rel == 0)
        def _():
            own_out(c).wait()

        @pl.when(rel != 0)
        def _():
            part_out(1, c).wait()

    def piece_load(i, c):
        @pl.when(c >= 2)
        def _():
            wait_out(i, c)

        @pl.when((c < 2) & (i > 0))
        def _():
            wait_out(i - 1, c)

        @pl.when(lax.rem(c, 2) == 0)
        def _():
            send_copy(i, c // 2).wait_recv()

        for cp in piece_loads(i, c):
            cp.start()

    def piece_sum(i, c):
        par = lax.rem(c, 2)
        rel = _relation(me, top_block - i)
        for cp in piece_loads(i, c):
            cp.wait()

        @pl.when(rel == 0)
        def _():
            k_buf[par] = k_buf[par] + s_buf[par]
            own_out(c).start()

        @pl.when(rel != 0)
        def _():
            o_buf[par] = (k_buf[par] + s_buf[par]).astype(BF16)
            for other in range(1, 4):
                @pl.when(rel == other)
                def _(other=other):
                    part_out(other, c).start()

    g_in_copy().start()
    _start_weights(me, sources, buffers, w_sem, top_block, 0)
    x_copy(0).start()
    x_copy(1).start()
    for step in range(RING - 2):
        u_copy(step).start()
    _sibling_barrier(me, core)
    g_in_copy().wait()
    x_copy(0).wait()
    x_t[0] = x_buf[0].T
    g_t[0] = act[pl.ds(0, TILE), :].T
    for cp in _weight_loads(sources, buffers, w_sem, top_block, 0, True):
        cp.wait()
    q_buf[0] = _dot_t(act[pl.ds(0, TILE), :], w2_buf[0, pl.ds(0, CHUNK), :])

    @pl.loop(0, n_blocks * tiles)
    def _(bt):
        i = bt // tiles
        tile = lax.rem(bt, tiles)
        blk = top_block - i
        par = lax.rem(i, 2)
        t_par = lax.rem(bt, 2)
        rows = _tile_rows(tile)
        next_rows = _tile_rows(lax.rem(tile + 1, tiles))

        @pl.when((tile == 1) & (i + 1 < n_blocks))
        def _():
            _start_weights(me, sources, buffers, w_sem, blk - 1, 1 - par)

        @pl.when(bt + 1 < n_blocks * tiles)
        def _():
            x_copy(bt + 1).wait()

        @pl.when(bt + 2 < n_blocks * tiles)
        def _():
            x_copy(bt + 2).start()

        @pl.when((i > 0) & (tile >= 2))
        def _():
            piece_sum(i - 1, 2 * tile - 4)
            piece_sum(i - 1, 2 * tile - 3)

        @pl.when((i > 0) & (tile >= 1) & (tile < tiles - 1))
        def _():
            piece_load(i - 1, 2 * tile - 2)
            piece_load(i - 1, 2 * tile - 1)

        acc[...] = act[rows, :].astype(F32)

        def chunk_prep(f, step):
            @pl.when(step + RING - 2 < total)
            def _():
                u_copy(step + RING - 2).start()

            u_copy(step).wait()

            @pl.when((tile == 0) & (i > 0))
            def _():
                for cp in local_copies(i - 1, f):
                    cp.wait()
                send_copy(i - 1, f).start()

            @pl.when(tile == 0)
            def _():
                dw[0, :, cols_of(f)] = jnp.zeros((d_model, CHUNK), F32)
                dw[1, :, cols_of(f)] = jnp.zeros((d_model, CHUNK), F32)

        def chunk_main(f, step, q_par, next_g, next_w2):
            cols = cols_of(f)
            q_buf[1 - q_par] = _dot_t(next_g, next_w2)
            a, slope = _gelu_grad(u_buf[lax.rem(step, RING)])
            r = (q_buf[q_par] * slope).astype(BF16)
            dw[0, :, cols] += _dot(x_t[t_par], r)
            dw[1, :, cols] += _dot(g_t[t_par], a.astype(BF16))
            acc[...] += _dot_t(r, w1_buf[par, :, cols])

        @pl.loop(0, n_chunk // 2)
        def _(pair):
            f0 = pair * 2
            step = bt * n_chunk + f0
            last = f0 + 2 == n_chunk
            end_block = last & (tile == tiles - 1)
            chunk_prep(f0, step)
            chunk_prep(f0 + 1, step + 1)

            @pl.when(end_block & (i + 1 < n_blocks))
            def _():
                for cp in _weight_loads(sources, buffers, w_sem, blk, 1 - par, True):
                    cp.wait()

            q_rows = _tile_rows(jnp.where(last, lax.rem(tile + 1, tiles), tile))
            next_f = jnp.where(last, 0, f0 + 2)
            next_par = jnp.where(end_block, 1 - par, par)
            third = pl.ds(pl.multiple_of(pair * 256, 256), 256)
            chunk_main(f0, step, 0, act[rows, :], w2_buf[par, cols_of(f0 + 1), :])
            x_t[1 - t_par, third, :] = x_buf[1 - t_par, :, third].T
            g_t[1 - t_par, third, :] = act[next_rows, third].T
            chunk_main(f0 + 1, step + 1, 1, act[q_rows, :], w2_buf[next_par, cols_of(next_f), :])

            @pl.when((tile == tiles - 1) & (i < final))
            def _():
                for f in (f0, f0 + 1):
                    for cp in local_copies(i, f):
                        cp.start()

            @pl.when((tile == tiles - 1) & (i == final))
            def _():
                for f in (f0, f0 + 1):
                    send_copy(i, f, dw.at[1 - core, :, cols_of(f)]).start()

        act[rows, :] = acc[...].astype(BF16)

    out = pltpu.make_async_copy(act, g_out, g_sem)
    out.start()
    final_rel = _relation(me, top_block - final)
    for c in range(2):
        wait_out(final - 1, c)
    for c in range(n_piece + 1):
        if c < n_piece:
            if c >= 2:
                wait_out(final, c)
            if c % 2 == 0:
                send_copy(final, c // 2).wait_recv()
            sib_load(final, c).start()
        if c > 0:
            done = c - 1
            par = done % 2
            sib_load(final, done).wait()
            val = dw[core, :, done * PIECE:(done + 1) * PIECE] + s_buf[par]

            @pl.when(final_rel == 0)
            def _(val=val, par=par, done=done):
                k_buf[par] = val
                own_out(done).start()

            @pl.when(final_rel != 0)
            def _(val=val, par=par, done=done):
                o_buf[par] = val.astype(BF16)
                for other in range(1, 4):
                    @pl.when(final_rel == other)
                    def _(other=other):
                        part_out(other, done).start()
    for c in (n_piece - 2, n_piece - 1):
        wait_out(final, c)
    for i in range(n_blocks):
        for f in range(n_chunk):
            send_copy(i, f).wait_send()
    out.wait()


def run_backward(top_block, n_blocks, grad, saved, u_all, weights):
    n_rows, d_model = grad.shape
    d_ff = weights[0].shape[2]
    tiles = n_rows // TILE
    n_chunk = d_ff // CHUNK
    return pl.pallas_call(
        functools.partial(backward_kernel, top_block, n_blocks, tiles),
        name="backward",
        out_shape=[
            jax.ShapeDtypeStruct((n_rows, d_model), BF16),
            jax.ShapeDtypeStruct((n_blocks, 2, d_model, d_ff), F32),
            jax.ShapeDtypeStruct((n_blocks, d_model, d_ff), F32),
            jax.ShapeDtypeStruct((d_model, d_ff), F32),
        ] + [jax.ShapeDtypeStruct((d_model, d_ff), BF16)] * 3,
        in_specs=[ANY] * 7,
        out_specs=[ANY] * 7,
        scratch_shapes=[
            pltpu.VMEM((n_rows, d_model), BF16),
            pltpu.VMEM((2, d_model, d_ff), BF16),
            pltpu.VMEM((2, d_ff, d_model), BF16),
            pltpu.VMEM((2, d_model, d_ff), F32),
            pltpu.VMEM((RING, TILE, CHUNK), F32),
            pltpu.VMEM((2, TILE, d_model), BF16),
            pltpu.VMEM((2, d_model, TILE), BF16),
            pltpu.VMEM((2, d_model, TILE), BF16),
            pltpu.VMEM((TILE, d_model), F32),
            pltpu.VMEM((2, TILE, CHUNK), F32),
            pltpu.VMEM((2, d_model, PIECE), F32),
            pltpu.VMEM((2, d_model, PIECE), F32),
            pltpu.VMEM((2, d_model, PIECE), BF16),
            pltpu.SemaphoreType.DMA(()),
            pltpu.SemaphoreType.DMA((2, 2)),
            pltpu.SemaphoreType.DMA((RING,)),
            pltpu.SemaphoreType.DMA((2,)),
            pltpu.SemaphoreType.DMA((n_chunk, 2)),
            pltpu.SemaphoreType.DMA((n_blocks, n_chunk)),
            pltpu.SemaphoreType.DMA((n_blocks, n_chunk)),
            pltpu.SemaphoreType.DMA((2, 2)),
            pltpu.SemaphoreType.DMA((2,)),
        ],
        compiler_params=pltpu.CompilerParams(collective_id=1, has_side_effects=True, vmem_limit_bytes=67043328),
        cost_estimate=pl.CostEstimate(flops=8 * n_blocks * n_rows * d_model * d_ff, bytes_accessed=400 * 2**20, transcendentals=0),
    )(grad, saved, u_all, *weights)


def chain_kernel(top_block, tiles, g_hbm, u_hbm, w1_loc, w2_loc, wg1, wg2, g_all, r_all, a_all,
                 act, w1_buf, w2_buf, u_buf, r_buf, a_buf, acc, q_buf, g_sem, w_sem, u_sem, r_sem, a_sem, s_sem):
    me = lax.axis_index("stage")
    d_ff = u_buf.shape[2]
    n_blocks = top_block + 1
    sources, buffers = (w1_loc, w2_loc, wg1, wg2), (w1_buf, w2_buf)
    steps = n_blocks * tiles

    def u_copy(bt):
        par = lax.rem(bt, 2)
        return pltpu.make_async_copy(u_hbm.at[top_block - bt // tiles, _tile_rows(lax.rem(bt, tiles)), :], u_buf.at[par], u_sem.at[par])

    def out_copies(bt):
        par = lax.rem(bt, 2)
        blk, rows = top_block - bt // tiles, _tile_rows(lax.rem(bt, tiles))
        return [pltpu.make_async_copy(r_buf.at[par], r_all.at[blk, rows, :], r_sem.at[par]),
                pltpu.make_async_copy(a_buf.at[par], a_all.at[blk, rows, :], a_sem.at[par])]

    def g_save(bt):
        rows = _tile_rows(lax.rem(bt, tiles))
        return pltpu.make_async_copy(act.at[rows, :], g_all.at[top_block - bt // tiles, rows, :], s_sem)

    g_in = pltpu.make_async_copy(g_hbm, act, g_sem)
    g_in.start()
    _start_weights(me, sources, buffers, w_sem, top_block, 0)
    u_copy(0).start()
    g_in.wait()

    @pl.loop(0, steps)
    def _(bt):
        i = bt // tiles
        tile = lax.rem(bt, tiles)
        blk = top_block - i
        par = lax.rem(i, 2)
        b_par = lax.rem(bt, 2)
        rows = _tile_rows(tile)

        @pl.when(tile == 0)
        def _():
            for cp in _weight_loads(sources, buffers, w_sem, blk, par, True):
                cp.wait()

            @pl.when(i + 1 < n_blocks)
            def _():
                _start_weights(me, sources, buffers, w_sem, blk - 1, 1 - par)

        @pl.when(bt + 1 < steps)
        def _():
            u_copy(bt + 1).start()

        g_save(bt).start()
        u_copy(bt).wait()

        @pl.when(bt >= 2)
        def _():
            for cp in out_copies(bt - 2):
                cp.wait()

        def body(with_input_grad):
            n_chunk = d_ff // CHUNK
            q_buf[0] = _dot_t(act[rows, :], w2_buf[par, :CHUNK, :])
            for f in range(n_chunk):
                cols = slice(f * CHUNK, (f + 1) * CHUNK)
                if f + 1 < n_chunk:
                    q_buf[(f + 1) % 2] = _dot_t(act[rows, :], w2_buf[par, (f + 1) * CHUNK:(f + 2) * CHUNK, :])
                a, slope = _gelu_grad(u_buf[b_par, :, cols])
                r = (q_buf[f % 2] * slope).astype(BF16)
                a_buf[b_par, :, cols] = a.astype(BF16)
                r_buf[b_par, :, cols] = r
                if with_input_grad:
                    part = _dot_t(r, w1_buf[par, :, cols])
                    if f == 0:
                        acc[...] = part
                    else:
                        acc[...] += part

        @pl.when(blk > 0)
        def _():
            body(True)

        @pl.when(blk == 0)
        def _():
            body(False)

        for cp in out_copies(bt):
            cp.start()
        g_save(bt).wait()

        @pl.when(blk > 0)
        def _():
            act[rows, :] = (act[rows, :].astype(F32) + acc[...]).astype(BF16)

    for bt in (steps - 2, steps - 1):
        for cp in out_copies(jnp.int32(bt)):
            cp.wait()


def run_chain(top_block, grad, u_all, weights):
    n_rows, d_model = grad.shape
    d_ff = weights[0].shape[2]
    tiles = n_rows // TILE
    n_blocks = top_block + 1
    return pl.pallas_call(
        functools.partial(chain_kernel, top_block, tiles),
        name="chain",
        out_shape=[
            jax.ShapeDtypeStruct((n_blocks, n_rows, d_model), BF16),
            jax.ShapeDtypeStruct((n_blocks, n_rows, d_ff), BF16),
            jax.ShapeDtypeStruct((n_blocks, n_rows, d_ff), BF16),
        ],
        in_specs=[ANY] * 6,
        out_specs=[ANY] * 3,
        scratch_shapes=[
            pltpu.VMEM((n_rows, d_model), BF16),
            pltpu.VMEM((2, d_model, d_ff), BF16),
            pltpu.VMEM((2, d_ff, d_model), BF16),
            pltpu.VMEM((2, TILE, d_ff), F32),
            pltpu.VMEM((2, TILE, d_ff), BF16),
            pltpu.VMEM((2, TILE, d_ff), BF16),
            pltpu.VMEM((TILE, d_model), F32),
            pltpu.VMEM((2, TILE, CHUNK), F32),
            pltpu.SemaphoreType.DMA(()),
            pltpu.SemaphoreType.DMA((2, 2)),
            pltpu.SemaphoreType.DMA((2,)),
            pltpu.SemaphoreType.DMA((2,)),
            pltpu.SemaphoreType.DMA((2,)),
            pltpu.SemaphoreType.DMA(()),
        ],
        compiler_params=pltpu.CompilerParams(vmem_limit_bytes=62 * 2**20),
        cost_estimate=pl.CostEstimate(flops=4 * n_blocks * n_rows * d_model * d_ff, bytes_accessed=400 * 2**20, transcendentals=0),
    )(grad, u_all, *weights)


DW_ROWS = 1024


def weight_grad_kernel(first_col, saved, g_all, r_all, a_all, own, part1, part2, part3,
                       x_buf, g_buf, r_buf, a_buf, dw, sib, o_buf, in_sem, send_sem, recv_sem, out_sem):
    me = lax.axis_index("stage")
    core = lax.axis_index("data")
    width = dw.shape[3]
    row_steps = saved.shape[1] // DW_ROWS
    steps = 4 * row_steps
    cols = pl.ds(first_col, width)

    def owner_at(n):
        return jnp.where(n == 0, 3, jnp.where(n == 3, 0, n))

    def block_at(n):
        rel = owner_at(n)
        bit0 = lax.rem(lax.rem(me, 2) + lax.rem(rel, 2), 2)
        bit1 = lax.rem(me // 2 + rel // 2, 2)
        return bit0 + 2 * bit1

    def loads(step):
        par = lax.rem(step, 2)
        blk = block_at(step // row_steps)
        rows = pl.ds(pl.multiple_of(lax.rem(step, row_steps) * DW_ROWS, DW_ROWS), DW_ROWS)
        return [pltpu.make_async_copy(saved.at[blk, rows, :], x_buf.at[par], in_sem.at[par, 0]),
                pltpu.make_async_copy(g_all.at[blk, rows, :], g_buf.at[par], in_sem.at[par, 1]),
                pltpu.make_async_copy(r_all.at[blk, rows, cols], r_buf.at[par], in_sem.at[par, 2]),
                pltpu.make_async_copy(a_all.at[blk, rows, cols], a_buf.at[par], in_sem.at[par, 3])]

    def send_copy(n):
        par = lax.rem(n, 2)
        return pltpu.make_async_remote_copy(
            src_ref=dw.at[par, 1 - core], dst_ref=sib.at[n], send_sem=send_sem.at[par], recv_sem=recv_sem.at[n],
            device_id=(me, 1 - core), device_id_type=MESH)

    def part_copy(which):
        return pltpu.make_async_copy(o_buf, (part3, part1, part2)[which], out_sem)

    for cp in loads(0):
        cp.start()
    _sibling_barrier(me, core)

    @pl.loop(0, steps)
    def _(step):
        n = step // row_steps
        k = lax.rem(step, row_steps)
        par = lax.rem(step, 2)
        d_par = lax.rem(n, 2)

        @pl.when(step + 1 < steps)
        def _():
            for cp in loads(step + 1):
                cp.start()

        @pl.when((k == 0) & (n >= 2))
        def _():
            send_copy(n).wait_send()

        for which in range(3):
            @pl.when((k == row_steps - 1) & (n == which + 1))
            def _(which=which):
                if which > 0:
                    part_copy(which - 1).wait()
                send_copy(jnp.int32(which)).wait_recv()
                o_buf[...] = (dw[which % 2, core] + sib[which]).astype(BF16)
                part_copy(which).start()
        for cp in loads(step):
            cp.wait()
        x_t = x_buf[par].T
        g_t = g_buf[par].T
        first = k == 0
        d1 = _dot(x_t, r_buf[par])
        d2 = _dot(g_t, a_buf[par])
        dw[d_par, 0] = jnp.where(first, 0.0, dw[d_par, 0]) + d1
        dw[d_par, 1] = jnp.where(first, 0.0, dw[d_par, 1]) + d2

        @pl.when(k == row_steps - 1)
        def _():
            send_copy(n).start()

    part_copy(2).wait()
    last = jnp.int32(3)
    send_copy(last).wait_recv()
    sib[3] = dw[1, core] + sib[3]
    done = pltpu.make_async_copy(sib.at[3], own, out_sem)
    done.start()
    done.wait()
    for n in (2, 3):
        send_copy(jnp.int32(n)).wait_send()


def run_weight_grad(first_col, width, ident, saved, g_all, r_all, a_all):
    n_rows, d_model = saved.shape[1:]
    return pl.pallas_call(
        functools.partial(weight_grad_kernel, first_col),
        out_shape=[jax.ShapeDtypeStruct((d_model, width), F32)] + [jax.ShapeDtypeStruct((d_model, width), BF16)] * 3,
        in_specs=[ANY] * 4,
        out_specs=[ANY] * 4,
        scratch_shapes=[
            pltpu.VMEM((2, DW_ROWS, d_model), BF16),
            pltpu.VMEM((2, DW_ROWS, d_model), BF16),
            pltpu.VMEM((2, DW_ROWS, width), BF16),
            pltpu.VMEM((2, DW_ROWS, width), BF16),
            pltpu.VMEM((2, 2, d_model, width), F32),
            pltpu.VMEM((4, d_model, width), F32),
            pltpu.VMEM((d_model, width), BF16),
            pltpu.SemaphoreType.DMA((2, 4)),
            pltpu.SemaphoreType.DMA((2,)),
            pltpu.SemaphoreType.DMA((4,)),
            pltpu.SemaphoreType.DMA(()),
        ],
        compiler_params=pltpu.CompilerParams(collective_id=ident, has_side_effects=True, vmem_limit_bytes=62 * 2**20),
        cost_estimate=pl.CostEstimate(flops=16 * n_rows * d_model * width, bytes_accessed=100 * 2**20, transcendentals=0),
    )(saved, g_all, r_all, a_all)


COMBINE_ROWS = 64


def combine_kernel(tau_clip, n_groups, *refs):
    groups = [refs[4 * g:4 * g + 4] for g in range(n_groups)]
    loss, total, clip_out, loss_out, mine, gathered, send_sem, recv_sem = refs[4 * n_groups:]
    step = pl.program_id(0)
    here = lax.axis_index("stage") * 2 + lax.axis_index("data")
    n_dev = gathered.shape[0]
    barrier = pltpu.get_barrier_semaphore()

    @pl.when(step == 0)
    def _():
        for k in range(1, n_dev):
            other = lax.rem(here + k, n_dev)
            pl.semaphore_signal(barrier, inc=1, device_id=(other // 2, lax.rem(other, 2)), device_id_type=MESH)
        mine[0] = jnp.zeros((8, 128), F32)
        mine[1] = loss[...]

    first = 0
    squares = mine[0]
    for g, (own, got1, got2, got3) in enumerate(groups):
        width = own.shape[1]
        val = (own[...] + got1[...].astype(F32)) + (got2[...].astype(F32) + got3[...].astype(F32))
        if g == 0:
            total[1] = val
        else:
            total[0, :, first:first + width] = val
            first += width
        part = jnp.sum((val * val).reshape(COMBINE_ROWS // 8, 8, width), axis=0)
        for j in range(width // 128):
            squares = squares + part[:, j * 128:(j + 1) * 128]
    mine[0] = squares

    def copy(k, slot):
        other = lax.rem(here + k, n_dev)
        return pltpu.make_async_remote_copy(
            src_ref=mine, dst_ref=gathered.at[slot], send_sem=send_sem.at[k], recv_sem=recv_sem.at[k],
            device_id=(other // 2, lax.rem(other, 2)), device_id_type=MESH)

    @pl.when(step == pl.num_programs(0) - 1)
    def _():
        gathered[here] = mine[...]
        pl.semaphore_wait(barrier, n_dev - 1)
        for k in range(1, n_dev):
            copy(k, here).start()
        for k in range(1, n_dev):
            copy(k, lax.rem(here + n_dev - k, n_dev)).wait_recv()
        sums = jnp.sum(gathered[...], axis=0)
        squared = jnp.sum(jnp.sum(sums[0], axis=0, keepdims=True), axis=1, keepdims=True)
        lost = jnp.sum(jnp.sum(sums[1], axis=0, keepdims=True), axis=1, keepdims=True)
        norm = jnp.sqrt(jnp.broadcast_to(squared, (8, 128)))
        clip_out[...] = jnp.minimum(1.0, tau_clip / norm)
        loss_out[...] = jnp.broadcast_to(lost, (8, 128))
        for k in range(1, n_dev):
            copy(k, here).wait_send()


def run_combine(tau_clip, groups, loss):
    d_model, d_ff = groups[0][0].shape
    specs = [pl.BlockSpec((COMBINE_ROWS, val.shape[1]), lambda i: (i, 0)) for group in groups for val in group]
    lanes = pl.BlockSpec((8, 128), lambda i: (0, 0))
    return pl.pallas_call(
        functools.partial(combine_kernel, tau_clip, len(groups)),
        name="combine",
        grid=(d_model // COMBINE_ROWS,),
        out_shape=[jax.ShapeDtypeStruct((2, d_model, d_ff), F32)] + [jax.ShapeDtypeStruct((8, 128), F32)] * 2,
        in_specs=specs + [lanes],
        out_specs=[pl.BlockSpec((2, COMBINE_ROWS, d_ff), lambda i: (0, i, 0)), lanes, lanes],
        scratch_shapes=[
            pltpu.VMEM((2, 8, 128), F32),
            pltpu.VMEM((8, 2, 8, 128), F32),
            pltpu.SemaphoreType.DMA((8,)),
            pltpu.SemaphoreType.DMA((8,)),
        ],
        compiler_params=pltpu.CompilerParams(collective_id=7, has_side_effects=True, dimension_semantics=("arbitrary",), vmem_limit_bytes=40 * 2**20),
    )(*[val for group in groups for val in group], loss)


FLAT_ROWS = 3072


def update_kernel(learn_rate, grad, clip, w_old, m_old, v_old, w_new, m_new, v_new, w1_half, w2_half,
                  g_one, g_two, flat, wide, n_one, n_two, g_sem, n_sem):
    step = pl.program_id(0)
    core = lax.axis_index("data")
    d_model, d_ff = grad.shape[1], grad.shape[2]
    rows1, rows2 = FLAT_ROWS * 128 // d_ff, FLAT_ROWS * 128 // d_model
    chunks = d_model // rows1
    steps = 2 * chunks

    def g_copy(n, of_core):
        par = lax.rem(n, 2)
        half, chunk = n // chunks, lax.rem(n, chunks)
        if of_core == 0:
            return pltpu.make_async_copy(grad.at[half, pl.ds(pl.multiple_of(chunk * rows1, rows1), rows1), :], g_one.at[par], g_sem.at[par])
        return pltpu.make_async_copy(grad.at[half, :, pl.ds(pl.multiple_of(chunk * rows2, rows2), rows2)], g_two.at[par], g_sem.at[par])

    def n_copy(n, of_core):
        par = lax.rem(n, 2)
        half, chunk = n // chunks, lax.rem(n, chunks)
        if of_core == 0:
            return pltpu.make_async_copy(n_one.at[par], w1_half.at[half, pl.ds(pl.multiple_of(chunk * rows1, rows1), rows1), :], n_sem.at[par])
        return pltpu.make_async_copy(n_two.at[par], w2_half.at[half, pl.ds(pl.multiple_of(chunk * rows2, rows2), rows2), :], n_sem.at[par])

    par = lax.rem(step, 2)
    for of_core in range(2):
        @pl.when(core == of_core)
        def _(of_core=of_core):
            @pl.when(step == 0)
            def _():
                g_copy(step, of_core).start()

            @pl.when(step + 1 < steps)
            def _():
                g_copy(step + 1, of_core).start()

            g_copy(step, of_core).wait()
            if of_core == 0:
                val = g_one[par]
                per_row = d_ff // 128
            else:
                val = g_two[par].T
                per_row = d_model // 128
            for j in range(per_row):
                flat[pl.ds(j, val.shape[0], per_row), :] = val[:, j * 128:(j + 1) * 128]

    grad_clip = jnp.broadcast_to(clip[0:1, :], (FLAT_ROWS, 128)) * flat[...]
    m_val = BETA_ONE * m_old[...] + (1.0 - BETA_ONE) * grad_clip
    v_val = BETA_TWO * v_old[...] + (1.0 - BETA_TWO) * grad_clip * grad_clip
    m_hat = m_val * (1.0 / (1.0 - BETA_ONE ** ADAM_STEP))
    v_hat = v_val * (1.0 / (1.0 - BETA_TWO ** ADAM_STEP))
    w_val = w_old[...]
    w_val = w_val - learn_rate * (m_hat / (jnp.sqrt(v_hat) + ADAM_EPS) + WEIGHT_DECAY * w_val)
    m_new[...] = m_val
    v_new[...] = v_val
    w_new[...] = w_val
    wide[...] = w_val

    for of_core in range(2):
        @pl.when(core == of_core)
        def _(of_core=of_core):
            @pl.when(step >= 2)
            def _():
                n_copy(step - 2, of_core).wait()

            buf, per_row = (n_one, d_ff // 128) if of_core == 0 else (n_two, d_model // 128)
            for j in range(per_row):
                buf[par, :, j * 128:(j + 1) * 128] = wide[pl.ds(j, buf.shape[1], per_row), :].astype(BF16)
            n_copy(step, of_core).start()

            @pl.when(step == steps - 1)
            def _():
                n_copy(step - 1, of_core).wait()
                n_copy(step, of_core).wait()


def run_update(learn_rate, grad, clip, w_old, m_old, v_old):
    _, d_model, d_ff = grad.shape
    rows1, rows2 = FLAT_ROWS * 128 // d_ff, FLAT_ROWS * 128 // d_model
    steps = w_old.shape[0] // FLAT_ROWS
    flat_spec = pl.BlockSpec((FLAT_ROWS, 128), lambda i: (i, 0))
    flat_shape = jax.ShapeDtypeStruct(w_old.shape, F32)
    return pl.pallas_call(
        functools.partial(update_kernel, learn_rate),
        name="update",
        grid=(steps,),
        out_shape=[flat_shape] * 3 + [jax.ShapeDtypeStruct((2, d_model, d_ff), BF16), jax.ShapeDtypeStruct((2, d_ff, d_model), BF16)],
        in_specs=[ANY, pl.BlockSpec((8, 128), lambda i: (0, 0))] + [flat_spec] * 3,
        out_specs=[flat_spec] * 3 + [ANY, ANY],
        scratch_shapes=[
            pltpu.VMEM((2, rows1, d_ff), F32),
            pltpu.VMEM((2, d_model, rows2), F32),
            pltpu.VMEM((FLAT_ROWS, 128), F32),
            pltpu.VMEM((FLAT_ROWS, 128), F32),
            pltpu.VMEM((2, rows1, d_ff), BF16),
            pltpu.VMEM((2, rows2, d_model), BF16),
            pltpu.SemaphoreType.DMA((2,)),
            pltpu.SemaphoreType.DMA((2,)),
        ],
        compiler_params=pltpu.CompilerParams(dimension_semantics=("arbitrary",), vmem_limit_bytes=60 * 2**20),
        cost_estimate=pl.CostEstimate(flops=10**9, bytes_accessed=150 * 2**20, transcendentals=0),
    )(grad, clip, w_old, m_old, v_old)


def merge_kernel(w1_half, w2_half, w1_got, w2_got, w1_new, w2_new, buf1, buf2, in_sem, out_sem):
    del w1_half, w2_half
    core = lax.axis_index("data")
    for of_core, got, new, buf in ((1, w1_got, w1_new, buf1), (0, w2_got, w2_new, buf2)):
        parts = [(half, slot) for half in range(2) for slot in range(MERGE_PARTS)]
        rows = buf.shape[1]

        @pl.when(core == of_core)
        def _(parts=parts, rows=rows, got=got, new=new, buf=buf):
            ins, outs = [], []
            for n, (half, slot) in enumerate(parts):
                where = pl.ds(slot * rows, rows)
                ins.append(pltpu.make_async_copy(got.at[half, where, :], buf.at[n], in_sem.at[n]))
                outs.append(pltpu.make_async_copy(buf.at[n], new.at[half, where, :], out_sem.at[n]))
            for cp in ins:
                cp.start()
            for cp_in, cp_out in zip(ins, outs):
                cp_in.wait()
                cp_out.start()
            for cp in outs:
                cp.wait()


MERGE_PARTS = 4


def run_merge(w1_half, w2_half, w1_got, w2_got):
    _, d_model, d_ff = w1_half.shape
    n = 2 * MERGE_PARTS
    return pl.pallas_call(
        merge_kernel,
        name="merge",
        out_shape=[jax.ShapeDtypeStruct(w1_half.shape, BF16), jax.ShapeDtypeStruct(w2_half.shape, BF16)],
        in_specs=[ANY] * 4,
        out_specs=[ANY] * 2,
        input_output_aliases={0: 0, 1: 1},
        scratch_shapes=[
            pltpu.VMEM((n, d_model // MERGE_PARTS, d_ff), BF16),
            pltpu.VMEM((n, d_ff // MERGE_PARTS, d_model), BF16),
            pltpu.SemaphoreType.DMA((n,)),
            pltpu.SemaphoreType.DMA((n,)),
        ],
        compiler_params=pltpu.CompilerParams(vmem_limit_bytes=40 * 2**20),
    )(w1_half, w2_half, w1_got, w2_got)


GROUPS = ((0, 1024), (1024, 1024), (2048, 512), (2560, 512))


def solution(mesh):
    n_stage = mesh.shape["stage"]
    n_data = mesh.shape["data"]
    axes = ("stage", "data")

    def device(stage, core):
        return stage * n_data + core

    def from_core(core):
        return [(device(s, core), device(s, 1 - core)) for s in range(n_stage)]

    def across(flip):
        return [(device(s, c), device(s ^ flip, c)) for s in range(n_stage) for c in range(n_data)]

    def exchange(parts):
        got = []
        for flip, part in enumerate(parts, start=1):
            got.append(lax.ppermute(part, axes, across(flip)))
        return got

    def device_step(x_loc, t_loc, w1_loc, w2_loc, wm_loc, m_loc, v_loc):
        n_micro, n_tok, d_model = x_loc.shape
        d_ff = w1_loc.shape[4]
        n_tokens = n_micro * n_tok * n_data
        n_blocks = 2 * n_stage
        n_rows = n_micro * n_tok // n_stage
        tau_clip = 0.3 * d_model * math.sqrt(n_blocks * (3.0 / n_tokens + 0.008))
        learn_rate = 0.1 / math.sqrt(4.0 * d_model * n_blocks)
        w1 = w1_loc.reshape(2, d_model, d_ff)
        w2 = w2_loc.reshape(2, d_ff, d_model)
        flat_rows = (n_micro * n_tok, d_model)
        wg1, wg2, saved, u_all, seed, loss_acc = run_forward(n_tokens, x_loc.reshape(flat_rows), t_loc.reshape(flat_rows), w1, w2, n_rows)
        weights = (w1, w2, wg1, wg2)
        grad, _, _, own_hi, *parts_hi = run_backward(7, 4, seed, saved, u_all, weights)
        groups = [[own_hi] + exchange(parts_hi)]
        g_all, r_all, a_all = run_chain(3, grad, u_all, weights)
        for n, (first, width) in enumerate(GROUPS):
            own, *parts = run_weight_grad(first, width, 2 + n, saved, g_all, r_all, a_all)
            groups.append([own] + exchange(parts))
        total, clip, loss_all = run_combine(tau_clip, groups, loss_acc)
        flat = [val.reshape(-1, 128) for val in (wm_loc, m_loc, v_loc)]
        w_new, m_new, v_new, w1_half, w2_half = run_update(learn_rate, total, clip, *flat)
        w1_got = lax.ppermute(w1_half, axes, from_core(0))
        w2_got = lax.ppermute(w2_half, axes, from_core(1))
        w1_new, w2_new = run_merge(w1_half, w2_half, w1_got, w2_got)
        mean_loss = loss_all[0, 0] / n_tokens
        return w1_new.reshape(w1_loc.shape), w2_new.reshape(w2_loc.shape), w_new.reshape(wm_loc.shape), m_new.reshape(wm_loc.shape), v_new.reshape(wm_loc.shape), mean_loss

    act_spec = P(None, "data", None)
    flat_spec = P("stage", None, None, "data")
    return jax.shard_map(device_step, mesh=mesh, in_specs=(act_spec, act_spec, P("stage"), P("stage"), flat_spec, flat_spec, flat_spec), out_specs=(P("stage"), P("stage"), flat_spec, flat_spec, flat_spec, P()), check_vma=False)
```

```python
import functools
import math
import jax
import jax.numpy as jnp
from jax import lax
from jax.experimental import pallas as pl
from jax.experimental.pallas import tpu as pltpu
from jax.sharding import PartitionSpec as P

BETA_ONE = 0.9
BETA_TWO = 0.999
ADAM_EPS = 1e-8
WEIGHT_DECAY = 0.1
ADAM_STEP = 1000
GELU_A = math.sqrt(2.0 / math.pi)
GELU_B = GELU_A * 0.044715
MESH = pl.DeviceIdType.MESH
ANY = pl.BlockSpec(memory_space=pl.ANY)
F32 = jnp.float32
BF16 = jnp.bfloat16

TILE = 512
PATH_PIECES = 4


def _dot_t(lhs, rhs):
    return lax.dot_general(lhs, rhs, (((1,), (1,)), ((), ())), preferred_element_type=F32)


def _dot(lhs, rhs):
    return jnp.dot(lhs, rhs, preferred_element_type=F32)


SEND_SLOT = (-45, -30, -28, -20)
HOP_SLOT = {1: (-27, -20, -18, -14), 2: (-18, -14, -8, -6), 3: (-12, -9, -2, -2)}
LOAD_SLOT = -1


def forward_kernel(n_blocks, tiles, n_tokens, x_hbm, t_hbm, w1_loc, w2_loc, wg1, wg2, saved, u_out, seed, loss,
                   act, w1_buf, w2_buf, u_buf, acc, t_buf, s_buf,
                   x_sem, act_sem, u_sem, w_sem, t_sem, s_sem, ici_send, ici_recv, d2d_send, d2d_recv):
    me = lax.axis_index("stage")
    core = lax.axis_index("data")
    d_model, d_ff = w1_loc.shape[1], w1_loc.shape[2]
    n_rows = act.shape[0]
    n_piece = 4 * PATH_PIECES
    rows1, rows2 = d_model // n_piece, d_ff // n_piece

    def peer(flip):
        bit0, bit1 = lax.rem(me, 2), me // 2
        return (1 - bit0 + 2 * bit1) if flip == 1 else (bit0 + 2 * (1 - bit1))

    def rel_of(blk):
        own = lax.rem(blk, 4)
        a0, a1, b0, b1 = lax.rem(me, 2), me // 2, lax.rem(own, 2), own // 2
        return (a0 + b0 - 2 * a0 * b0) + 2 * (a1 + b1 - 2 * a1 * b1)

    def piece(j, path, of_core):
        return j * 4 + path * 2 + of_core

    def views(blk, idx):
        return (wg1.at[blk, pl.ds(pl.multiple_of(idx * rows1, 16), rows1), :],
                wg2.at[blk, pl.ds(pl.multiple_of(idx * rows2, 64), rows2), :])

    def local_views(blk, idx):
        half = blk // 4
        return (w1_loc.at[half, pl.ds(pl.multiple_of(idx * rows1, 16), rows1), :],
                w2_loc.at[half, pl.ds(pl.multiple_of(idx * rows2, 64), rows2), :])

    def ici_copies(blk, path, j, sources, flip):
        idx = piece(j, path, core)
        slot = path * PATH_PIECES + j
        return [pltpu.make_async_remote_copy(
            src_ref=src, dst_ref=dst, send_sem=ici_send.at[blk, slot, m], recv_sem=ici_recv.at[blk, slot, m],
            device_id=(peer(flip), core), device_id_type=MESH)
            for m, (src, dst) in enumerate(zip(sources, views(blk, idx)))]

    def d2d_copies(blk, path, j, of_core):
        idx = piece(j, path, of_core)
        slot = path * PATH_PIECES + j
        return [pltpu.make_async_remote_copy(
            src_ref=ref, dst_ref=ref, send_sem=d2d_send.at[blk, slot, m], recv_sem=d2d_recv.at[blk, slot, m],
            device_id=(me, 1 - core), device_id_type=MESH) for m, ref in enumerate(views(blk, idx))]

    def first_flip(path):
        return 1 if path == 0 else 2

    def own_send(blk, j):
        @pl.when(rel_of(blk) == 0)
        def _():
            for path in range(2):
                for cp in ici_copies(blk, path, j, local_views(blk, piece(j, path, core)), first_flip(path)):
                    cp.start()

    def hop_event(blk, hop, j):
        rel = rel_of(blk)
        for path in range(2):
            at_rel = {1: (1, 2), 2: (3, 3), 3: (2, 1)}[hop][path]

            @pl.when(rel == at_rel)
            def _(path=path):
                flip = first_flip(path)
                if hop == 1:
                    flip = 3 - flip
                copies = ici_copies(blk, path, j, views(blk, piece(j, path, core)), flip)
                for cp in copies:
                    cp.wait_recv()
                if hop < 3:
                    for cp in copies:
                        cp.start()
                for cp in d2d_copies(blk, path, j, core):
                    cp.start()

    def weight_loads(blk, par, is_own):
        half = blk // 4
        src1, src2 = (w1_loc.at[half], w2_loc.at[half]) if is_own else (wg1.at[blk], wg2.at[blk])
        return [pltpu.make_async_copy(src1, w1_buf.at[par], w_sem.at[par, 0]),
                pltpu.make_async_copy(src2, w2_buf.at[par], w_sem.at[par, 1])]

    def load_event(blk):
        rel = rel_of(blk)
        par = lax.rem(blk, 2)

        @pl.when(rel == 0)
        def _():
            for cp in weight_loads(blk, par, True):
                cp.start()

        @pl.when(rel != 0)
        def _():
            for path in range(2):
                for j in range(PATH_PIECES):
                    for cp in d2d_copies(blk, path, j, 1 - core):
                        cp.wait_recv()
            for cp in weight_loads(blk, par, False):
                cp.start()

    def x_copy():
        return pltpu.make_async_copy(x_hbm.at[pl.ds(pl.multiple_of(me * n_rows, n_rows), n_rows), :], act, x_sem)

    def act_copy(slot, tile):
        rows = pl.ds(pl.multiple_of(tile * TILE, TILE), TILE)
        return pltpu.make_async_copy(act.at[rows, :], saved.at[slot, rows, :], act_sem.at[tile])

    def t_copy(tile):
        return pltpu.make_async_copy(t_hbm.at[pl.ds(pl.multiple_of(me * n_rows + tile * TILE, TILE), TILE), :], t_buf, t_sem)

    def seed_copy(tile):
        return pltpu.make_async_copy(s_buf, seed.at[pl.ds(pl.multiple_of(tile * TILE, TILE), TILE), :], s_sem)

    def u_copy(blk, tile, par):
        rows = pl.ds(pl.multiple_of(tile * TILE, TILE), TILE)
        return pltpu.make_async_copy(u_buf.at[par], u_out.at[blk, rows, :], u_sem.at[par])

    barrier = pltpu.get_barrier_semaphore()
    for target in ((peer(1), core), (peer(2), core), (me, 1 - core)):
        pl.semaphore_signal(barrier, inc=1, device_id=target, device_id_type=MESH)
    x_copy().start()
    pl.semaphore_wait(barrier, 3)

    events = []
    for hop in (3, 2, 1):
        for j in range(PATH_PIECES):
            events.append((HOP_SLOT[hop][j], functools.partial(lambda blk, hop, j: hop_event(blk, hop, j), hop=hop, j=j)))
    for j in range(PATH_PIECES):
        events.append((SEND_SLOT[j], functools.partial(lambda blk, j: own_send(blk, j), j=j)))
    events.append((LOAD_SLOT, load_event))

    def comm_slot(blk, tile):
        for offset, fn in events:
            residue = offset % tiles
            ahead = (residue - offset) // tiles
            target = blk + ahead

            @pl.when((tile == residue) & (target >= 0) & (target < n_blocks))
            def _(fn=fn, target=target):
                fn(target)

    def compute(blk, tile):
        par = lax.rem(blk, 2)
        u_par = lax.rem(tile, 2)
        rows = pl.ds(pl.multiple_of(tile * TILE, TILE), TILE)

        @pl.when(tile == 0)
        def _():
            for cp in weight_loads(blk, par, True):
                cp.wait()

        @pl.when((blk == 0) & (tile == 0))
        def _():
            x_copy().wait()
            for t in range(tiles):
                act_copy(0, t).start()

        @pl.when((blk > 0) | (tile > 1))
        def _():
            u_copy(blk, tile, u_par).wait()

        @pl.when(blk == n_blocks - 1)
        def _():
            t_copy(tile).start()

        act_copy(blk, tile).wait()
        x = act[rows, :]
        chunk = 256
        n_chunk = d_ff // chunk
        for f in range(n_chunk):
            cols = slice(f * chunk, (f + 1) * chunk)
            u = _dot(x, w1_buf[par, :, cols])
            u_buf[u_par, :, cols] = u
            inner = u * (GELU_A + GELU_B * (u * u))
            a = (u * (0.5 + 0.5 * jnp.tanh(inner))).astype(BF16)
            part = _dot(a, w2_buf[par, cols, :])
            if f == 0:
                acc[...] = part
            elif f < n_chunk - 1:
                acc[...] += part
            else:
                act[rows, :] = (x.astype(F32) + (acc[...] + part)).astype(BF16)
        u_copy(blk, tile, u_par).start()

        @pl.when(blk < n_blocks - 1)
        def _():
            act_copy(blk + 1, tile).start()

        @pl.when(blk == n_blocks - 1)
        def _():
            t_copy(tile).wait()

            @pl.when(tile > 0)
            def _():
                seed_copy(tile - 1).wait()
            residual = act[rows, :].astype(F32) - t_buf[...].astype(F32)
            s_buf[...] = (residual / n_tokens).astype(BF16)
            squares = jnp.sum((residual * residual).reshape(TILE // 8, 8, residual.shape[1]), axis=0)
            folded = squares[:, :128]
            for j in range(1, residual.shape[1] // 128):
                folded = folded + squares[:, j * 128:(j + 1) * 128]
            loss[...] += 0.5 * folded
            seed_copy(tile).start()

    lead = -(min(SEND_SLOT) // tiles)
    loss[...] = jnp.zeros_like(loss)

    @pl.loop(0, (n_blocks + lead) * tiles)
    def _(step):
        blk = step // tiles - lead
        tile = lax.rem(step, tiles)
        comm_slot(blk, tile)

        @pl.when(blk >= 0)
        def _():
            compute(blk, tile)

    for par in range(2):
        u_copy(0, 0, par).wait()
    seed_copy(0).wait()

    @pl.loop(0, n_blocks)
    def _(blk):
        rel = rel_of(blk)
        for path in range(2):
            last = (2, 1)[path]

            @pl.when(rel != last)
            def _(path=path):
                for j in range(PATH_PIECES):
                    for cp in ici_copies(blk, path, j, views(blk, piece(j, path, core)), 1):
                        cp.wait_send()

        @pl.when(rel != 0)
        def _():
            for path in range(2):
                for j in range(PATH_PIECES):
                    for cp in d2d_copies(blk, path, j, core):
                        cp.wait_send()


def run_forward(n_tokens, x_flat, t_flat, w1_loc, w2_loc, n_rows):
    n_half, d_model, d_ff = w1_loc.shape
    n_blocks = 4 * n_half
    tiles = n_rows // TILE
    slots = 2 * PATH_PIECES
    out_shape = [
        jax.ShapeDtypeStruct((n_blocks, d_model, d_ff), BF16),
        jax.ShapeDtypeStruct((n_blocks, d_ff, d_model), BF16),
        jax.ShapeDtypeStruct((n_blocks, n_rows, d_model), BF16),
        jax.ShapeDtypeStruct((n_blocks, n_rows, d_ff), F32),
        jax.ShapeDtypeStruct((n_rows, d_model), BF16),
        jax.ShapeDtypeStruct((8, 128), F32),
    ]
    return pl.pallas_call(
        functools.partial(forward_kernel, n_blocks, tiles, n_tokens),
        name="forward",
        out_shape=out_shape,
        in_specs=[ANY] * 4,
        out_specs=[ANY] * 5 + [pl.BlockSpec(memory_space=pltpu.VMEM)],
        scratch_shapes=[
            pltpu.VMEM((n_rows, d_model), BF16),
            pltpu.VMEM((2, d_model, d_ff), BF16),
            pltpu.VMEM((2, d_ff, d_model), BF16),
            pltpu.VMEM((2, TILE, d_ff), F32),
            pltpu.VMEM((TILE, d_model), F32),
            pltpu.VMEM((TILE, d_model), BF16),
            pltpu.VMEM((TILE, d_model), BF16),
            pltpu.SemaphoreType.DMA(()),
            pltpu.SemaphoreType.DMA((tiles,)),
            pltpu.SemaphoreType.DMA((2,)),
            pltpu.SemaphoreType.DMA((2, 2)),
            pltpu.SemaphoreType.DMA(()),
            pltpu.SemaphoreType.DMA(()),
            pltpu.SemaphoreType.DMA((n_blocks, slots, 2)),
            pltpu.SemaphoreType.DMA((n_blocks, slots, 2)),
            pltpu.SemaphoreType.DMA((n_blocks, slots, 2)),
            pltpu.SemaphoreType.DMA((n_blocks, slots, 2)),
        ],
        compiler_params=pltpu.CompilerParams(collective_id=0, has_side_effects=True, vmem_limit_bytes=60 * 2**20),
        cost_estimate=pl.CostEstimate(flops=4 * n_blocks * n_rows * d_model * d_ff, bytes_accessed=600 * 2**20, transcendentals=0),
    )(x_flat, t_flat, w1_loc, w2_loc)


RING = 5
CHUNK = 512
PIECE = 256


def _relation(me, blk):
    own = lax.rem(blk, 4)
    a0, a1, b0, b1 = lax.rem(me, 2), me // 2, lax.rem(own, 2), own // 2
    return (a0 + b0 - 2 * a0 * b0) + 2 * (a1 + b1 - 2 * a1 * b1)


def _tile_rows(tile):
    return pl.ds(pl.multiple_of(tile * TILE, TILE), TILE)


def _gelu_grad(u):
    cube = GELU_B * (u * u)
    th = jnp.tanh(u * (GELU_A + cube))
    cdf = 0.5 + 0.5 * th
    a = u * cdf
    return a, cdf + (a * (3.0 - 3.0 * th)) * (cube + GELU_A / 3.0)


STAGE_SLOT = (2, 5, 8, 10)


def backward_kernel(n_blocks, tiles, g_hbm, saved, u_hbm, w1_loc, w2_loc, wg1, wg2, local, sib, inbox, own, squares,
                    act, w1_buf, w2_buf, dw, u_buf, x_buf, x_t, g_t, acc, q_buf, k_buf, s_buf, r_buf, o_buf,
                    g_sem, w_sem, u_sem, x_sem, keep_sem, d2d_send, d2d_recv, load_sem, own_sem, ici_send, ici_recv):
    me = lax.axis_index("stage")
    core = lax.axis_index("data")
    d_model, d_ff = dw.shape[1], dw.shape[2]
    n_chunk = d_ff // CHUNK
    n_pair = n_chunk // 2
    n_slot = d_ff // PIECE // 2
    steps = n_blocks * tiles
    total = steps * n_chunk
    top = n_blocks - 1

    def cols_of(f):
        return pl.ds(pl.multiple_of(f * CHUNK, CHUNK), CHUNK)

    def pair_of(p):
        return pl.ds(pl.multiple_of(p * 2 * CHUNK, 2 * CHUNK), 2 * CHUNK)

    def piece_of(c):
        return pl.ds(pl.multiple_of(c * PIECE, PIECE), PIECE)

    def weight_copies(blk, pair, is_own):
        half = blk // 4
        src1, src2 = (w1_loc.at[half], w2_loc.at[half]) if is_own else (wg1.at[blk], wg2.at[blk])
        cols = pair_of(pair)
        return [pltpu.make_async_copy(src1.at[:, cols], w1_buf.at[:, cols], w_sem.at[pair, 0]),
                pltpu.make_async_copy(src2.at[cols, :], w2_buf.at[cols, :], w_sem.at[pair, 1])]

    def start_weights(blk, pair):
        rel = _relation(me, blk)

        @pl.when(rel == 0)
        def _():
            for cp in weight_copies(blk, pair, True):
                cp.start()

        @pl.when(rel != 0)
        def _():
            for cp in weight_copies(blk, pair, False):
                cp.start()

    def u_copy(step):
        blk = top - step // (tiles * n_chunk)
        tile = lax.rem(step // n_chunk, tiles)
        f = lax.rem(step, n_chunk)
        slot = lax.rem(step, RING)
        return pltpu.make_async_copy(u_hbm.at[blk, _tile_rows(tile), cols_of(f)], u_buf.at[slot], u_sem.at[slot])

    def x_copy(bt):
        par = lax.rem(bt, 2)
        return pltpu.make_async_copy(saved.at[top - bt // tiles, _tile_rows(lax.rem(bt, tiles)), :], x_buf.at[par], x_sem.at[par])

    def g_in_copy():
        return pltpu.make_async_copy(g_hbm, act, g_sem)

    def keep_copy(j, f):
        return pltpu.make_async_copy(dw.at[core, :, cols_of(f)], local.at[lax.rem(j, 3), :, cols_of(f)], keep_sem.at[f])

    def give_copy(j, c):
        return pltpu.make_async_remote_copy(
            src_ref=dw.at[1 - core, :, piece_of(c)], dst_ref=sib.at[j, :, piece_of(c)], send_sem=d2d_send.at[c],
            recv_sem=d2d_recv.at[j, c], device_id=(me, 1 - core), device_id_type=MESH)

    def stage_of(j, path):
        rel = _relation(me, top - j)
        first, last = (1, 2) if path == 0 else (2, 1)
        return jnp.where(rel == 0, 3, jnp.where(rel == 3, 1, jnp.where(rel == last, 0, 2)))

    def next_chip(stage, path):
        first = 1 if path == 0 else 2
        flip = jnp.where(stage == 1, 3 - first, first)
        bit0, bit1 = lax.rem(me, 2), me // 2
        return jnp.where(flip == 1, 1 - bit0 + 2 * bit1, bit0 + 2 * (1 - bit1))

    def piece_loads(j, c, buf):
        return [pltpu.make_async_copy(local.at[lax.rem(j, 3), :, piece_of(c)], k_buf.at[buf], load_sem.at[buf, 0]),
                pltpu.make_async_copy(sib.at[j, :, piece_of(c)], s_buf.at[buf], load_sem.at[buf, 1])]

    def inbox_load(j, c, buf):
        return pltpu.make_async_copy(inbox.at[j, :, piece_of(c)], r_buf.at[buf], load_sem.at[buf, 2])

    def own_copy(j, c, buf):
        return pltpu.make_async_copy(k_buf.at[buf], own.at[(top - j) // 4, :, piece_of(c)], own_sem.at[buf])

    def pass_copy(j, c, buf, stage, path):
        return pltpu.make_async_remote_copy(
            src_ref=o_buf.at[buf], dst_ref=inbox.at[j, :, piece_of(c)], send_sem=ici_send.at[buf],
            recv_sem=ici_recv.at[j, c], device_id=(next_chip(stage, path), core), device_id_type=MESH)

    def last_use(j, m, path, want_own, fn):
        before = jnp.where(m > 0, stage_of(j, path), stage_of(j - 2, path))
        used = (m > 0) | (j >= 2)
        ended = (before == 3) if want_own else (before != 3)

        @pl.when(used & ended)
        def _():
            fn()

    def piece_events(j, slot):
        for path in range(2):
            stage = stage_of(j, path)
            offset = jnp.where(stage == 0, STAGE_SLOT[0], jnp.where(stage == 1, STAGE_SLOT[1], jnp.where(stage == 2, STAGE_SLOT[2], STAGE_SLOT[3])))
            buf = lax.rem(j, 2) * 2 + path
            live = (j >= 0) & (j < n_blocks)
            m_sum = slot - offset
            m_load = m_sum + 1

            @pl.when(live & (m_sum >= 0) & (m_sum < n_slot))
            def _(path=path, stage=stage, buf=buf, m=m_sum):
                c = 2 * m + path
                for cp in piece_loads(j, c, buf):
                    cp.wait()

                @pl.when(stage > 0)
                def _():
                    inbox_load(j, c, buf).wait()

                last_use(j, m, path, False, lambda: pass_copy(j, c, buf, stage, path).wait_send())

                @pl.when(stage == 0)
                def _():
                    o_buf[buf] = (k_buf[buf] + s_buf[buf]).astype(BF16)

                @pl.when((stage == 1) | (stage == 2))
                def _():
                    o_buf[buf] = ((k_buf[buf] + s_buf[buf]) + r_buf[buf].astype(F32)).astype(BF16)

                @pl.when(stage < 3)
                def _():
                    pass_copy(j, c, buf, stage, path).start()

                @pl.when(stage == 3)
                def _():
                    val = (k_buf[buf] + s_buf[buf]) + r_buf[buf].astype(F32)
                    k_buf[buf] = val
                    part = jnp.sum((val * val).reshape(d_model // 8, 8, PIECE), axis=0)
                    squares[...] += part[:, :128] + part[:, 128:]
                    own_copy(j, c, buf).start()

            @pl.when(live & (m_load >= 0) & (m_load < n_slot))
            def _(path=path, stage=stage, buf=buf, m=m_load):
                c = 2 * m + path
                last_use(j, m, path, True, lambda: own_copy(j, c, buf).wait())
                give_copy(j, c).wait_recv()
                for cp in piece_loads(j, c, buf):
                    cp.start()

                @pl.when(stage > 0)
                def _():
                    pass_copy(j, c, buf, stage, path).wait_recv()
                    inbox_load(j, c, buf).start()

    barrier = pltpu.get_barrier_semaphore()
    bit0, bit1 = lax.rem(me, 2), me // 2
    near = ((1 - bit0 + 2 * bit1, core), (bit0 + 2 * (1 - bit1), core), (me, 1 - core))
    for target in near:
        pl.semaphore_signal(barrier, inc=1, device_id=target, device_id_type=MESH)
    g_in_copy().start()
    for pair in range(n_pair):
        start_weights(jnp.int32(top), jnp.int32(pair))
    x_copy(0).start()
    x_copy(1).start()
    for step in range(RING - 2):
        u_copy(step).start()
    squares[...] = jnp.zeros_like(squares)
    pl.semaphore_wait(barrier, 3)
    g_in_copy().wait()
    x_copy(0).wait()
    x_t[0] = x_buf[0].T
    g_t[0] = act[pl.ds(0, TILE), :].T
    weight_copies(0, 0, True)[1].wait()
    q_buf[0] = _dot_t(act[pl.ds(0, TILE), :], w2_buf[pl.ds(0, CHUNK), :])

    def compute(bt):
        i = bt // tiles
        tile = lax.rem(bt, tiles)
        blk = top - i
        t_par = lax.rem(bt, 2)
        rows = _tile_rows(tile)
        next_rows = _tile_rows(lax.rem(tile + 1, tiles))

        @pl.when(bt + 1 < steps)
        def _():
            x_copy(bt + 1).wait()

        @pl.when(bt + 2 < steps)
        def _():
            x_copy(bt + 2).start()

        acc[...] = act[rows, :].astype(F32)

        def chunk_prep(f, step):
            @pl.when(step + RING - 2 < total)
            def _():
                u_copy(step + RING - 2).start()
            u_copy(step).wait()

            @pl.when((tile == 0) & (i > 0))
            def _():
                keep_copy(i - 1, f).wait()
                for c in (2 * f, 2 * f + 1):
                    give_copy(i - 1, c).wait_send()

            @pl.when(tile == 0)
            def _():
                dw[0, :, cols_of(f)] = jnp.zeros((d_model, CHUNK), F32)
                dw[1, :, cols_of(f)] = jnp.zeros((d_model, CHUNK), F32)

        def chunk_main(f, step, q_par, next_g, next_w2, with_input_grad):
            cols = cols_of(f)
            q_buf[1 - q_par] = _dot_t(next_g, next_w2)
            a, slope = _gelu_grad(u_buf[lax.rem(step, RING)])
            r = (q_buf[q_par] * slope).astype(BF16)
            dw[0, :, cols] += _dot(x_t[t_par], r)
            dw[1, :, cols] += _dot(g_t[t_par], a.astype(BF16))
            if with_input_grad:
                acc[...] += _dot_t(r, w1_buf[:, cols])

        def pair_step(pair, with_input_grad):
            f0 = pair * 2
            step = bt * n_chunk + f0
            last = pair == n_pair - 1
            chunk_prep(f0, step)
            chunk_prep(f0 + 1, step + 1)

            @pl.when(tile == 0)
            def _():
                weight_copies(0, pair, True)[0].wait()

            @pl.when((tile == 0) & (pair < n_pair - 1))
            def _():
                weight_copies(0, pair + 1, True)[1].wait()

            @pl.when(last & (tile == tiles - 1) & (bt + 1 < steps))
            def _():
                weight_copies(0, jnp.int32(0), True)[1].wait()

            q_rows = _tile_rows(jnp.where(last, lax.rem(tile + 1, tiles), tile))
            next_f = jnp.where(last, 0, f0 + 2)
            third = pl.ds(pl.multiple_of(pair * 256, 256), 256)
            chunk_main(f0, step, 0, act[rows, :], w2_buf[cols_of(f0 + 1), :], with_input_grad)
            x_t[1 - t_par, third, :] = x_buf[1 - t_par, :, third].T
            g_t[1 - t_par, third, :] = act[next_rows, third].T
            chunk_main(f0 + 1, step + 1, 1, act[q_rows, :], w2_buf[cols_of(next_f), :], with_input_grad)

            @pl.when(tile == tiles - 1)
            def _():
                for f in (f0, f0 + 1):
                    keep_copy(i, f).start()
                    for c in (2 * f, 2 * f + 1):
                        give_copy(i, c).start()

            if with_input_grad:
                @pl.when(tile == tiles - 1)
                def _():
                    start_weights(blk - 1, pair)

        @pl.when(blk > 0)
        def _():
            @pl.loop(0, n_pair)
            def _(pair):
                pair_step(pair, True)
            act[rows, :] = acc[...].astype(BF16)

        @pl.when(blk == 0)
        def _():
            @pl.loop(0, n_pair)
            def _(pair):
                pair_step(pair, False)

    @pl.loop(0, steps + 2 * tiles)
    def _(bt):
        i = bt // tiles
        tile = lax.rem(bt, tiles)

        @pl.when(bt == steps)
        def _():
            for f in range(n_chunk):
                keep_copy(top, f).wait()
                for c in (2 * f, 2 * f + 1):
                    give_copy(top, c).wait_send()

        piece_events(i - 2, tile + tiles)
        piece_events(i - 1, tile)

        @pl.when(bt < steps)
        def _():
            compute(bt)

    for j in (n_blocks - 2, n_blocks - 1):
        for path in range(2):
            stage = stage_of(j, path)
            buf = j % 2 * 2 + path

            @pl.when(stage == 3)
            def _(j=j, path=path, buf=buf):
                own_copy(j, path, buf).wait()

            @pl.when(stage < 3)
            def _(j=j, path=path, buf=buf, stage=stage):
                pass_copy(j, path, buf, stage, path).wait_send()


def run_backward(grad, saved, u_all, weights):
    n_rows, d_model = grad.shape
    n_half, _, d_ff = weights[0].shape
    n_blocks = 4 * n_half
    tiles = n_rows // TILE
    n_chunk = d_ff // CHUNK
    n_piece = d_ff // PIECE
    return pl.pallas_call(
        functools.partial(backward_kernel, n_blocks, tiles),
        name="backward",
        out_shape=[
            jax.ShapeDtypeStruct((3, d_model, d_ff), F32),
            jax.ShapeDtypeStruct((n_blocks, d_model, d_ff), F32),
            jax.ShapeDtypeStruct((n_blocks, d_model, d_ff), BF16),
            jax.ShapeDtypeStruct((n_half, d_model, d_ff), F32),
            jax.ShapeDtypeStruct((8, 128), F32),
        ],
        in_specs=[ANY] * 7,
        out_specs=[ANY] * 4 + [pl.BlockSpec(memory_space=pltpu.VMEM)],
        scratch_shapes=[
            pltpu.VMEM((n_rows, d_model), BF16),
            pltpu.VMEM((d_model, d_ff), BF16),
            pltpu.VMEM((d_ff, d_model), BF16),
            pltpu.VMEM((2, d_model, d_ff), F32),
            pltpu.VMEM((RING, TILE, CHUNK), F32),
            pltpu.VMEM((2, TILE, d_model), BF16),
            pltpu.VMEM((2, d_model, TILE), BF16),
            pltpu.VMEM((2, d_model, TILE), BF16),
            pltpu.VMEM((TILE, d_model), F32),
            pltpu.VMEM((2, TILE, CHUNK), F32),
            pltpu.VMEM((4, d_model, PIECE), F32),
            pltpu.VMEM((4, d_model, PIECE), F32),
            pltpu.VMEM((4, d_model, PIECE), BF16),
            pltpu.VMEM((4, d_model, PIECE), BF16),
            pltpu.SemaphoreType.DMA(()),
            pltpu.SemaphoreType.DMA((n_chunk // 2, 2)),
            pltpu.SemaphoreType.DMA((RING,)),
            pltpu.SemaphoreType.DMA((2,)),
            pltpu.SemaphoreType.DMA((n_chunk,)),
            pltpu.SemaphoreType.DMA((n_piece,)),
            pltpu.SemaphoreType.DMA((n_blocks, n_piece)),
            pltpu.SemaphoreType.DMA((4, 3)),
            pltpu.SemaphoreType.DMA((4,)),
            pltpu.SemaphoreType.DMA((4,)),
            pltpu.SemaphoreType.DMA((n_blocks, n_piece)),
        ],
        compiler_params=pltpu.CompilerParams(collective_id=1, has_side_effects=True, vmem_limit_bytes=67043328),
        cost_estimate=pl.CostEstimate(flops=8 * n_blocks * n_rows * d_model * d_ff, bytes_accessed=800 * 2**20, transcendentals=0),
    )(grad, saved, u_all, *weights)


def scalars_kernel(tau_clip, squares, loss, clip_out, loss_out, mine, gathered, send_sem, recv_sem):
    stage = lax.axis_index("stage")
    core = lax.axis_index("data")
    n_dev = gathered.shape[0]
    here = stage * 2 + core
    barrier = pltpu.get_barrier_semaphore()
    for k in range(1, n_dev):
        other = lax.rem(here + k, n_dev)
        pl.semaphore_signal(barrier, inc=1, device_id=(other // 2, lax.rem(other, 2)), device_id_type=MESH)
    mine[0] = squares[...]
    mine[1] = loss[...]
    gathered[here] = mine[...]
    pl.semaphore_wait(barrier, n_dev - 1)

    def copy(k, slot):
        other = lax.rem(here + k, n_dev)
        return pltpu.make_async_remote_copy(
            src_ref=mine, dst_ref=gathered.at[slot], send_sem=send_sem.at[k], recv_sem=recv_sem.at[k],
            device_id=(other // 2, lax.rem(other, 2)), device_id_type=MESH)

    for k in range(1, n_dev):
        copy(k, here).start()
    for k in range(1, n_dev):
        copy(k, lax.rem(here + n_dev - k, n_dev)).wait_recv()
    sums = jnp.sum(gathered[...], axis=0)
    squared = jnp.sum(jnp.sum(sums[0], axis=0, keepdims=True), axis=1, keepdims=True)
    lost = jnp.sum(jnp.sum(sums[1], axis=0, keepdims=True), axis=1, keepdims=True)
    norm = jnp.sqrt(jnp.broadcast_to(squared, (8, 128)))
    clip_out[...] = jnp.minimum(1.0, tau_clip / norm)
    loss_out[...] = jnp.broadcast_to(lost, (8, 128))
    for k in range(1, n_dev):
        copy(k, here).wait_send()


def run_scalars(tau_clip, squares, loss):
    vmem = pl.BlockSpec(memory_space=pltpu.VMEM)
    return pl.pallas_call(
        functools.partial(scalars_kernel, tau_clip),
        name="scalars",
        out_shape=[jax.ShapeDtypeStruct((8, 128), F32)] * 2,
        in_specs=[vmem] * 2,
        out_specs=[vmem] * 2,
        scratch_shapes=[
            pltpu.VMEM((2, 8, 128), F32),
            pltpu.VMEM((8, 2, 8, 128), F32),
            pltpu.SemaphoreType.DMA((8,)),
            pltpu.SemaphoreType.DMA((8,)),
        ],
        compiler_params=pltpu.CompilerParams(collective_id=2, has_side_effects=True),
    )(squares, loss)


FLAT_ROWS = 3072


def update_kernel(learn_rate, grad, clip, w_old, m_old, v_old, w_new, m_new, v_new, w1_half, w2_half,
                  g_one, g_two, flat, wide, n_one, n_two, g_sem, n_sem):
    step = pl.program_id(0)
    core = lax.axis_index("data")
    d_model, d_ff = grad.shape[1], grad.shape[2]
    rows1, rows2 = FLAT_ROWS * 128 // d_ff, FLAT_ROWS * 128 // d_model
    chunks = d_model // rows1
    steps = 2 * chunks

    def g_copy(n, of_core):
        par = lax.rem(n, 2)
        half, chunk = n // chunks, lax.rem(n, chunks)
        if of_core == 0:
            return pltpu.make_async_copy(grad.at[half, pl.ds(pl.multiple_of(chunk * rows1, rows1), rows1), :], g_one.at[par], g_sem.at[par])
        return pltpu.make_async_copy(grad.at[half, :, pl.ds(pl.multiple_of(chunk * rows2, rows2), rows2)], g_two.at[par], g_sem.at[par])

    def n_copy(n, of_core):
        par = lax.rem(n, 2)
        half, chunk = n // chunks, lax.rem(n, chunks)
        if of_core == 0:
            return pltpu.make_async_copy(n_one.at[par], w1_half.at[half, pl.ds(pl.multiple_of(chunk * rows1, rows1), rows1), :], n_sem.at[par])
        return pltpu.make_async_copy(n_two.at[par], w2_half.at[half, pl.ds(pl.multiple_of(chunk * rows2, rows2), rows2), :], n_sem.at[par])

    par = lax.rem(step, 2)
    for of_core in range(2):
        @pl.when(core == of_core)
        def _(of_core=of_core):
            @pl.when(step == 0)
            def _():
                g_copy(step, of_core).start()

            @pl.when(step + 1 < steps)
            def _():
                g_copy(step + 1, of_core).start()
            g_copy(step, of_core).wait()
            if of_core == 0:
                val = g_one[par]
                per_row = d_ff // 128
            else:
                val = g_two[par].T
                per_row = d_model // 128
            for j in range(per_row):
                flat[pl.ds(j, val.shape[0], per_row), :] = val[:, j * 128:(j + 1) * 128]

    grad_clip = jnp.broadcast_to(clip[0:1, :], (FLAT_ROWS, 128)) * flat[...]
    m_val = BETA_ONE * m_old[...] + (1.0 - BETA_ONE) * grad_clip
    v_val = BETA_TWO * v_old[...] + (1.0 - BETA_TWO) * grad_clip * grad_clip
    m_hat = m_val * (1.0 / (1.0 - BETA_ONE ** ADAM_STEP))
    v_hat = v_val * (1.0 / (1.0 - BETA_TWO ** ADAM_STEP))
    w_val = w_old[...]
    w_val = w_val - learn_rate * (m_hat / (jnp.sqrt(v_hat) + ADAM_EPS) + WEIGHT_DECAY * w_val)
    m_new[...] = m_val
    v_new[...] = v_val
    w_new[...] = w_val
    wide[...] = w_val

    for of_core in range(2):
        @pl.when(core == of_core)
        def _(of_core=of_core):
            @pl.when(step >= 2)
            def _():
                n_copy(step - 2, of_core).wait()
            buf, per_row = (n_one, d_ff // 128) if of_core == 0 else (n_two, d_model // 128)
            for j in range(per_row):
                buf[par, :, j * 128:(j + 1) * 128] = wide[pl.ds(j, buf.shape[1], per_row), :].astype(BF16)
            n_copy(step, of_core).start()

            @pl.when(step == steps - 1)
            def _():
                n_copy(step - 1, of_core).wait()
                n_copy(step, of_core).wait()


def run_update(learn_rate, grad, clip, w_old, m_old, v_old):
    _, d_model, d_ff = grad.shape
    rows1, rows2 = FLAT_ROWS * 128 // d_ff, FLAT_ROWS * 128 // d_model
    steps = w_old.shape[0] // FLAT_ROWS
    flat_spec = pl.BlockSpec((FLAT_ROWS, 128), lambda i: (i, 0))
    flat_shape = jax.ShapeDtypeStruct(w_old.shape, F32)
    return pl.pallas_call(
        functools.partial(update_kernel, learn_rate),
        name="update",
        grid=(steps,),
        out_shape=[flat_shape] * 3 + [jax.ShapeDtypeStruct((2, d_model, d_ff), BF16), jax.ShapeDtypeStruct((2, d_ff, d_model), BF16)],
        in_specs=[ANY, pl.BlockSpec((8, 128), lambda i: (0, 0))] + [flat_spec] * 3,
        out_specs=[flat_spec] * 3 + [ANY, ANY],
        scratch_shapes=[
            pltpu.VMEM((2, rows1, d_ff), F32),
            pltpu.VMEM((2, d_model, rows2), F32),
            pltpu.VMEM((FLAT_ROWS, 128), F32),
            pltpu.VMEM((FLAT_ROWS, 128), F32),
            pltpu.VMEM((2, rows1, d_ff), BF16),
            pltpu.VMEM((2, rows2, d_model), BF16),
            pltpu.SemaphoreType.DMA((2,)),
            pltpu.SemaphoreType.DMA((2,)),
        ],
        compiler_params=pltpu.CompilerParams(dimension_semantics=("arbitrary",), vmem_limit_bytes=60 * 2**20),
        cost_estimate=pl.CostEstimate(flops=10**9, bytes_accessed=150 * 2**20, transcendentals=0),
    )(grad, clip, w_old, m_old, v_old)


def merge_kernel(w1_half, w2_half, w1_got, w2_got, w1_new, w2_new, buf1, buf2, in_sem, out_sem):
    del w1_half, w2_half
    core = lax.axis_index("data")
    for of_core, got, new, buf in ((1, w1_got, w1_new, buf1), (0, w2_got, w2_new, buf2)):
        parts = [(half, slot) for half in range(2) for slot in range(MERGE_PARTS)]
        rows = buf.shape[1]

        @pl.when(core == of_core)
        def _(parts=parts, rows=rows, got=got, new=new, buf=buf):
            ins, outs = [], []
            for n, (half, slot) in enumerate(parts):
                where = pl.ds(slot * rows, rows)
                ins.append(pltpu.make_async_copy(got.at[half, where, :], buf.at[n], in_sem.at[n]))
                outs.append(pltpu.make_async_copy(buf.at[n], new.at[half, where, :], out_sem.at[n]))
            for cp in ins:
                cp.start()
            for cp_in, cp_out in zip(ins, outs):
                cp_in.wait()
                cp_out.start()
            for cp in outs:
                cp.wait()


MERGE_PARTS = 4


def run_merge(w1_half, w2_half, w1_got, w2_got):
    _, d_model, d_ff = w1_half.shape
    n = 2 * MERGE_PARTS
    return pl.pallas_call(
        merge_kernel,
        name="merge",
        out_shape=[jax.ShapeDtypeStruct(w1_half.shape, BF16), jax.ShapeDtypeStruct(w2_half.shape, BF16)],
        in_specs=[ANY] * 4,
        out_specs=[ANY] * 2,
        input_output_aliases={0: 0, 1: 1},
        scratch_shapes=[
            pltpu.VMEM((n, d_model // MERGE_PARTS, d_ff), BF16),
            pltpu.VMEM((n, d_ff // MERGE_PARTS, d_model), BF16),
            pltpu.SemaphoreType.DMA((n,)),
            pltpu.SemaphoreType.DMA((n,)),
        ],
        compiler_params=pltpu.CompilerParams(vmem_limit_bytes=40 * 2**20),
    )(w1_half, w2_half, w1_got, w2_got)


def solution(mesh):
    n_stage = mesh.shape["stage"]
    n_data = mesh.shape["data"]
    axes = ("stage", "data")

    def device(stage, core):
        return stage * n_data + core

    def from_core(core):
        return [(device(s, core), device(s, 1 - core)) for s in range(n_stage)]

    def device_step(x_loc, t_loc, w1_loc, w2_loc, wm_loc, m_loc, v_loc):
        n_micro, n_tok, d_model = x_loc.shape
        d_ff = w1_loc.shape[4]
        n_tokens = n_micro * n_tok * n_data
        n_blocks = 2 * n_stage
        n_rows = n_micro * n_tok // n_stage
        tau_clip = 0.3 * d_model * math.sqrt(n_blocks * (3.0 / n_tokens + 0.008))
        learn_rate = 0.1 / math.sqrt(4.0 * d_model * n_blocks)
        w1 = w1_loc.reshape(2, d_model, d_ff)
        w2 = w2_loc.reshape(2, d_ff, d_model)
        flat_rows = (n_micro * n_tok, d_model)
        wg1, wg2, saved, u_all, seed, loss_acc = run_forward(n_tokens, x_loc.reshape(flat_rows), t_loc.reshape(flat_rows), w1, w2, n_rows)
        weights = (w1, w2, wg1, wg2)
        _, _, _, total, squares = run_backward(seed, saved, u_all, weights)
        clip, loss_all = run_scalars(tau_clip, squares, loss_acc)
        flat = [val.reshape(-1, 128) for val in (wm_loc, m_loc, v_loc)]
        w_new, m_new, v_new, w1_half, w2_half = run_update(learn_rate, total, clip, *flat)
        w1_got = lax.ppermute(w1_half, axes, from_core(0))
        w2_got = lax.ppermute(w2_half, axes, from_core(1))
        w1_new, w2_new = run_merge(w1_half, w2_half, w1_got, w2_got)
        mean_loss = loss_all[0, 0] / n_tokens
        return w1_new.reshape(w1_loc.shape), w2_new.reshape(w2_loc.shape), w_new.reshape(wm_loc.shape), m_new.reshape(wm_loc.shape), v_new.reshape(wm_loc.shape), mean_loss

    act_spec = P(None, "data", None)
    flat_spec = P("stage", None, None, "data")
    return jax.shard_map(device_step, mesh=mesh, in_specs=(act_spec, act_spec, P("stage"), P("stage"), flat_spec, flat_spec, flat_spec), out_specs=(P("stage"), P("stage"), flat_spec, flat_spec, flat_spec, P()), check_vma=False)
```

```python
import functools
import math
import jax
import jax.numpy as jnp
from jax import lax
from jax.experimental import pallas as pl
from jax.experimental.pallas import tpu as pltpu
from jax.sharding import PartitionSpec as P

BETA_ONE = 0.9
BETA_TWO = 0.999
ADAM_EPS = 1e-8
WEIGHT_DECAY = 0.1
ADAM_STEP = 1000
GELU_A = math.sqrt(2.0 / math.pi)
GELU_B = GELU_A * 0.044715
MESH = pl.DeviceIdType.MESH
ANY = pl.BlockSpec(memory_space=pl.ANY)
F32 = jnp.float32
BF16 = jnp.bfloat16

TILE = 512
PATH_PIECES = 4


def _dot_t(lhs, rhs):
    return lax.dot_general(lhs, rhs, (((1,), (1,)), ((), ())), preferred_element_type=F32)


def _dot(lhs, rhs):
    return jnp.dot(lhs, rhs, preferred_element_type=F32)


SEND_SLOT = (-45, -30, -28, -20)
HOP_SLOT = {1: (-27, -20, -18, -14), 2: (-18, -14, -8, -6), 3: (-12, -9, -2, -2)}
LOAD_SLOT = -1


def forward_kernel(n_blocks, tiles, n_tokens, x_hbm, t_hbm, w1_loc, w2_loc, wg1, wg2, saved, u_out, seed, loss,
                   act, w1_buf, w2_buf, u_buf, acc, t_buf, s_buf,
                   x_sem, act_sem, u_sem, w_sem, t_sem, s_sem, ici_send, ici_recv, d2d_send, d2d_recv):
    me = lax.axis_index("stage")
    core = lax.axis_index("data")
    d_model, d_ff = w1_loc.shape[1], w1_loc.shape[2]
    n_rows = act.shape[0]
    n_piece = 4 * PATH_PIECES
    rows1, rows2 = d_model // n_piece, d_ff // n_piece

    def peer(flip):
        bit0, bit1 = lax.rem(me, 2), me // 2
        return (1 - bit0 + 2 * bit1) if flip == 1 else (bit0 + 2 * (1 - bit1))

    def rel_of(blk):
        own = lax.rem(blk, 4)
        a0, a1, b0, b1 = lax.rem(me, 2), me // 2, lax.rem(own, 2), own // 2
        return (a0 + b0 - 2 * a0 * b0) + 2 * (a1 + b1 - 2 * a1 * b1)

    def piece(j, path, of_core):
        return j * 4 + path * 2 + of_core

    def views(blk, idx):
        return (wg1.at[blk, pl.ds(pl.multiple_of(idx * rows1, 16), rows1), :],
                wg2.at[blk, pl.ds(pl.multiple_of(idx * rows2, 64), rows2), :])

    def local_views(blk, idx):
        half = blk // 4
        return (w1_loc.at[half, pl.ds(pl.multiple_of(idx * rows1, 16), rows1), :],
                w2_loc.at[half, pl.ds(pl.multiple_of(idx * rows2, 64), rows2), :])

    def ici_copies(blk, path, j, sources, flip):
        idx = piece(j, path, core)
        slot = path * PATH_PIECES + j
        return [pltpu.make_async_remote_copy(
            src_ref=src, dst_ref=dst, send_sem=ici_send.at[blk, slot, m], recv_sem=ici_recv.at[blk, slot, m],
            device_id=(peer(flip), core), device_id_type=MESH)
            for m, (src, dst) in enumerate(zip(sources, views(blk, idx)))]

    def d2d_copies(blk, path, j, of_core):
        idx = piece(j, path, of_core)
        slot = path * PATH_PIECES + j
        return [pltpu.make_async_remote_copy(
            src_ref=ref, dst_ref=ref, send_sem=d2d_send.at[blk, slot, m], recv_sem=d2d_recv.at[blk, slot, m],
            device_id=(me, 1 - core), device_id_type=MESH) for m, ref in enumerate(views(blk, idx))]

    def first_flip(path):
        return 1 if path == 0 else 2

    def own_send(blk, j):
        @pl.when(rel_of(blk) == 0)
        def _():
            for path in range(2):
                for cp in ici_copies(blk, path, j, local_views(blk, piece(j, path, core)), first_flip(path)):
                    cp.start()

    def hop_event(blk, hop, j):
        rel = rel_of(blk)
        for path in range(2):
            at_rel = {1: (1, 2), 2: (3, 3), 3: (2, 1)}[hop][path]

            @pl.when(rel == at_rel)
            def _(path=path):
                flip = first_flip(path)
                if hop == 1:
                    flip = 3 - flip
                copies = ici_copies(blk, path, j, views(blk, piece(j, path, core)), flip)
                for cp in copies:
                    cp.wait_recv()
                if hop < 3:
                    for cp in copies:
                        cp.start()
                for cp in d2d_copies(blk, path, j, core):
                    cp.start()

    def weight_loads(blk, par, is_own):
        half = blk // 4
        src1, src2 = (w1_loc.at[half], w2_loc.at[half]) if is_own else (wg1.at[blk], wg2.at[blk])
        return [pltpu.make_async_copy(src1, w1_buf.at[par], w_sem.at[par, 0]),
                pltpu.make_async_copy(src2, w2_buf.at[par], w_sem.at[par, 1])]

    def load_event(blk):
        rel = rel_of(blk)
        par = lax.rem(blk, 2)

        @pl.when(rel == 0)
        def _():
            for cp in weight_loads(blk, par, True):
                cp.start()

        @pl.when(rel != 0)
        def _():
            for path in range(2):
                for j in range(PATH_PIECES):
                    for cp in d2d_copies(blk, path, j, 1 - core):
                        cp.wait_recv()
            for cp in weight_loads(blk, par, False):
                cp.start()

    def x_copy():
        return pltpu.make_async_copy(x_hbm.at[pl.ds(pl.multiple_of(me * n_rows, n_rows), n_rows), :], act, x_sem)

    def act_copy(slot, tile):
        rows = pl.ds(pl.multiple_of(tile * TILE, TILE), TILE)
        return pltpu.make_async_copy(act.at[rows, :], saved.at[slot, rows, :], act_sem.at[tile])

    def t_copy(tile):
        return pltpu.make_async_copy(t_hbm.at[pl.ds(pl.multiple_of(me * n_rows + tile * TILE, TILE), TILE), :], t_buf, t_sem)

    def seed_copy(tile):
        return pltpu.make_async_copy(s_buf, seed.at[pl.ds(pl.multiple_of(tile * TILE, TILE), TILE), :], s_sem)

    def u_copy(blk, tile, par):
        rows = pl.ds(pl.multiple_of(tile * TILE, TILE), TILE)
        return pltpu.make_async_copy(u_buf.at[par], u_out.at[blk, rows, :], u_sem.at[par])

    barrier = pltpu.get_barrier_semaphore()
    for target in ((peer(1), core), (peer(2), core), (me, 1 - core)):
        pl.semaphore_signal(barrier, inc=1, device_id=target, device_id_type=MESH)
    x_copy().start()
    pl.semaphore_wait(barrier, 3)

    events = []
    for hop in (3, 2, 1):
        for j in range(PATH_PIECES):
            events.append((HOP_SLOT[hop][j], functools.partial(lambda blk, hop, j: hop_event(blk, hop, j), hop=hop, j=j)))
    for j in range(PATH_PIECES):
        events.append((SEND_SLOT[j], functools.partial(lambda blk, j: own_send(blk, j), j=j)))
    events.append((LOAD_SLOT, load_event))

    def comm_slot(blk, tile):
        for offset, fn in events:
            residue = offset % tiles
            ahead = (residue - offset) // tiles
            target = blk + ahead

            @pl.when((tile == residue) & (target >= 0) & (target < n_blocks))
            def _(fn=fn, target=target):
                fn(target)

    def compute(blk, tile):
        par = lax.rem(blk, 2)
        u_par = lax.rem(tile, 2)
        rows = pl.ds(pl.multiple_of(tile * TILE, TILE), TILE)

        @pl.when(tile == 0)
        def _():
            for cp in weight_loads(blk, par, True):
                cp.wait()

        @pl.when((blk == 0) & (tile == 0))
        def _():
            x_copy().wait()
            for t in range(tiles):
                act_copy(0, t).start()

        @pl.when((blk > 0) | (tile > 1))
        def _():
            u_copy(blk, tile, u_par).wait()

        @pl.when(blk == n_blocks - 1)
        def _():
            t_copy(tile).start()

        act_copy(blk, tile).wait()
        x = act[rows, :]
        chunk = 256
        n_chunk = d_ff // chunk
        for f in range(n_chunk):
            cols = slice(f * chunk, (f + 1) * chunk)
            u = _dot(x, w1_buf[par, :, cols])
            u_buf[u_par, :, cols] = u
            inner = u * (GELU_A + GELU_B * (u * u))
            a = (u * (0.5 + 0.5 * jnp.tanh(inner))).astype(BF16)
            part = _dot(a, w2_buf[par, cols, :])
            if f == 0:
                acc[...] = part
            elif f < n_chunk - 1:
                acc[...] += part
            else:
                act[rows, :] = (x.astype(F32) + (acc[...] + part)).astype(BF16)
        u_copy(blk, tile, u_par).start()

        @pl.when(blk < n_blocks - 1)
        def _():
            act_copy(blk + 1, tile).start()

        @pl.when(blk == n_blocks - 1)
        def _():
            t_copy(tile).wait()

            @pl.when(tile > 0)
            def _():
                seed_copy(tile - 1).wait()
            residual = act[rows, :].astype(F32) - t_buf[...].astype(F32)
            s_buf[...] = (residual / n_tokens).astype(BF16)
            squares = jnp.sum((residual * residual).reshape(TILE // 8, 8, residual.shape[1]), axis=0)
            folded = squares[:, :128]
            for j in range(1, residual.shape[1] // 128):
                folded = folded + squares[:, j * 128:(j + 1) * 128]
            loss[...] += 0.5 * folded
            seed_copy(tile).start()

    lead = -(min(SEND_SLOT) // tiles)
    loss[...] = jnp.zeros_like(loss)

    @pl.loop(0, (n_blocks + lead) * tiles)
    def _(step):
        blk = step // tiles - lead
        tile = lax.rem(step, tiles)
        comm_slot(blk, tile)

        @pl.when(blk >= 0)
        def _():
            compute(blk, tile)

    for par in range(2):
        u_copy(0, 0, par).wait()
    seed_copy(0).wait()

    @pl.loop(0, n_blocks)
    def _(blk):
        rel = rel_of(blk)
        for path in range(2):
            last = (2, 1)[path]

            @pl.when(rel != last)
            def _(path=path):
                for j in range(PATH_PIECES):
                    for cp in ici_copies(blk, path, j, views(blk, piece(j, path, core)), 1):
                        cp.wait_send()

        @pl.when(rel != 0)
        def _():
            for path in range(2):
                for j in range(PATH_PIECES):
                    for cp in d2d_copies(blk, path, j, core):
                        cp.wait_send()


def run_forward(n_tokens, x_flat, t_flat, w1_loc, w2_loc, n_rows):
    n_half, d_model, d_ff = w1_loc.shape
    n_blocks = 4 * n_half
    tiles = n_rows // TILE
    slots = 2 * PATH_PIECES
    out_shape = [
        jax.ShapeDtypeStruct((n_blocks, d_model, d_ff), BF16),
        jax.ShapeDtypeStruct((n_blocks, d_ff, d_model), BF16),
        jax.ShapeDtypeStruct((n_blocks, n_rows, d_model), BF16),
        jax.ShapeDtypeStruct((n_blocks, n_rows, d_ff), F32),
        jax.ShapeDtypeStruct((n_rows, d_model), BF16),
        jax.ShapeDtypeStruct((8, 128), F32),
    ]
    return pl.pallas_call(
        functools.partial(forward_kernel, n_blocks, tiles, n_tokens),
        name="forward",
        out_shape=out_shape,
        in_specs=[ANY] * 4,
        out_specs=[ANY] * 5 + [pl.BlockSpec(memory_space=pltpu.VMEM)],
        scratch_shapes=[
            pltpu.VMEM((n_rows, d_model), BF16),
            pltpu.VMEM((2, d_model, d_ff), BF16),
            pltpu.VMEM((2, d_ff, d_model), BF16),
            pltpu.VMEM((2, TILE, d_ff), F32),
            pltpu.VMEM((TILE, d_model), F32),
            pltpu.VMEM((TILE, d_model), BF16),
            pltpu.VMEM((TILE, d_model), BF16),
            pltpu.SemaphoreType.DMA(()),
            pltpu.SemaphoreType.DMA((tiles,)),
            pltpu.SemaphoreType.DMA((2,)),
            pltpu.SemaphoreType.DMA((2, 2)),
            pltpu.SemaphoreType.DMA(()),
            pltpu.SemaphoreType.DMA(()),
            pltpu.SemaphoreType.DMA((n_blocks, slots, 2)),
            pltpu.SemaphoreType.DMA((n_blocks, slots, 2)),
            pltpu.SemaphoreType.DMA((n_blocks, slots, 2)),
            pltpu.SemaphoreType.DMA((n_blocks, slots, 2)),
        ],
        compiler_params=pltpu.CompilerParams(collective_id=0, has_side_effects=True, vmem_limit_bytes=60 * 2**20),
        cost_estimate=pl.CostEstimate(flops=4 * n_blocks * n_rows * d_model * d_ff, bytes_accessed=600 * 2**20, transcendentals=0),
    )(x_flat, t_flat, w1_loc, w2_loc)


RING = 5
CHUNK = 512
PIECE = 256


def _relation(me, blk):
    own = lax.rem(blk, 4)
    a0, a1, b0, b1 = lax.rem(me, 2), me // 2, lax.rem(own, 2), own // 2
    return (a0 + b0 - 2 * a0 * b0) + 2 * (a1 + b1 - 2 * a1 * b1)


def _tile_rows(tile):
    return pl.ds(pl.multiple_of(tile * TILE, TILE), TILE)


def _gelu_grad(u):
    cube = GELU_B * (u * u)
    th = jnp.tanh(u * (GELU_A + cube))
    cdf = 0.5 + 0.5 * th
    a = u * cdf
    return a, cdf + (a * (3.0 - 3.0 * th)) * (cube + GELU_A / 3.0)


STAGE_TILE = (0, 3, 5, 8)
SENDS = 3


def backward_kernel(n_blocks, tiles, g_hbm, saved, u_hbm, w1_loc, w2_loc, wg1, wg2, local, sib, inbox, own, squares,
                    act, w1_buf, w2_buf, dw, u_buf, x_buf, x_t, g_t, acc, q_buf, k_buf, s_buf, r_buf, o_buf,
                    g_sem, w_sem, u_sem, x_sem, keep_sem, d2d_send, d2d_recv, load_sem, own_sem, ici_send, ici_recv):
    me = lax.axis_index("stage")
    core = lax.axis_index("data")
    d_model, d_ff = act.shape[1], w1_buf.shape[1]
    n_chunk = d_ff // CHUNK
    n_pair = n_chunk // 2
    n_slot = d_ff // PIECE // 2
    steps = n_blocks * tiles
    total = steps * n_chunk
    top = n_blocks - 1

    def cols_of(f):
        return pl.ds(pl.multiple_of(f * CHUNK, CHUNK), CHUNK)

    def pair_of(p):
        return pl.ds(pl.multiple_of(p * 2 * CHUNK, 2 * CHUNK), 2 * CHUNK)

    def pieces_of(f):
        return pl.ds(f * (CHUNK // PIECE), CHUNK // PIECE)

    def weight_copies(blk, pair, is_own):
        half = blk // 4
        src1, src2 = (w1_loc.at[half], w2_loc.at[half]) if is_own else (wg1.at[blk], wg2.at[blk])
        cols = pair_of(pair)
        return [pltpu.make_async_copy(src1.at[:, cols], w1_buf.at[:, cols], w_sem.at[pair, 0]),
                pltpu.make_async_copy(src2.at[cols, :], w2_buf.at[cols, :], w_sem.at[pair, 1])]

    def start_weights(blk, pair):
        rel = _relation(me, blk)

        @pl.when(rel == 0)
        def _():
            for cp in weight_copies(blk, pair, True):
                cp.start()

        @pl.when(rel != 0)
        def _():
            for cp in weight_copies(blk, pair, False):
                cp.start()

    def u_copy(step):
        blk = top - step // (tiles * n_chunk)
        tile = lax.rem(step // n_chunk, tiles)
        f = lax.rem(step, n_chunk)
        slot = lax.rem(step, RING)
        return pltpu.make_async_copy(u_hbm.at[blk, _tile_rows(tile), cols_of(f)], u_buf.at[slot], u_sem.at[slot])

    def x_copy(bt):
        par = lax.rem(bt, 2)
        return pltpu.make_async_copy(saved.at[top - bt // tiles, _tile_rows(lax.rem(bt, tiles)), :], x_buf.at[par], x_sem.at[par])

    def g_in_copy():
        return pltpu.make_async_copy(g_hbm, act, g_sem)

    def keep_copy(j, f):
        return pltpu.make_async_copy(dw.at[core, pieces_of(f)], local.at[lax.rem(j, 3), pieces_of(f)], keep_sem.at[f])

    def give_copy(j, c):
        return pltpu.make_async_remote_copy(
            src_ref=dw.at[1 - core, c], dst_ref=sib.at[j, c], send_sem=d2d_send.at[c],
            recv_sem=d2d_recv.at[j, c], device_id=(me, 1 - core), device_id_type=MESH)

    def stages_of(j):
        rel = _relation(me, top - j)
        return [jnp.where(rel == 0, 3, jnp.where(rel == 3, 1, jnp.where(rel == last, 0, 2))) for last in (2, 1)]

    def next_chip(stage, path):
        first = 1 if path == 0 else 2
        flip = jnp.where(stage == 1, 3 - first, first)
        bit0, bit1 = lax.rem(me, 2), me // 2
        return jnp.where(flip == 1, 1 - bit0 + 2 * bit1, bit0 + 2 * (1 - bit1))

    def piece_loads(j, c, buf):
        return [pltpu.make_async_copy(local.at[lax.rem(j, 3), c], k_buf.at[buf], load_sem.at[buf, 0]),
                pltpu.make_async_copy(sib.at[j, c], s_buf.at[buf], load_sem.at[buf, 1])]

    def inbox_load(j, c, buf):
        return pltpu.make_async_copy(inbox.at[j, c], r_buf.at[buf], load_sem.at[buf, 2])

    def own_copy(j, c, buf):
        return pltpu.make_async_copy(k_buf.at[buf], own.at[(top - j) // 4, c], own_sem.at[buf])

    def pass_copy(j, m, buf, stage, path):
        slot = lax.rem(m, SENDS)
        c = 2 * m + path
        return pltpu.make_async_remote_copy(
            src_ref=o_buf.at[buf, slot], dst_ref=inbox.at[j, c], send_sem=ici_send.at[buf, slot],
            recv_sem=ici_recv.at[j, c], device_id=(next_chip(stage, path), core), device_id_type=MESH)

    def first_piece(stage):
        return jnp.where(stage == 0, STAGE_TILE[0], jnp.where(stage == 1, STAGE_TILE[1], jnp.where(stage == 2, STAGE_TILE[2], STAGE_TILE[3])))

    def load_pieces(j, tile):
        live = (j >= 0) & (j < n_blocks)
        for path, (stage, before) in enumerate(zip(stages_of(j), stages_of(j - 2))):
            m = tile - first_piece(stage)

            @pl.when(live & (m >= 0) & (m < n_slot))
            def _(path=path, stage=stage, before=before, m=m):
                buf = lax.rem(j, 2) * 2 + path
                c = 2 * m + path

                @pl.when(((m >= 1) & (stage == 3)) | ((m == 0) & (j >= 2) & (before == 3)))
                def _():
                    own_copy(j, c, buf).wait()
                give_copy(j, c).wait_recv()
                for cp in piece_loads(j, c, buf):
                    cp.start()

                @pl.when(stage > 0)
                def _():
                    pass_copy(j, m, buf, stage, path).wait_recv()
                    inbox_load(j, c, buf).start()

    def sum_pieces(j, tile):
        live = (j >= 0) & (j < n_blocks)
        for path, (stage, before) in enumerate(zip(stages_of(j), stages_of(j - 2))):
            m = tile - first_piece(stage)

            @pl.when(live & (m >= 0) & (m < n_slot))
            def _(path=path, stage=stage, before=before, m=m):
                buf = lax.rem(j, 2) * 2 + path
                slot = lax.rem(m, SENDS)
                c = 2 * m + path

                @pl.when(((m >= SENDS) & (stage < 3)) | ((m < SENDS) & (j >= 2) & (before < 3)))
                def _():
                    pass_copy(j, m, buf, stage, path).wait_send()
                for cp in piece_loads(j, c, buf):
                    cp.wait()

                @pl.when(stage == 0)
                def _():
                    o_buf[buf, slot] = (k_buf[buf] + s_buf[buf]).astype(BF16)

                @pl.when(stage > 0)
                def _():
                    inbox_load(j, c, buf).wait()

                @pl.when((stage == 1) | (stage == 2))
                def _():
                    o_buf[buf, slot] = ((k_buf[buf] + s_buf[buf]) + r_buf[buf].astype(F32)).astype(BF16)

                @pl.when(stage < 3)
                def _():
                    pass_copy(j, m, buf, stage, path).start()

                @pl.when(stage == 3)
                def _():
                    val = (k_buf[buf] + s_buf[buf]) + r_buf[buf].astype(F32)
                    k_buf[buf] = val
                    part = jnp.sum((val * val).reshape(d_model // 8, 8, PIECE), axis=0)
                    squares[...] += part[:, :128] + part[:, 128:]
                    own_copy(j, c, buf).start()

    barrier = pltpu.get_barrier_semaphore()
    bit0, bit1 = lax.rem(me, 2), me // 2
    near = ((1 - bit0 + 2 * bit1, core), (bit0 + 2 * (1 - bit1), core), (me, 1 - core))
    for target in near:
        pl.semaphore_signal(barrier, inc=1, device_id=target, device_id_type=MESH)
    g_in_copy().start()
    for pair in range(n_pair):
        start_weights(jnp.int32(top), jnp.int32(pair))
    x_copy(0).start()
    x_copy(1).start()
    for step in range(RING - 2):
        u_copy(step).start()
    squares[...] = jnp.zeros_like(squares)
    pl.semaphore_wait(barrier, 3)
    g_in_copy().wait()
    x_copy(0).wait()
    x_t[0] = x_buf[0].T
    g_t[0] = act[pl.ds(0, TILE), :].T
    weight_copies(0, 0, True)[1].wait()
    q_buf[0] = _dot_t(act[pl.ds(0, TILE), :], w2_buf[pl.ds(0, CHUNK), :])

    def compute(n):
        bt = n // n_pair
        pair = lax.rem(n, n_pair)
        i = bt // tiles
        tile = lax.rem(bt, tiles)
        blk = top - i
        t_par = lax.rem(bt, 2)
        rows = _tile_rows(tile)
        next_rows = _tile_rows(lax.rem(tile + 1, tiles))

        @pl.when((pair == 0) & (bt + 1 < steps))
        def _():
            x_copy(bt + 1).wait()

        @pl.when((pair == 0) & (bt + 2 < steps))
        def _():
            x_copy(bt + 2).start()

        @pl.when(pair == 0)
        def _():
            acc[...] = act[rows, :].astype(F32)

        def chunk_prep(f, step):
            @pl.when(step + RING - 2 < total)
            def _():
                u_copy(step + RING - 2).start()
            u_copy(step).wait()

            @pl.when((tile == 0) & (i > 0))
            def _():
                keep_copy(i - 1, f).wait()
                for c in (2 * f, 2 * f + 1):
                    give_copy(i - 1, c).wait_send()

        def chunk_main(f, step, q_par, next_g, next_w2, with_input_grad):
            cols = cols_of(f)
            q_buf[1 - q_par] = _dot_t(next_g, next_w2)
            a, slope = _gelu_grad(u_buf[lax.rem(step, RING)])
            r = (q_buf[q_par] * slope).astype(BF16)
            for m, val in enumerate((_dot(x_t[t_par], r), _dot(g_t[t_par], a.astype(BF16)))):
                for part in range(CHUNK // PIECE):
                    c = f * (CHUNK // PIECE) + part
                    dw[m, c] = jnp.where(tile == 0, 0.0, dw[m, c]) + val[:, part * PIECE:(part + 1) * PIECE]
            if with_input_grad:
                acc[...] += _dot_t(r, w1_buf[:, cols])

        def pair_step(with_input_grad):
            f0 = pair * 2
            step = bt * n_chunk + f0
            last = pair == n_pair - 1
            chunk_prep(f0, step)
            chunk_prep(f0 + 1, step + 1)

            @pl.when(tile == 0)
            def _():
                weight_copies(0, pair, True)[0].wait()

            @pl.when((tile == 0) & (pair < n_pair - 1))
            def _():
                weight_copies(0, pair + 1, True)[1].wait()

            @pl.when(last & (tile == tiles - 1) & (bt + 1 < steps))
            def _():
                weight_copies(0, jnp.int32(0), True)[1].wait()

            q_rows = _tile_rows(jnp.where(last, lax.rem(tile + 1, tiles), tile))
            next_f = jnp.where(last, 0, f0 + 2)
            third = pl.ds(pl.multiple_of(pair * 256, 256), 256)
            chunk_main(f0, step, 0, act[rows, :], w2_buf[cols_of(f0 + 1), :], with_input_grad)
            x_t[1 - t_par, third, :] = x_buf[1 - t_par, :, third].T
            g_t[1 - t_par, third, :] = act[next_rows, third].T
            chunk_main(f0 + 1, step + 1, 1, act[q_rows, :], w2_buf[cols_of(next_f), :], with_input_grad)

            @pl.when(tile == tiles - 1)
            def _():
                for f in (f0, f0 + 1):
                    keep_copy(i, f).start()
                    for c in (2 * f, 2 * f + 1):
                        give_copy(i, c).start()

            if with_input_grad:
                @pl.when(tile == tiles - 1)
                def _():
                    start_weights(blk - 1, pair)

        @pl.when(blk > 0)
        def _():
            pair_step(True)

            @pl.when(pair == n_pair - 1)
            def _():
                act[rows, :] = acc[...].astype(BF16)

        @pl.when(blk == 0)
        def _():
            pair_step(False)

    span = tiles * n_pair
    all_steps = n_blocks * span

    @pl.loop(0, all_steps + (STAGE_TILE[3] + n_slot) * n_pair)
    def _(n):
        i = n // span
        tile = lax.rem(n, span) // n_pair
        phase = lax.rem(n, n_pair)

        @pl.when(n < all_steps)
        def _():
            compute(n)

        @pl.when(n == all_steps)
        def _():
            for f in range(n_chunk):
                keep_copy(top, f).wait()
                for c in (2 * f, 2 * f + 1):
                    give_copy(top, c).wait_send()

        @pl.when((phase == 0) & (i > 0))
        def _():
            load_pieces(i - 2, tile + tiles)
            load_pieces(i - 1, tile)

        @pl.when((phase == 1) & (i > 0))
        def _():
            sum_pieces(i - 2, tile + tiles)
            sum_pieces(i - 1, tile)

    for j in (n_blocks - 2, n_blocks - 1):
        for path, stage in enumerate(stages_of(j)):
            buf = j % 2 * 2 + path

            @pl.when(stage == 3)
            def _(j=j, path=path, buf=buf):
                own_copy(j, path, buf).wait()

            @pl.when(stage < 3)
            def _(j=j, path=path, buf=buf, stage=stage):
                for m in range(SENDS):
                    pass_copy(j, m, buf, stage, path).wait_send()


def run_backward(grad, saved, u_all, weights):
    n_rows, d_model = grad.shape
    n_half, _, d_ff = weights[0].shape
    n_blocks = 4 * n_half
    tiles = n_rows // TILE
    n_chunk = d_ff // CHUNK
    n_piece = d_ff // PIECE
    pieces = (n_piece, d_model, PIECE)
    return pl.pallas_call(
        functools.partial(backward_kernel, n_blocks, tiles),
        name="backward",
        out_shape=[
            jax.ShapeDtypeStruct((3,) + pieces, F32),
            jax.ShapeDtypeStruct((n_blocks,) + pieces, F32),
            jax.ShapeDtypeStruct((n_blocks,) + pieces, BF16),
            jax.ShapeDtypeStruct((n_half,) + pieces, F32),
            jax.ShapeDtypeStruct((8, 128), F32),
        ],
        in_specs=[ANY] * 7,
        out_specs=[ANY] * 4 + [pl.BlockSpec(memory_space=pltpu.VMEM)],
        scratch_shapes=[
            pltpu.VMEM((n_rows, d_model), BF16),
            pltpu.VMEM((d_model, d_ff), BF16),
            pltpu.VMEM((d_ff, d_model), BF16),
            pltpu.VMEM((2,) + pieces, F32),
            pltpu.VMEM((RING, TILE, CHUNK), F32),
            pltpu.VMEM((2, TILE, d_model), BF16),
            pltpu.VMEM((2, d_model, TILE), BF16),
            pltpu.VMEM((2, d_model, TILE), BF16),
            pltpu.VMEM((TILE, d_model), F32),
            pltpu.VMEM((2, TILE, CHUNK), F32),
            pltpu.VMEM((4, d_model, PIECE), F32),
            pltpu.VMEM((4, d_model, PIECE), F32),
            pltpu.VMEM((4, d_model, PIECE), BF16),
            pltpu.VMEM((4, SENDS, d_model, PIECE), BF16),
            pltpu.SemaphoreType.DMA(()),
            pltpu.SemaphoreType.DMA((n_chunk // 2, 2)),
            pltpu.SemaphoreType.DMA((RING,)),
            pltpu.SemaphoreType.DMA((2,)),
            pltpu.SemaphoreType.DMA((n_chunk,)),
            pltpu.SemaphoreType.DMA((n_piece,)),
            pltpu.SemaphoreType.DMA((n_blocks, n_piece)),
            pltpu.SemaphoreType.DMA((4, 3)),
            pltpu.SemaphoreType.DMA((4,)),
            pltpu.SemaphoreType.DMA((4, SENDS)),
            pltpu.SemaphoreType.DMA((n_blocks, n_piece)),
        ],
        compiler_params=pltpu.CompilerParams(collective_id=1, has_side_effects=True, vmem_limit_bytes=67043328),
        cost_estimate=pl.CostEstimate(flops=8 * n_blocks * n_rows * d_model * d_ff, bytes_accessed=800 * 2**20, transcendentals=0),
    )(grad, saved, u_all, *weights)


def scalars_kernel(tau_clip, squares, loss, clip_out, loss_out, mine, gathered, send_sem, recv_sem):
    stage = lax.axis_index("stage")
    core = lax.axis_index("data")
    n_dev = gathered.shape[0]
    here = stage * 2 + core
    barrier = pltpu.get_barrier_semaphore()
    for k in range(1, n_dev):
        other = lax.rem(here + k, n_dev)
        pl.semaphore_signal(barrier, inc=1, device_id=(other // 2, lax.rem(other, 2)), device_id_type=MESH)
    mine[0] = squares[...]
    mine[1] = loss[...]
    gathered[here] = mine[...]
    pl.semaphore_wait(barrier, n_dev - 1)

    def copy(k, slot):
        other = lax.rem(here + k, n_dev)
        return pltpu.make_async_remote_copy(
            src_ref=mine, dst_ref=gathered.at[slot], send_sem=send_sem.at[k], recv_sem=recv_sem.at[k],
            device_id=(other // 2, lax.rem(other, 2)), device_id_type=MESH)

    for k in range(1, n_dev):
        copy(k, here).start()
    for k in range(1, n_dev):
        copy(k, lax.rem(here + n_dev - k, n_dev)).wait_recv()
    sums = jnp.sum(gathered[...], axis=0)
    squared = jnp.sum(jnp.sum(sums[0], axis=0, keepdims=True), axis=1, keepdims=True)
    lost = jnp.sum(jnp.sum(sums[1], axis=0, keepdims=True), axis=1, keepdims=True)
    norm = jnp.sqrt(jnp.broadcast_to(squared, (8, 128)))
    clip_out[...] = jnp.minimum(1.0, tau_clip / norm)
    loss_out[...] = jnp.broadcast_to(lost, (8, 128))
    for k in range(1, n_dev):
        copy(k, here).wait_send()


def run_scalars(tau_clip, squares, loss):
    vmem = pl.BlockSpec(memory_space=pltpu.VMEM)
    return pl.pallas_call(
        functools.partial(scalars_kernel, tau_clip),
        name="scalars",
        out_shape=[jax.ShapeDtypeStruct((8, 128), F32)] * 2,
        in_specs=[vmem] * 2,
        out_specs=[vmem] * 2,
        scratch_shapes=[
            pltpu.VMEM((2, 8, 128), F32),
            pltpu.VMEM((8, 2, 8, 128), F32),
            pltpu.SemaphoreType.DMA((8,)),
            pltpu.SemaphoreType.DMA((8,)),
        ],
        compiler_params=pltpu.CompilerParams(collective_id=2, has_side_effects=True),
    )(squares, loss)


FLAT_ROWS = 3072


def update_kernel(learn_rate, grad, clip, w_old, m_old, v_old, w_new, m_new, v_new, w1_half, w2_half,
                  g_one, g_two, flat, wide, n_one, n_two, g_sem, n_sem):
    step = pl.program_id(0)
    core = lax.axis_index("data")
    d_model, d_ff = grad.shape[2], grad.shape[1] * grad.shape[3]
    rows1, rows2 = FLAT_ROWS * 128 // d_ff, FLAT_ROWS * 128 // d_model
    chunks = d_model // rows1
    steps = 2 * chunks

    def g_copy(n, of_core):
        par = lax.rem(n, 2)
        half, chunk = n // chunks, lax.rem(n, chunks)
        if of_core == 0:
            return pltpu.make_async_copy(grad.at[half, :, pl.ds(pl.multiple_of(chunk * rows1, rows1), rows1), :], g_one.at[par], g_sem.at[par])
        per_step = rows2 // PIECE
        return pltpu.make_async_copy(grad.at[half, pl.ds(chunk * per_step, per_step)], g_two.at[par], g_sem.at[par])

    def n_copy(n, of_core):
        par = lax.rem(n, 2)
        half, chunk = n // chunks, lax.rem(n, chunks)
        if of_core == 0:
            return pltpu.make_async_copy(n_one.at[par], w1_half.at[half, pl.ds(pl.multiple_of(chunk * rows1, rows1), rows1), :], n_sem.at[par])
        return pltpu.make_async_copy(n_two.at[par], w2_half.at[half, pl.ds(pl.multiple_of(chunk * rows2, rows2), rows2), :], n_sem.at[par])

    par = lax.rem(step, 2)
    for of_core in range(2):
        @pl.when(core == of_core)
        def _(of_core=of_core):
            @pl.when(step == 0)
            def _():
                g_copy(step, of_core).start()

            @pl.when(step + 1 < steps)
            def _():
                g_copy(step + 1, of_core).start()
            g_copy(step, of_core).wait()
            if of_core == 0:
                per_row = d_ff // 128
                for j in range(per_row):
                    c, lane = divmod(j * 128, PIECE)
                    flat[pl.ds(j, rows1, per_row), :] = g_one[par, c, :, lane:lane + 128]
            else:
                per_row = d_model // 128
                for c in range(rows2 // PIECE):
                    val = g_two[par, c].T
                    for j in range(per_row):
                        flat[pl.ds(c * PIECE * per_row + j, PIECE, per_row), :] = val[:, j * 128:(j + 1) * 128]

    grad_clip = jnp.broadcast_to(clip[0:1, :], (FLAT_ROWS, 128)) * flat[...]
    m_val = BETA_ONE * m_old[...] + (1.0 - BETA_ONE) * grad_clip
    v_val = BETA_TWO * v_old[...] + (1.0 - BETA_TWO) * grad_clip * grad_clip
    m_hat = m_val * (1.0 / (1.0 - BETA_ONE ** ADAM_STEP))
    v_hat = v_val * (1.0 / (1.0 - BETA_TWO ** ADAM_STEP))
    w_val = w_old[...]
    w_val = w_val - learn_rate * (m_hat / (jnp.sqrt(v_hat) + ADAM_EPS) + WEIGHT_DECAY * w_val)
    m_new[...] = m_val
    v_new[...] = v_val
    w_new[...] = w_val
    wide[...] = w_val

    for of_core in range(2):
        @pl.when(core == of_core)
        def _(of_core=of_core):
            @pl.when(step >= 2)
            def _():
                n_copy(step - 2, of_core).wait()
            buf, per_row = (n_one, d_ff // 128) if of_core == 0 else (n_two, d_model // 128)
            for j in range(per_row):
                buf[par, :, j * 128:(j + 1) * 128] = wide[pl.ds(j, buf.shape[1], per_row), :].astype(BF16)
            n_copy(step, of_core).start()

            @pl.when(step == steps - 1)
            def _():
                n_copy(step - 1, of_core).wait()
                n_copy(step, of_core).wait()


def run_update(learn_rate, grad, clip, w_old, m_old, v_old):
    d_model, d_ff = grad.shape[2], grad.shape[1] * grad.shape[3]
    rows1, rows2 = FLAT_ROWS * 128 // d_ff, FLAT_ROWS * 128 // d_model
    steps = w_old.shape[0] // FLAT_ROWS
    flat_spec = pl.BlockSpec((FLAT_ROWS, 128), lambda i: (i, 0))
    flat_shape = jax.ShapeDtypeStruct(w_old.shape, F32)
    return pl.pallas_call(
        functools.partial(update_kernel, learn_rate),
        name="update",
        grid=(steps,),
        out_shape=[flat_shape] * 3 + [jax.ShapeDtypeStruct((2, d_model, d_ff), BF16), jax.ShapeDtypeStruct((2, d_ff, d_model), BF16)],
        in_specs=[ANY, pl.BlockSpec((8, 128), lambda i: (0, 0))] + [flat_spec] * 3,
        out_specs=[flat_spec] * 3 + [ANY, ANY],
        scratch_shapes=[
            pltpu.VMEM((2, d_ff // PIECE, rows1, PIECE), F32),
            pltpu.VMEM((2, rows2 // PIECE, d_model, PIECE), F32),
            pltpu.VMEM((FLAT_ROWS, 128), F32),
            pltpu.VMEM((FLAT_ROWS, 128), F32),
            pltpu.VMEM((2, rows1, d_ff), BF16),
            pltpu.VMEM((2, rows2, d_model), BF16),
            pltpu.SemaphoreType.DMA((2,)),
            pltpu.SemaphoreType.DMA((2,)),
        ],
        compiler_params=pltpu.CompilerParams(dimension_semantics=("arbitrary",), vmem_limit_bytes=60 * 2**20),
        cost_estimate=pl.CostEstimate(flops=10**9, bytes_accessed=150 * 2**20, transcendentals=0),
    )(grad, clip, w_old, m_old, v_old)


def merge_kernel(w1_half, w2_half, w1_got, w2_got, w1_new, w2_new, buf1, buf2, in_sem, out_sem):
    del w1_half, w2_half
    core = lax.axis_index("data")
    for of_core, got, new, buf in ((1, w1_got, w1_new, buf1), (0, w2_got, w2_new, buf2)):
        parts = [(half, slot) for half in range(2) for slot in range(MERGE_PARTS)]
        rows = buf.shape[1]

        @pl.when(core == of_core)
        def _(parts=parts, rows=rows, got=got, new=new, buf=buf):
            ins, outs = [], []
            for n, (half, slot) in enumerate(parts):
                where = pl.ds(slot * rows, rows)
                ins.append(pltpu.make_async_copy(got.at[half, where, :], buf.at[n], in_sem.at[n]))
                outs.append(pltpu.make_async_copy(buf.at[n], new.at[half, where, :], out_sem.at[n]))
            for cp in ins:
                cp.start()
            for cp_in, cp_out in zip(ins, outs):
                cp_in.wait()
                cp_out.start()
            for cp in outs:
                cp.wait()


MERGE_PARTS = 4


def run_merge(w1_half, w2_half, w1_got, w2_got):
    _, d_model, d_ff = w1_half.shape
    n = 2 * MERGE_PARTS
    return pl.pallas_call(
        merge_kernel,
        name="merge",
        out_shape=[jax.ShapeDtypeStruct(w1_half.shape, BF16), jax.ShapeDtypeStruct(w2_half.shape, BF16)],
        in_specs=[ANY] * 4,
        out_specs=[ANY] * 2,
        input_output_aliases={0: 0, 1: 1},
        scratch_shapes=[
            pltpu.VMEM((n, d_model // MERGE_PARTS, d_ff), BF16),
            pltpu.VMEM((n, d_ff // MERGE_PARTS, d_model), BF16),
            pltpu.SemaphoreType.DMA((n,)),
            pltpu.SemaphoreType.DMA((n,)),
        ],
        compiler_params=pltpu.CompilerParams(vmem_limit_bytes=40 * 2**20),
    )(w1_half, w2_half, w1_got, w2_got)


def solution(mesh):
    n_stage = mesh.shape["stage"]
    n_data = mesh.shape["data"]
    axes = ("stage", "data")

    def device(stage, core):
        return stage * n_data + core

    def from_core(core):
        return [(device(s, core), device(s, 1 - core)) for s in range(n_stage)]

    def device_step(x_loc, t_loc, w1_loc, w2_loc, wm_loc, m_loc, v_loc):
        n_micro, n_tok, d_model = x_loc.shape
        d_ff = w1_loc.shape[4]
        n_tokens = n_micro * n_tok * n_data
        n_blocks = 2 * n_stage
        n_rows = n_micro * n_tok // n_stage
        tau_clip = 0.3 * d_model * math.sqrt(n_blocks * (3.0 / n_tokens + 0.008))
        learn_rate = 0.1 / math.sqrt(4.0 * d_model * n_blocks)
        w1 = w1_loc.reshape(2, d_model, d_ff)
        w2 = w2_loc.reshape(2, d_ff, d_model)
        flat_rows = (n_micro * n_tok, d_model)
        wg1, wg2, saved, u_all, seed, loss_acc = run_forward(n_tokens, x_loc.reshape(flat_rows), t_loc.reshape(flat_rows), w1, w2, n_rows)
        weights = (w1, w2, wg1, wg2)
        _, _, _, total, squares = run_backward(seed, saved, u_all, weights)
        clip, loss_all = run_scalars(tau_clip, squares, loss_acc)
        flat = [val.reshape(-1, 128) for val in (wm_loc, m_loc, v_loc)]
        w_new, m_new, v_new, w1_half, w2_half = run_update(learn_rate, total, clip, *flat)
        w1_got = lax.ppermute(w1_half, axes, from_core(0))
        w2_got = lax.ppermute(w2_half, axes, from_core(1))
        w1_new, w2_new = run_merge(w1_half, w2_half, w1_got, w2_got)
        mean_loss = loss_all[0, 0] / n_tokens
        return w1_new.reshape(w1_loc.shape), w2_new.reshape(w2_loc.shape), w_new.reshape(wm_loc.shape), m_new.reshape(wm_loc.shape), v_new.reshape(wm_loc.shape), mean_loss

    act_spec = P(None, "data", None)
    flat_spec = P("stage", None, None, "data")
    return jax.shard_map(device_step, mesh=mesh, in_specs=(act_spec, act_spec, P("stage"), P("stage"), flat_spec, flat_spec, flat_spec), out_specs=(P("stage"), P("stage"), flat_spec, flat_spec, flat_spec, P()), check_vma=False)
```

```python
import functools
import math
import jax
import jax.numpy as jnp
from jax import lax
from jax.experimental import pallas as pl
from jax.experimental.pallas import tpu as pltpu
from jax.sharding import PartitionSpec as P

BETA_ONE = 0.9
BETA_TWO = 0.999
ADAM_EPS = 1e-8
WEIGHT_DECAY = 0.1
ADAM_STEP = 1000
GELU_A = math.sqrt(2.0 / math.pi)
GELU_B = GELU_A * 0.044715
MESH = pl.DeviceIdType.MESH
ANY = pl.BlockSpec(memory_space=pl.ANY)
F32 = jnp.float32
BF16 = jnp.bfloat16

TILE = 512
PATH_PIECES = 4


def _dot_t(lhs, rhs):
    return lax.dot_general(lhs, rhs, (((1,), (1,)), ((), ())), preferred_element_type=F32)


def _dot(lhs, rhs):
    return jnp.dot(lhs, rhs, preferred_element_type=F32)


SEND_SLOT = (-45, -30, -28, -20)
HOP_SLOT = {1: (-27, -20, -18, -14), 2: (-18, -14, -8, -6), 3: (-12, -9, -2, -2)}
LOAD_SLOT = -1


def forward_kernel(n_blocks, tiles, n_tokens, x_hbm, t_hbm, w1_loc, w2_loc, wg1, wg2, saved, u_out, seed, loss,
                   act, w1_buf, w2_buf, u_buf, acc, t_buf, s_buf,
                   x_sem, act_sem, u_sem, w_sem, t_sem, s_sem, ici_send, ici_recv, d2d_send, d2d_recv):
    me = lax.axis_index("stage")
    core = lax.axis_index("data")
    d_model, d_ff = w1_loc.shape[1], w1_loc.shape[2]
    n_rows = act.shape[0]
    n_piece = 4 * PATH_PIECES
    rows1, rows2 = d_model // n_piece, d_ff // n_piece

    def peer(flip):
        bit0, bit1 = lax.rem(me, 2), me // 2
        return (1 - bit0 + 2 * bit1) if flip == 1 else (bit0 + 2 * (1 - bit1))

    def rel_of(blk):
        own = lax.rem(blk, 4)
        a0, a1, b0, b1 = lax.rem(me, 2), me // 2, lax.rem(own, 2), own // 2
        return (a0 + b0 - 2 * a0 * b0) + 2 * (a1 + b1 - 2 * a1 * b1)

    def piece(j, path, of_core):
        return j * 4 + path * 2 + of_core

    def views(blk, idx):
        return (wg1.at[blk, pl.ds(pl.multiple_of(idx * rows1, 16), rows1), :],
                wg2.at[blk, pl.ds(pl.multiple_of(idx * rows2, 64), rows2), :])

    def local_views(blk, idx):
        half = blk // 4
        return (w1_loc.at[half, pl.ds(pl.multiple_of(idx * rows1, 16), rows1), :],
                w2_loc.at[half, pl.ds(pl.multiple_of(idx * rows2, 64), rows2), :])

    def ici_copies(blk, path, j, sources, flip):
        idx = piece(j, path, core)
        slot = path * PATH_PIECES + j
        return [pltpu.make_async_remote_copy(
            src_ref=src, dst_ref=dst, send_sem=ici_send.at[blk, slot, m], recv_sem=ici_recv.at[blk, slot, m],
            device_id=(peer(flip), core), device_id_type=MESH)
            for m, (src, dst) in enumerate(zip(sources, views(blk, idx)))]

    def d2d_copies(blk, path, j, of_core):
        idx = piece(j, path, of_core)
        slot = path * PATH_PIECES + j
        return [pltpu.make_async_remote_copy(
            src_ref=ref, dst_ref=ref, send_sem=d2d_send.at[blk, slot, m], recv_sem=d2d_recv.at[blk, slot, m],
            device_id=(me, 1 - core), device_id_type=MESH) for m, ref in enumerate(views(blk, idx))]

    def first_flip(path):
        return 1 if path == 0 else 2

    def own_send(blk, j):
        @pl.when(rel_of(blk) == 0)
        def _():
            for path in range(2):
                for cp in ici_copies(blk, path, j, local_views(blk, piece(j, path, core)), first_flip(path)):
                    cp.start()

    def hop_event(blk, hop, j):
        rel = rel_of(blk)
        for path in range(2):
            at_rel = {1: (1, 2), 2: (3, 3), 3: (2, 1)}[hop][path]

            @pl.when(rel == at_rel)
            def _(path=path):
                flip = first_flip(path)
                if hop == 1:
                    flip = 3 - flip
                copies = ici_copies(blk, path, j, views(blk, piece(j, path, core)), flip)
                for cp in copies:
                    cp.wait_recv()
                if hop < 3:
                    for cp in copies:
                        cp.start()
                for cp in d2d_copies(blk, path, j, core):
                    cp.start()

    def weight_loads(blk, par, is_own):
        half = blk // 4
        src1, src2 = (w1_loc.at[half], w2_loc.at[half]) if is_own else (wg1.at[blk], wg2.at[blk])
        return [pltpu.make_async_copy(src1, w1_buf.at[par], w_sem.at[par, 0]),
                pltpu.make_async_copy(src2, w2_buf.at[par], w_sem.at[par, 1])]

    def load_event(blk):
        rel = rel_of(blk)
        par = lax.rem(blk, 2)

        @pl.when(rel == 0)
        def _():
            for cp in weight_loads(blk, par, True):
                cp.start()

        @pl.when(rel != 0)
        def _():
            for path in range(2):
                for j in range(PATH_PIECES):
                    for cp in d2d_copies(blk, path, j, 1 - core):
                        cp.wait_recv()
            for cp in weight_loads(blk, par, False):
                cp.start()

    def x_copy():
        return pltpu.make_async_copy(x_hbm.at[pl.ds(pl.multiple_of(me * n_rows, n_rows), n_rows), :], act, x_sem)

    def act_copy(slot, tile):
        rows = pl.ds(pl.multiple_of(tile * TILE, TILE), TILE)
        return pltpu.make_async_copy(act.at[rows, :], saved.at[slot, rows, :], act_sem.at[tile])

    def t_copy(tile):
        return pltpu.make_async_copy(t_hbm.at[pl.ds(pl.multiple_of(me * n_rows + tile * TILE, TILE), TILE), :], t_buf, t_sem)

    def seed_copy(tile):
        return pltpu.make_async_copy(s_buf, seed.at[pl.ds(pl.multiple_of(tile * TILE, TILE), TILE), :], s_sem)

    def u_copy(blk, tile, par):
        rows = pl.ds(pl.multiple_of(tile * TILE, TILE), TILE)
        return pltpu.make_async_copy(u_buf.at[par], u_out.at[blk, rows, :], u_sem.at[par])

    barrier = pltpu.get_barrier_semaphore()
    for target in ((peer(1), core), (peer(2), core), (me, 1 - core)):
        pl.semaphore_signal(barrier, inc=1, device_id=target, device_id_type=MESH)
    x_copy().start()
    pl.semaphore_wait(barrier, 3)

    events = []
    for hop in (3, 2, 1):
        for j in range(PATH_PIECES):
            events.append((HOP_SLOT[hop][j], functools.partial(lambda blk, hop, j: hop_event(blk, hop, j), hop=hop, j=j)))
    for j in range(PATH_PIECES):
        events.append((SEND_SLOT[j], functools.partial(lambda blk, j: own_send(blk, j), j=j)))
    events.append((LOAD_SLOT, load_event))

    def comm_slot(blk, tile):
        for residue in range(tiles):
            due = [(fn, (residue - offset) // tiles) for offset, fn in events if offset % tiles == residue]
            if not due:
                continue

            @pl.when(tile == residue)
            def _(due=due):
                for fn, ahead in due:
                    target = blk + ahead

                    @pl.when((target >= 0) & (target < n_blocks))
                    def _(fn=fn, target=target):
                        fn(target)

    def compute(blk, tile):
        par = lax.rem(blk, 2)
        u_par = lax.rem(tile, 2)
        rows = pl.ds(pl.multiple_of(tile * TILE, TILE), TILE)

        @pl.when(tile == 0)
        def _():
            for cp in weight_loads(blk, par, True):
                cp.wait()

        @pl.when((blk == 0) & (tile == 0))
        def _():
            x_copy().wait()
            for t in range(tiles):
                act_copy(0, t).start()

        @pl.when((blk > 0) | (tile > 1))
        def _():
            u_copy(blk, tile, u_par).wait()

        @pl.when(blk == n_blocks - 1)
        def _():
            t_copy(tile).start()

        act_copy(blk, tile).wait()
        x = act[rows, :]
        chunk = 256
        n_chunk = d_ff // chunk
        for f in range(n_chunk):
            cols = slice(f * chunk, (f + 1) * chunk)
            u = _dot(x, w1_buf[par, :, cols])
            u_buf[u_par, :, cols] = u
            inner = u * (GELU_A + GELU_B * (u * u))
            a = (u * (0.5 + 0.5 * jnp.tanh(inner))).astype(BF16)
            part = _dot(a, w2_buf[par, cols, :])
            if f == 0:
                acc[...] = part
            elif f < n_chunk - 1:
                acc[...] += part
            else:
                act[rows, :] = (x.astype(F32) + (acc[...] + part)).astype(BF16)
        u_copy(blk, tile, u_par).start()

        @pl.when(blk < n_blocks - 1)
        def _():
            act_copy(blk + 1, tile).start()

        @pl.when(blk == n_blocks - 1)
        def _():
            t_copy(tile).wait()

            @pl.when(tile > 0)
            def _():
                seed_copy(tile - 1).wait()
            residual = act[rows, :].astype(F32) - t_buf[...].astype(F32)
            s_buf[...] = (residual / n_tokens).astype(BF16)
            squares = jnp.sum((residual * residual).reshape(TILE // 8, 8, residual.shape[1]), axis=0)
            folded = squares[:, :128]
            for j in range(1, residual.shape[1] // 128):
                folded = folded + squares[:, j * 128:(j + 1) * 128]
            loss[...] += 0.5 * folded
            seed_copy(tile).start()

    lead = -(min(SEND_SLOT) // tiles)
    loss[...] = jnp.zeros_like(loss)

    @pl.loop(0, (n_blocks + lead) * tiles)
    def _(step):
        blk = step // tiles - lead
        tile = lax.rem(step, tiles)
        comm_slot(blk, tile)

        @pl.when(blk >= 0)
        def _():
            compute(blk, tile)

    for par in range(2):
        u_copy(0, 0, par).wait()
    seed_copy(0).wait()

    @pl.loop(0, n_blocks)
    def _(blk):
        rel = rel_of(blk)
        for path in range(2):
            last = (2, 1)[path]

            @pl.when(rel != last)
            def _(path=path):
                for j in range(PATH_PIECES):
                    for cp in ici_copies(blk, path, j, views(blk, piece(j, path, core)), 1):
                        cp.wait_send()

        @pl.when(rel != 0)
        def _():
            for path in range(2):
                for j in range(PATH_PIECES):
                    for cp in d2d_copies(blk, path, j, core):
                        cp.wait_send()


def run_forward(n_tokens, x_flat, t_flat, w1_loc, w2_loc, n_rows):
    n_half, d_model, d_ff = w1_loc.shape
    n_blocks = 4 * n_half
    tiles = n_rows // TILE
    slots = 2 * PATH_PIECES
    out_shape = [
        jax.ShapeDtypeStruct((n_blocks, d_model, d_ff), BF16),
        jax.ShapeDtypeStruct((n_blocks, d_ff, d_model), BF16),
        jax.ShapeDtypeStruct((n_blocks, n_rows, d_model), BF16),
        jax.ShapeDtypeStruct((n_blocks, n_rows, d_ff), F32),
        jax.ShapeDtypeStruct((n_rows, d_model), BF16),
        jax.ShapeDtypeStruct((8, 128), F32),
    ]
    return pl.pallas_call(
        functools.partial(forward_kernel, n_blocks, tiles, n_tokens),
        name="forward",
        out_shape=out_shape,
        in_specs=[ANY] * 4,
        out_specs=[ANY] * 5 + [pl.BlockSpec(memory_space=pltpu.VMEM)],
        scratch_shapes=[
            pltpu.VMEM((n_rows, d_model), BF16),
            pltpu.VMEM((2, d_model, d_ff), BF16),
            pltpu.VMEM((2, d_ff, d_model), BF16),
            pltpu.VMEM((2, TILE, d_ff), F32),
            pltpu.VMEM((TILE, d_model), F32),
            pltpu.VMEM((TILE, d_model), BF16),
            pltpu.VMEM((TILE, d_model), BF16),
            pltpu.SemaphoreType.DMA(()),
            pltpu.SemaphoreType.DMA((tiles,)),
            pltpu.SemaphoreType.DMA((2,)),
            pltpu.SemaphoreType.DMA((2, 2)),
            pltpu.SemaphoreType.DMA(()),
            pltpu.SemaphoreType.DMA(()),
            pltpu.SemaphoreType.DMA((n_blocks, slots, 2)),
            pltpu.SemaphoreType.DMA((n_blocks, slots, 2)),
            pltpu.SemaphoreType.DMA((n_blocks, slots, 2)),
            pltpu.SemaphoreType.DMA((n_blocks, slots, 2)),
        ],
        compiler_params=pltpu.CompilerParams(collective_id=0, has_side_effects=True, vmem_limit_bytes=60 * 2**20),
        cost_estimate=pl.CostEstimate(flops=4 * n_blocks * n_rows * d_model * d_ff, bytes_accessed=600 * 2**20, transcendentals=0),
    )(x_flat, t_flat, w1_loc, w2_loc)


RING = 5
CHUNK = 512
PIECE = 256


def _relation(me, blk):
    own = lax.rem(blk, 4)
    a0, a1, b0, b1 = lax.rem(me, 2), me // 2, lax.rem(own, 2), own // 2
    return (a0 + b0 - 2 * a0 * b0) + 2 * (a1 + b1 - 2 * a1 * b1)


def _tile_rows(tile):
    return pl.ds(pl.multiple_of(tile * TILE, TILE), TILE)


def _gelu_grad(u):
    cube = GELU_B * (u * u)
    th = jnp.tanh(u * (GELU_A + cube))
    cdf = 0.5 + 0.5 * th
    a = u * cdf
    return a, cdf + (a * (3.0 - 3.0 * th)) * (cube + GELU_A / 3.0)


STAGE_TILE = (0, 3, 5, 8)
SENDS = 3


def backward_kernel(n_blocks, tiles, g_hbm, saved, u_hbm, w1_loc, w2_loc, wg1, wg2, local, sib, inbox, own, squares,
                    act, w1_buf, w2_buf, dw, u_buf, x_buf, x_t, g_t, acc, q_buf, k_buf, s_buf, r_buf, o_buf,
                    g_sem, w_sem, u_sem, x_sem, keep_sem, d2d_send, d2d_recv, load_sem, own_sem, ici_send, ici_recv):
    me = lax.axis_index("stage")
    core = lax.axis_index("data")
    d_model, d_ff = act.shape[1], w1_buf.shape[1]
    n_chunk = d_ff // CHUNK
    n_pair = n_chunk // 2
    n_slot = d_ff // PIECE // 2
    steps = n_blocks * tiles
    total = steps * n_chunk
    top = n_blocks - 1

    def cols_of(f):
        return pl.ds(pl.multiple_of(f * CHUNK, CHUNK), CHUNK)

    def pair_of(p):
        return pl.ds(pl.multiple_of(p * 2 * CHUNK, 2 * CHUNK), 2 * CHUNK)

    def pieces_of(f):
        return pl.ds(f * (CHUNK // PIECE), CHUNK // PIECE)

    def weight_copies(blk, pair, is_own):
        half = blk // 4
        src1, src2 = (w1_loc.at[half], w2_loc.at[half]) if is_own else (wg1.at[blk], wg2.at[blk])
        cols = pair_of(pair)
        return [pltpu.make_async_copy(src1.at[:, cols], w1_buf.at[:, cols], w_sem.at[pair, 0]),
                pltpu.make_async_copy(src2.at[cols, :], w2_buf.at[cols, :], w_sem.at[pair, 1])]

    def start_weights(blk, pair):
        rel = _relation(me, blk)

        @pl.when(rel == 0)
        def _():
            for cp in weight_copies(blk, pair, True):
                cp.start()

        @pl.when(rel != 0)
        def _():
            for cp in weight_copies(blk, pair, False):
                cp.start()

    def u_copy(step):
        blk = top - step // (tiles * n_chunk)
        tile = lax.rem(step // n_chunk, tiles)
        f = lax.rem(step, n_chunk)
        slot = lax.rem(step, RING)
        return pltpu.make_async_copy(u_hbm.at[blk, _tile_rows(tile), cols_of(f)], u_buf.at[slot], u_sem.at[slot])

    def x_copy(bt):
        par = lax.rem(bt, 2)
        return pltpu.make_async_copy(saved.at[top - bt // tiles, _tile_rows(lax.rem(bt, tiles)), :], x_buf.at[par], x_sem.at[par])

    def g_in_copy():
        return pltpu.make_async_copy(g_hbm, act, g_sem)

    def keep_copy(j, f):
        return pltpu.make_async_copy(dw.at[core, pieces_of(f)], local.at[lax.rem(j, 3), pieces_of(f)], keep_sem.at[f])

    def give_copy(j, c):
        return pltpu.make_async_remote_copy(
            src_ref=dw.at[1 - core, c], dst_ref=sib.at[j, c], send_sem=d2d_send.at[c],
            recv_sem=d2d_recv.at[j, c], device_id=(me, 1 - core), device_id_type=MESH)

    def stages_of(j):
        rel = _relation(me, top - j)
        return [jnp.where(rel == 0, 3, jnp.where(rel == 3, 1, jnp.where(rel == last, 0, 2))) for last in (2, 1)]

    def next_chip(stage, path):
        first = 1 if path == 0 else 2
        flip = jnp.where(stage == 1, 3 - first, first)
        bit0, bit1 = lax.rem(me, 2), me // 2
        return jnp.where(flip == 1, 1 - bit0 + 2 * bit1, bit0 + 2 * (1 - bit1))

    def piece_loads(j, c, buf):
        return [pltpu.make_async_copy(local.at[lax.rem(j, 3), c], k_buf.at[buf], load_sem.at[buf, 0]),
                pltpu.make_async_copy(sib.at[j, c], s_buf.at[buf], load_sem.at[buf, 1])]

    def inbox_load(j, c, buf):
        return pltpu.make_async_copy(inbox.at[j, c], r_buf.at[buf], load_sem.at[buf, 2])

    def own_copy(j, c, buf):
        return pltpu.make_async_copy(k_buf.at[buf], own.at[(top - j) // 4, c], own_sem.at[buf])

    def pass_copy(j, m, buf, stage, path):
        slot = lax.rem(m, SENDS)
        c = 2 * m + path
        return pltpu.make_async_remote_copy(
            src_ref=o_buf.at[buf, slot], dst_ref=inbox.at[j, c], send_sem=ici_send.at[buf, slot],
            recv_sem=ici_recv.at[j, c], device_id=(next_chip(stage, path), core), device_id_type=MESH)

    def first_piece(stage):
        return jnp.where(stage == 0, STAGE_TILE[0], jnp.where(stage == 1, STAGE_TILE[1], jnp.where(stage == 2, STAGE_TILE[2], STAGE_TILE[3])))

    def load_pieces(j, tile):
        live = (j >= 0) & (j < n_blocks)
        for path, (stage, before) in enumerate(zip(stages_of(j), stages_of(j - 2))):
            m = tile - first_piece(stage)

            @pl.when(live & (m >= 0) & (m < n_slot))
            def _(path=path, stage=stage, before=before, m=m):
                buf = lax.rem(j, 2) * 2 + path
                c = 2 * m + path

                @pl.when(((m >= 1) & (stage == 3)) | ((m == 0) & (j >= 2) & (before == 3)))
                def _():
                    own_copy(j, c, buf).wait()
                give_copy(j, c).wait_recv()
                for cp in piece_loads(j, c, buf):
                    cp.start()

                @pl.when(stage > 0)
                def _():
                    pass_copy(j, m, buf, stage, path).wait_recv()
                    inbox_load(j, c, buf).start()

    def sum_pieces(j, tile):
        live = (j >= 0) & (j < n_blocks)
        for path, (stage, before) in enumerate(zip(stages_of(j), stages_of(j - 2))):
            m = tile - first_piece(stage)

            @pl.when(live & (m >= 0) & (m < n_slot))
            def _(path=path, stage=stage, before=before, m=m):
                buf = lax.rem(j, 2) * 2 + path
                slot = lax.rem(m, SENDS)
                c = 2 * m + path

                @pl.when(((m >= SENDS) & (stage < 3)) | ((m < SENDS) & (j >= 2) & (before < 3)))
                def _():
                    pass_copy(j, m, buf, stage, path).wait_send()
                for cp in piece_loads(j, c, buf):
                    cp.wait()

                @pl.when(stage == 0)
                def _():
                    o_buf[buf, slot] = (k_buf[buf] + s_buf[buf]).astype(BF16)

                @pl.when(stage > 0)
                def _():
                    inbox_load(j, c, buf).wait()

                @pl.when((stage == 1) | (stage == 2))
                def _():
                    o_buf[buf, slot] = ((k_buf[buf] + s_buf[buf]) + r_buf[buf].astype(F32)).astype(BF16)

                @pl.when(stage < 3)
                def _():
                    pass_copy(j, m, buf, stage, path).start()

                @pl.when(stage == 3)
                def _():
                    val = (k_buf[buf] + s_buf[buf]) + r_buf[buf].astype(F32)
                    k_buf[buf] = val
                    part = jnp.sum((val * val).reshape(d_model // 8, 8, PIECE), axis=0)
                    squares[...] += part[:, :128] + part[:, 128:]
                    own_copy(j, c, buf).start()

    barrier = pltpu.get_barrier_semaphore()
    bit0, bit1 = lax.rem(me, 2), me // 2
    near = ((1 - bit0 + 2 * bit1, core), (bit0 + 2 * (1 - bit1), core), (me, 1 - core))
    for target in near:
        pl.semaphore_signal(barrier, inc=1, device_id=target, device_id_type=MESH)
    g_in_copy().start()
    for pair in range(n_pair):
        start_weights(jnp.int32(top), jnp.int32(pair))
    x_copy(0).start()
    x_copy(1).start()
    for step in range(RING - 2):
        u_copy(step).start()
    squares[...] = jnp.zeros_like(squares)
    pl.semaphore_wait(barrier, 3)
    g_in_copy().wait()
    x_copy(0).wait()
    x_t[0] = x_buf[0].T
    g_t[0] = act[pl.ds(0, TILE), :].T
    weight_copies(0, 0, True)[1].wait()
    q_buf[0] = _dot_t(act[pl.ds(0, TILE), :], w2_buf[pl.ds(0, CHUNK), :])

    def compute(n):
        bt = n // n_pair
        pair = lax.rem(n, n_pair)
        i = bt // tiles
        tile = lax.rem(bt, tiles)
        blk = top - i
        t_par = lax.rem(bt, 2)
        rows = _tile_rows(tile)
        next_rows = _tile_rows(lax.rem(tile + 1, tiles))

        @pl.when((pair == 0) & (bt + 1 < steps))
        def _():
            x_copy(bt + 1).wait()

        @pl.when((pair == 0) & (bt + 2 < steps))
        def _():
            x_copy(bt + 2).start()

        @pl.when(pair == 0)
        def _():
            acc[...] = act[rows, :].astype(F32)

        def chunk_prep(f, step):
            @pl.when(step + RING - 2 < total)
            def _():
                u_copy(step + RING - 2).start()
            u_copy(step).wait()

            @pl.when((tile == 0) & (i > 0))
            def _():
                keep_copy(i - 1, f).wait()
                for c in (2 * f, 2 * f + 1):
                    give_copy(i - 1, c).wait_send()

        def add_to(m, f, val):
            for part in range(CHUNK // PIECE):
                c = f * (CHUNK // PIECE) + part
                dw[m, c] = jnp.where(tile == 0, 0.0, dw[m, c]) + val[:, part * PIECE:(part + 1) * PIECE]

        def chunk_main(f, step, q_par, next_g, next_w2, with_input_grad):
            cols = cols_of(f)
            q_buf[1 - q_par] = _dot_t(next_g, next_w2)
            a, slope = _gelu_grad(u_buf[lax.rem(step, RING)])
            r = (q_buf[q_par] * slope).astype(BF16)
            add_to(0, f, _dot(x_t[t_par], r))
            add_to(1, f, _dot(g_t[t_par], a.astype(BF16)))
            if with_input_grad:
                acc[...] += _dot_t(r, w1_buf[:, cols])

        def pair_step(with_input_grad):
            f0 = pair * 2
            step = bt * n_chunk + f0
            last = pair == n_pair - 1
            chunk_prep(f0, step)
            chunk_prep(f0 + 1, step + 1)

            @pl.when(tile == 0)
            def _():
                weight_copies(0, pair, True)[0].wait()

            @pl.when((tile == 0) & (pair < n_pair - 1))
            def _():
                weight_copies(0, pair + 1, True)[1].wait()

            @pl.when(last & (tile == tiles - 1) & (bt + 1 < steps))
            def _():
                weight_copies(0, jnp.int32(0), True)[1].wait()

            q_rows = _tile_rows(jnp.where(last, lax.rem(tile + 1, tiles), tile))
            next_f = jnp.where(last, 0, f0 + 2)
            third = pl.ds(pl.multiple_of(pair * 256, 256), 256)
            x_t[1 - t_par, third, :] = x_buf[1 - t_par, :, third].T
            g_t[1 - t_par, third, :] = act[next_rows, third].T
            chunk_main(f0, step, 0, act[rows, :], w2_buf[cols_of(f0 + 1), :], with_input_grad)
            chunk_main(f0 + 1, step + 1, 1, act[q_rows, :], w2_buf[cols_of(next_f), :], with_input_grad)

            @pl.when(tile == tiles - 1)
            def _():
                for f in (f0, f0 + 1):
                    keep_copy(i, f).start()
                    for c in (2 * f, 2 * f + 1):
                        give_copy(i, c).start()

            if with_input_grad:
                @pl.when(tile == tiles - 1)
                def _():
                    start_weights(blk - 1, pair)

        @pl.when(blk > 0)
        def _():
            pair_step(True)

            @pl.when(pair == n_pair - 1)
            def _():
                act[rows, :] = acc[...].astype(BF16)

        @pl.when(blk == 0)
        def _():
            pair_step(False)

    span = tiles * n_pair
    all_steps = n_blocks * span

    @pl.loop(0, all_steps + (STAGE_TILE[3] + n_slot) * n_pair)
    def _(n):
        i = n // span
        tile = lax.rem(n, span) // n_pair
        phase = lax.rem(n, n_pair)

        @pl.when(n < all_steps)
        def _():
            compute(n)

        @pl.when(n == all_steps)
        def _():
            for f in range(n_chunk):
                keep_copy(top, f).wait()
                for c in (2 * f, 2 * f + 1):
                    give_copy(top, c).wait_send()

        @pl.when((phase == 0) & (i > 0))
        def _():
            load_pieces(i - 2, tile + tiles)
            load_pieces(i - 1, tile)

        @pl.when((phase == 1) & (i > 0))
        def _():
            sum_pieces(i - 2, tile + tiles)
            sum_pieces(i - 1, tile)

    for j in (n_blocks - 2, n_blocks - 1):
        for path, stage in enumerate(stages_of(j)):
            buf = j % 2 * 2 + path

            @pl.when(stage == 3)
            def _(j=j, path=path, buf=buf):
                own_copy(j, path, buf).wait()

            @pl.when(stage < 3)
            def _(j=j, path=path, buf=buf, stage=stage):
                for m in range(SENDS):
                    pass_copy(j, m, buf, stage, path).wait_send()


def run_backward(grad, saved, u_all, weights):
    n_rows, d_model = grad.shape
    n_half, _, d_ff = weights[0].shape
    n_blocks = 4 * n_half
    tiles = n_rows // TILE
    n_chunk = d_ff // CHUNK
    n_piece = d_ff // PIECE
    pieces = (n_piece, d_model, PIECE)
    return pl.pallas_call(
        functools.partial(backward_kernel, n_blocks, tiles),
        name="backward",
        out_shape=[
            jax.ShapeDtypeStruct((3,) + pieces, F32),
            jax.ShapeDtypeStruct((n_blocks,) + pieces, F32),
            jax.ShapeDtypeStruct((n_blocks,) + pieces, BF16),
            jax.ShapeDtypeStruct((n_half,) + pieces, F32),
            jax.ShapeDtypeStruct((8, 128), F32),
        ],
        in_specs=[ANY] * 7,
        out_specs=[ANY] * 4 + [pl.BlockSpec(memory_space=pltpu.VMEM)],
        scratch_shapes=[
            pltpu.VMEM((n_rows, d_model), BF16),
            pltpu.VMEM((d_model, d_ff), BF16),
            pltpu.VMEM((d_ff, d_model), BF16),
            pltpu.VMEM((2,) + pieces, F32),
            pltpu.VMEM((RING, TILE, CHUNK), F32),
            pltpu.VMEM((2, TILE, d_model), BF16),
            pltpu.VMEM((2, d_model, TILE), BF16),
            pltpu.VMEM((2, d_model, TILE), BF16),
            pltpu.VMEM((TILE, d_model), F32),
            pltpu.VMEM((2, TILE, CHUNK), F32),
            pltpu.VMEM((4, d_model, PIECE), F32),
            pltpu.VMEM((4, d_model, PIECE), F32),
            pltpu.VMEM((4, d_model, PIECE), BF16),
            pltpu.VMEM((4, SENDS, d_model, PIECE), BF16),
            pltpu.SemaphoreType.DMA(()),
            pltpu.SemaphoreType.DMA((n_chunk // 2, 2)),
            pltpu.SemaphoreType.DMA((RING,)),
            pltpu.SemaphoreType.DMA((2,)),
            pltpu.SemaphoreType.DMA((n_chunk,)),
            pltpu.SemaphoreType.DMA((n_piece,)),
            pltpu.SemaphoreType.DMA((n_blocks, n_piece)),
            pltpu.SemaphoreType.DMA((4, 3)),
            pltpu.SemaphoreType.DMA((4,)),
            pltpu.SemaphoreType.DMA((4, SENDS)),
            pltpu.SemaphoreType.DMA((n_blocks, n_piece)),
        ],
        compiler_params=pltpu.CompilerParams(collective_id=1, has_side_effects=True, vmem_limit_bytes=67043328),
        cost_estimate=pl.CostEstimate(flops=8 * n_blocks * n_rows * d_model * d_ff, bytes_accessed=800 * 2**20, transcendentals=0),
    )(grad, saved, u_all, *weights)


def scalars_kernel(tau_clip, squares, loss, clip_out, loss_out, mine, gathered, send_sem, recv_sem):
    stage = lax.axis_index("stage")
    core = lax.axis_index("data")
    n_dev = gathered.shape[0]
    here = stage * 2 + core
    barrier = pltpu.get_barrier_semaphore()
    for k in range(1, n_dev):
        other = lax.rem(here + k, n_dev)
        pl.semaphore_signal(barrier, inc=1, device_id=(other // 2, lax.rem(other, 2)), device_id_type=MESH)
    mine[0] = squares[...]
    mine[1] = loss[...]
    gathered[here] = mine[...]
    pl.semaphore_wait(barrier, n_dev - 1)

    def copy(k, slot):
        other = lax.rem(here + k, n_dev)
        return pltpu.make_async_remote_copy(
            src_ref=mine, dst_ref=gathered.at[slot], send_sem=send_sem.at[k], recv_sem=recv_sem.at[k],
            device_id=(other // 2, lax.rem(other, 2)), device_id_type=MESH)

    for k in range(1, n_dev):
        copy(k, here).start()
    for k in range(1, n_dev):
        copy(k, lax.rem(here + n_dev - k, n_dev)).wait_recv()
    sums = jnp.sum(gathered[...], axis=0)
    squared = jnp.sum(jnp.sum(sums[0], axis=0, keepdims=True), axis=1, keepdims=True)
    lost = jnp.sum(jnp.sum(sums[1], axis=0, keepdims=True), axis=1, keepdims=True)
    norm = jnp.sqrt(jnp.broadcast_to(squared, (8, 128)))
    clip_out[...] = jnp.minimum(1.0, tau_clip / norm)
    loss_out[...] = jnp.broadcast_to(lost, (8, 128))
    for k in range(1, n_dev):
        copy(k, here).wait_send()


def run_scalars(tau_clip, squares, loss):
    vmem = pl.BlockSpec(memory_space=pltpu.VMEM)
    return pl.pallas_call(
        functools.partial(scalars_kernel, tau_clip),
        name="scalars",
        out_shape=[jax.ShapeDtypeStruct((8, 128), F32)] * 2,
        in_specs=[vmem] * 2,
        out_specs=[vmem] * 2,
        scratch_shapes=[
            pltpu.VMEM((2, 8, 128), F32),
            pltpu.VMEM((8, 2, 8, 128), F32),
            pltpu.SemaphoreType.DMA((8,)),
            pltpu.SemaphoreType.DMA((8,)),
        ],
        compiler_params=pltpu.CompilerParams(collective_id=2, has_side_effects=True),
    )(squares, loss)


FLAT_ROWS = 3072


def update_kernel(learn_rate, grad, clip, w_old, m_old, v_old, w_new, m_new, v_new, w1_half, w2_half,
                  g_one, g_two, flat, wide, n_one, n_two, g_sem, n_sem):
    step = pl.program_id(0)
    core = lax.axis_index("data")
    d_model, d_ff = grad.shape[2], grad.shape[1] * grad.shape[3]
    rows1, rows2 = FLAT_ROWS * 128 // d_ff, FLAT_ROWS * 128 // d_model
    chunks = d_model // rows1
    steps = 2 * chunks

    def g_copy(n, of_core):
        par = lax.rem(n, 2)
        half, chunk = n // chunks, lax.rem(n, chunks)
        if of_core == 0:
            return pltpu.make_async_copy(grad.at[half, :, pl.ds(pl.multiple_of(chunk * rows1, rows1), rows1), :], g_one.at[par], g_sem.at[par])
        per_step = rows2 // PIECE
        return pltpu.make_async_copy(grad.at[half, pl.ds(chunk * per_step, per_step)], g_two.at[par], g_sem.at[par])

    def n_copy(n, of_core):
        par = lax.rem(n, 2)
        half, chunk = n // chunks, lax.rem(n, chunks)
        if of_core == 0:
            return pltpu.make_async_copy(n_one.at[par], w1_half.at[half, pl.ds(pl.multiple_of(chunk * rows1, rows1), rows1), :], n_sem.at[par])
        return pltpu.make_async_copy(n_two.at[par], w2_half.at[half, pl.ds(pl.multiple_of(chunk * rows2, rows2), rows2), :], n_sem.at[par])

    par = lax.rem(step, 2)
    for of_core in range(2):
        @pl.when(core == of_core)
        def _(of_core=of_core):
            @pl.when(step == 0)
            def _():
                g_copy(step, of_core).start()

            @pl.when(step + 1 < steps)
            def _():
                g_copy(step + 1, of_core).start()
            g_copy(step, of_core).wait()
            if of_core == 0:
                per_row = d_ff // 128
                for j in range(per_row):
                    c, lane = divmod(j * 128, PIECE)
                    flat[pl.ds(j, rows1, per_row), :] = g_one[par, c, :, lane:lane + 128]
            else:
                per_row = d_model // 128
                for c in range(rows2 // PIECE):
                    val = g_two[par, c].T
                    for j in range(per_row):
                        flat[pl.ds(c * PIECE * per_row + j, PIECE, per_row), :] = val[:, j * 128:(j + 1) * 128]

    grad_clip = jnp.broadcast_to(clip[0:1, :], (FLAT_ROWS, 128)) * flat[...]
    m_val = BETA_ONE * m_old[...] + (1.0 - BETA_ONE) * grad_clip
    v_val = BETA_TWO * v_old[...] + (1.0 - BETA_TWO) * grad_clip * grad_clip
    m_hat = m_val * (1.0 / (1.0 - BETA_ONE ** ADAM_STEP))
    v_hat = v_val * (1.0 / (1.0 - BETA_TWO ** ADAM_STEP))
    w_val = w_old[...]
    w_val = w_val - learn_rate * (m_hat / (jnp.sqrt(v_hat) + ADAM_EPS) + WEIGHT_DECAY * w_val)
    m_new[...] = m_val
    v_new[...] = v_val
    w_new[...] = w_val
    wide[...] = w_val

    for of_core in range(2):
        @pl.when(core == of_core)
        def _(of_core=of_core):
            @pl.when(step >= 2)
            def _():
                n_copy(step - 2, of_core).wait()
            buf, per_row = (n_one, d_ff // 128) if of_core == 0 else (n_two, d_model // 128)
            for j in range(per_row):
                buf[par, :, j * 128:(j + 1) * 128] = wide[pl.ds(j, buf.shape[1], per_row), :].astype(BF16)
            n_copy(step, of_core).start()

            @pl.when(step == steps - 1)
            def _():
                n_copy(step - 1, of_core).wait()
                n_copy(step, of_core).wait()


def run_update(learn_rate, grad, clip, w_old, m_old, v_old):
    d_model, d_ff = grad.shape[2], grad.shape[1] * grad.shape[3]
    rows1, rows2 = FLAT_ROWS * 128 // d_ff, FLAT_ROWS * 128 // d_model
    steps = w_old.shape[0] // FLAT_ROWS
    flat_spec = pl.BlockSpec((FLAT_ROWS, 128), lambda i: (i, 0))
    flat_shape = jax.ShapeDtypeStruct(w_old.shape, F32)
    return pl.pallas_call(
        functools.partial(update_kernel, learn_rate),
        name="update",
        grid=(steps,),
        out_shape=[flat_shape] * 3 + [jax.ShapeDtypeStruct((2, d_model, d_ff), BF16), jax.ShapeDtypeStruct((2, d_ff, d_model), BF16)],
        in_specs=[ANY, pl.BlockSpec((8, 128), lambda i: (0, 0))] + [flat_spec] * 3,
        out_specs=[flat_spec] * 3 + [ANY, ANY],
        scratch_shapes=[
            pltpu.VMEM((2, d_ff // PIECE, rows1, PIECE), F32),
            pltpu.VMEM((2, rows2 // PIECE, d_model, PIECE), F32),
            pltpu.VMEM((FLAT_ROWS, 128), F32),
            pltpu.VMEM((FLAT_ROWS, 128), F32),
            pltpu.VMEM((2, rows1, d_ff), BF16),
            pltpu.VMEM((2, rows2, d_model), BF16),
            pltpu.SemaphoreType.DMA((2,)),
            pltpu.SemaphoreType.DMA((2,)),
        ],
        compiler_params=pltpu.CompilerParams(dimension_semantics=("arbitrary",), vmem_limit_bytes=60 * 2**20),
        cost_estimate=pl.CostEstimate(flops=10**9, bytes_accessed=150 * 2**20, transcendentals=0),
    )(grad, clip, w_old, m_old, v_old)


def merge_kernel(w1_half, w2_half, w1_got, w2_got, w1_new, w2_new, buf1, buf2, in_sem, out_sem):
    del w1_half, w2_half
    core = lax.axis_index("data")
    for of_core, got, new, buf in ((1, w1_got, w1_new, buf1), (0, w2_got, w2_new, buf2)):
        parts = [(half, slot) for half in range(2) for slot in range(MERGE_PARTS)]
        rows = buf.shape[1]

        @pl.when(core == of_core)
        def _(parts=parts, rows=rows, got=got, new=new, buf=buf):
            ins, outs = [], []
            for n, (half, slot) in enumerate(parts):
                where = pl.ds(slot * rows, rows)
                ins.append(pltpu.make_async_copy(got.at[half, where, :], buf.at[n], in_sem.at[n]))
                outs.append(pltpu.make_async_copy(buf.at[n], new.at[half, where, :], out_sem.at[n]))
            for cp in ins:
                cp.start()
            for cp_in, cp_out in zip(ins, outs):
                cp_in.wait()
                cp_out.start()
            for cp in outs:
                cp.wait()


MERGE_PARTS = 4


def run_merge(w1_half, w2_half, w1_got, w2_got):
    _, d_model, d_ff = w1_half.shape
    n = 2 * MERGE_PARTS
    return pl.pallas_call(
        merge_kernel,
        name="merge",
        out_shape=[jax.ShapeDtypeStruct(w1_half.shape, BF16), jax.ShapeDtypeStruct(w2_half.shape, BF16)],
        in_specs=[ANY] * 4,
        out_specs=[ANY] * 2,
        input_output_aliases={0: 0, 1: 1},
        scratch_shapes=[
            pltpu.VMEM((n, d_model // MERGE_PARTS, d_ff), BF16),
            pltpu.VMEM((n, d_ff // MERGE_PARTS, d_model), BF16),
            pltpu.SemaphoreType.DMA((n,)),
            pltpu.SemaphoreType.DMA((n,)),
        ],
        compiler_params=pltpu.CompilerParams(vmem_limit_bytes=24 * 2**20),
    )(w1_half, w2_half, w1_got, w2_got)


def solution(mesh):
    n_stage = mesh.shape["stage"]
    n_data = mesh.shape["data"]
    axes = ("stage", "data")

    def device(stage, core):
        return stage * n_data + core

    def from_core(core):
        return [(device(s, core), device(s, 1 - core)) for s in range(n_stage)]

    def device_step(x_loc, t_loc, w1_loc, w2_loc, wm_loc, m_loc, v_loc):
        n_micro, n_tok, d_model = x_loc.shape
        d_ff = w1_loc.shape[4]
        n_tokens = n_micro * n_tok * n_data
        n_blocks = 2 * n_stage
        n_rows = n_micro * n_tok // n_stage
        tau_clip = 0.3 * d_model * math.sqrt(n_blocks * (3.0 / n_tokens + 0.008))
        learn_rate = 0.1 / math.sqrt(4.0 * d_model * n_blocks)
        w1 = w1_loc.reshape(2, d_model, d_ff)
        w2 = w2_loc.reshape(2, d_ff, d_model)
        flat_rows = (n_micro * n_tok, d_model)
        wg1, wg2, saved, u_all, seed, loss_acc = run_forward(n_tokens, x_loc.reshape(flat_rows), t_loc.reshape(flat_rows), w1, w2, n_rows)
        weights = (w1, w2, wg1, wg2)
        _, _, _, total, squares = run_backward(seed, saved, u_all, weights)
        clip, loss_all = run_scalars(tau_clip, squares, loss_acc)
        flat = [val.reshape(-1, 128) for val in (wm_loc, m_loc, v_loc)]
        w_new, m_new, v_new, w1_half, w2_half = run_update(learn_rate, total, clip, *flat)
        w1_got = lax.ppermute(w1_half, axes, from_core(0))
        w2_got = lax.ppermute(w2_half, axes, from_core(1))
        w1_new, w2_new = run_merge(w1_half, w2_half, w1_got, w2_got)
        mean_loss = loss_all[0, 0] / n_tokens
        return w1_new.reshape(w1_loc.shape), w2_new.reshape(w2_loc.shape), w_new.reshape(wm_loc.shape), m_new.reshape(wm_loc.shape), v_new.reshape(wm_loc.shape), mean_loss

    act_spec = P(None, "data", None)
    flat_spec = P("stage", None, None, "data")
    return jax.shard_map(device_step, mesh=mesh, in_specs=(act_spec, act_spec, P("stage"), P("stage"), flat_spec, flat_spec, flat_spec), out_specs=(P("stage"), P("stage"), flat_spec, flat_spec, flat_spec, P()), check_vma=False)
```

```python
import functools
import math
import jax
import jax.numpy as jnp
from jax import lax
from jax.experimental import pallas as pl
from jax.experimental.pallas import tpu as pltpu
from jax.sharding import PartitionSpec as P

BETA_ONE = 0.9
BETA_TWO = 0.999
ADAM_EPS = 1e-8
WEIGHT_DECAY = 0.1
ADAM_STEP = 1000
GELU_A = math.sqrt(2.0 / math.pi)
GELU_B = GELU_A * 0.044715
MESH = pl.DeviceIdType.MESH
ANY = pl.BlockSpec(memory_space=pl.ANY)
F32 = jnp.float32
BF16 = jnp.bfloat16

TILE = 512
PATH_PIECES = 4


def _dot_t(lhs, rhs):
    return lax.dot_general(lhs, rhs, (((1,), (1,)), ((), ())), preferred_element_type=F32)


def _dot(lhs, rhs):
    return jnp.dot(lhs, rhs, preferred_element_type=F32)


SEND_SLOT = (-45, -30, -28, -20)
HOP_SLOT = {1: (-27, -20, -18, -14), 2: (-18, -14, -8, -6), 3: (-12, -9, -2, -2)}
LOAD_SLOT = -1


def forward_kernel(n_blocks, tiles, n_tokens, x_hbm, t_hbm, w1_loc, w2_loc, wg1, wg2, saved, u_out, seed, loss,
                   act, w1_buf, w2_buf, u_buf, acc, t_buf, s_buf,
                   x_sem, act_sem, u_sem, w_sem, t_sem, s_sem, ici_send, ici_recv, d2d_send, d2d_recv):
    me = lax.axis_index("stage")
    core = lax.axis_index("data")
    d_model, d_ff = w1_loc.shape[1], w1_loc.shape[2]
    n_rows = act.shape[0]
    n_piece = 4 * PATH_PIECES
    rows1, rows2 = d_model // n_piece, d_ff // n_piece

    def peer(flip):
        bit0, bit1 = lax.rem(me, 2), me // 2
        return (1 - bit0 + 2 * bit1) if flip == 1 else (bit0 + 2 * (1 - bit1))

    def rel_of(blk):
        own = lax.rem(blk, 4)
        a0, a1, b0, b1 = lax.rem(me, 2), me // 2, lax.rem(own, 2), own // 2
        return (a0 + b0 - 2 * a0 * b0) + 2 * (a1 + b1 - 2 * a1 * b1)

    def piece(j, path, of_core):
        return j * 4 + path * 2 + of_core

    def views(blk, idx):
        return (wg1.at[blk, pl.ds(pl.multiple_of(idx * rows1, 16), rows1), :],
                wg2.at[blk, pl.ds(pl.multiple_of(idx * rows2, 64), rows2), :])

    def local_views(blk, idx):
        half = blk // 4
        return (w1_loc.at[half, pl.ds(pl.multiple_of(idx * rows1, 16), rows1), :],
                w2_loc.at[half, pl.ds(pl.multiple_of(idx * rows2, 64), rows2), :])

    def ici_copies(blk, path, j, sources, flip):
        idx = piece(j, path, core)
        slot = path * PATH_PIECES + j
        return [pltpu.make_async_remote_copy(
            src_ref=src, dst_ref=dst, send_sem=ici_send.at[blk, slot, m], recv_sem=ici_recv.at[blk, slot, m],
            device_id=(peer(flip), core), device_id_type=MESH)
            for m, (src, dst) in enumerate(zip(sources, views(blk, idx)))]

    def d2d_copies(blk, path, j, of_core):
        idx = piece(j, path, of_core)
        slot = path * PATH_PIECES + j
        return [pltpu.make_async_remote_copy(
            src_ref=ref, dst_ref=ref, send_sem=d2d_send.at[blk, slot, m], recv_sem=d2d_recv.at[blk, slot, m],
            device_id=(me, 1 - core), device_id_type=MESH) for m, ref in enumerate(views(blk, idx))]

    def first_flip(path):
        return 1 if path == 0 else 2

    def own_send(blk, j):
        @pl.when(rel_of(blk) == 0)
        def _():
            for path in range(2):
                for cp in ici_copies(blk, path, j, local_views(blk, piece(j, path, core)), first_flip(path)):
                    cp.start()

    def hop_event(blk, hop, j):
        rel = rel_of(blk)
        for path in range(2):
            at_rel = {1: (1, 2), 2: (3, 3), 3: (2, 1)}[hop][path]

            @pl.when(rel == at_rel)
            def _(path=path):
                flip = first_flip(path)
                if hop == 1:
                    flip = 3 - flip
                copies = ici_copies(blk, path, j, views(blk, piece(j, path, core)), flip)
                for cp in copies:
                    cp.wait_recv()
                if hop < 3:
                    for cp in copies:
                        cp.start()
                for cp in d2d_copies(blk, path, j, core):
                    cp.start()

    def weight_loads(blk, par, is_own):
        half = blk // 4
        src1, src2 = (w1_loc.at[half], w2_loc.at[half]) if is_own else (wg1.at[blk], wg2.at[blk])
        return [pltpu.make_async_copy(src1, w1_buf.at[par], w_sem.at[par, 0]),
                pltpu.make_async_copy(src2, w2_buf.at[par], w_sem.at[par, 1])]

    def load_event(blk):
        rel = rel_of(blk)
        par = lax.rem(blk, 2)

        @pl.when(rel == 0)
        def _():
            for cp in weight_loads(blk, par, True):
                cp.start()

        @pl.when(rel != 0)
        def _():
            for path in range(2):
                for j in range(PATH_PIECES):
                    for cp in d2d_copies(blk, path, j, 1 - core):
                        cp.wait_recv()
            for cp in weight_loads(blk, par, False):
                cp.start()

    def x_copy():
        return pltpu.make_async_copy(x_hbm.at[pl.ds(pl.multiple_of(me * n_rows, n_rows), n_rows), :], act, x_sem)

    def act_copy(slot, tile):
        rows = pl.ds(pl.multiple_of(tile * TILE, TILE), TILE)
        return pltpu.make_async_copy(act.at[rows, :], saved.at[slot, rows, :], act_sem.at[tile])

    def t_copy(tile):
        return pltpu.make_async_copy(t_hbm.at[pl.ds(pl.multiple_of(me * n_rows + tile * TILE, TILE), TILE), :], t_buf, t_sem)

    def seed_copy(tile):
        return pltpu.make_async_copy(s_buf, seed.at[pl.ds(pl.multiple_of(tile * TILE, TILE), TILE), :], s_sem)

    def u_copy(blk, tile, par):
        rows = pl.ds(pl.multiple_of(tile * TILE, TILE), TILE)
        return pltpu.make_async_copy(u_buf.at[par], u_out.at[blk, rows, :], u_sem.at[par])

    barrier = pltpu.get_barrier_semaphore()
    for target in ((peer(1), core), (peer(2), core), (me, 1 - core)):
        pl.semaphore_signal(barrier, inc=1, device_id=target, device_id_type=MESH)
    x_copy().start()
    pl.semaphore_wait(barrier, 3)

    events = []
    for hop in (3, 2, 1):
        for j in range(PATH_PIECES):
            events.append((HOP_SLOT[hop][j], functools.partial(lambda blk, hop, j: hop_event(blk, hop, j), hop=hop, j=j)))
    for j in range(PATH_PIECES):
        events.append((SEND_SLOT[j], functools.partial(lambda blk, j: own_send(blk, j), j=j)))
    events.append((LOAD_SLOT, load_event))

    def comm_slot(blk, tile):
        for residue in range(tiles):
            due = [(fn, (residue - offset) // tiles) for offset, fn in events if offset % tiles == residue]
            if not due:
                continue

            @pl.when(tile == residue)
            def _(due=due):
                for fn, ahead in due:
                    target = blk + ahead

                    @pl.when((target >= 0) & (target < n_blocks))
                    def _(fn=fn, target=target):
                        fn(target)

    def compute(blk, tile):
        par = lax.rem(blk, 2)
        u_par = lax.rem(tile, 2)
        rows = pl.ds(pl.multiple_of(tile * TILE, TILE), TILE)

        @pl.when(tile == 0)
        def _():
            for cp in weight_loads(blk, par, True):
                cp.wait()

        @pl.when((blk == 0) & (tile == 0))
        def _():
            x_copy().wait()
            for t in range(tiles):
                act_copy(0, t).start()

        @pl.when((blk > 0) | (tile > 1))
        def _():
            u_copy(blk, tile, u_par).wait()

        @pl.when(blk == n_blocks - 1)
        def _():
            t_copy(tile).start()

        act_copy(blk, tile).wait()
        x = act[rows, :]
        chunk = 256
        n_chunk = d_ff // chunk
        for f in range(n_chunk):
            cols = slice(f * chunk, (f + 1) * chunk)
            u = _dot(x, w1_buf[par, :, cols])
            u_buf[u_par, :, cols] = u
            inner = u * (GELU_A + GELU_B * (u * u))
            a = (u * (0.5 + 0.5 * jnp.tanh(inner))).astype(BF16)
            part = _dot(a, w2_buf[par, cols, :])
            if f == 0:
                acc[...] = part
            elif f < n_chunk - 1:
                acc[...] += part
            else:
                act[rows, :] = (x.astype(F32) + (acc[...] + part)).astype(BF16)
        u_copy(blk, tile, u_par).start()

        @pl.when(blk < n_blocks - 1)
        def _():
            act_copy(blk + 1, tile).start()

        @pl.when(blk == n_blocks - 1)
        def _():
            t_copy(tile).wait()

            @pl.when(tile > 0)
            def _():
                seed_copy(tile - 1).wait()
            residual = act[rows, :].astype(F32) - t_buf[...].astype(F32)
            s_buf[...] = (residual / n_tokens).astype(BF16)
            squares = jnp.sum((residual * residual).reshape(TILE // 8, 8, residual.shape[1]), axis=0)
            folded = squares[:, :128]
            for j in range(1, residual.shape[1] // 128):
                folded = folded + squares[:, j * 128:(j + 1) * 128]
            loss[...] += 0.5 * folded
            seed_copy(tile).start()

    lead = -(min(SEND_SLOT) // tiles)
    loss[...] = jnp.zeros_like(loss)

    @pl.loop(0, (n_blocks + lead) * tiles)
    def _(step):
        blk = step // tiles - lead
        tile = lax.rem(step, tiles)
        comm_slot(blk, tile)

        @pl.when(blk >= 0)
        def _():
            compute(blk, tile)

    for par in range(2):
        u_copy(0, 0, par).wait()
    seed_copy(0).wait()

    @pl.loop(0, n_blocks)
    def _(blk):
        rel = rel_of(blk)
        for path in range(2):
            last = (2, 1)[path]

            @pl.when(rel != last)
            def _(path=path):
                for j in range(PATH_PIECES):
                    for cp in ici_copies(blk, path, j, views(blk, piece(j, path, core)), 1):
                        cp.wait_send()

        @pl.when(rel != 0)
        def _():
            for path in range(2):
                for j in range(PATH_PIECES):
                    for cp in d2d_copies(blk, path, j, core):
                        cp.wait_send()


def run_forward(n_tokens, x_flat, t_flat, w1_loc, w2_loc, n_rows):
    n_half, d_model, d_ff = w1_loc.shape
    n_blocks = 4 * n_half
    tiles = n_rows // TILE
    slots = 2 * PATH_PIECES
    out_shape = [
        jax.ShapeDtypeStruct((n_blocks, d_model, d_ff), BF16),
        jax.ShapeDtypeStruct((n_blocks, d_ff, d_model), BF16),
        jax.ShapeDtypeStruct((n_blocks, n_rows, d_model), BF16),
        jax.ShapeDtypeStruct((n_blocks, n_rows, d_ff), F32),
        jax.ShapeDtypeStruct((n_rows, d_model), BF16),
        jax.ShapeDtypeStruct((8, 128), F32),
    ]
    return pl.pallas_call(
        functools.partial(forward_kernel, n_blocks, tiles, n_tokens),
        name="forward",
        out_shape=out_shape,
        in_specs=[ANY] * 4,
        out_specs=[ANY] * 5 + [pl.BlockSpec(memory_space=pltpu.VMEM)],
        scratch_shapes=[
            pltpu.VMEM((n_rows, d_model), BF16),
            pltpu.VMEM((2, d_model, d_ff), BF16),
            pltpu.VMEM((2, d_ff, d_model), BF16),
            pltpu.VMEM((2, TILE, d_ff), F32),
            pltpu.VMEM((TILE, d_model), F32),
            pltpu.VMEM((TILE, d_model), BF16),
            pltpu.VMEM((TILE, d_model), BF16),
            pltpu.SemaphoreType.DMA(()),
            pltpu.SemaphoreType.DMA((tiles,)),
            pltpu.SemaphoreType.DMA((2,)),
            pltpu.SemaphoreType.DMA((2, 2)),
            pltpu.SemaphoreType.DMA(()),
            pltpu.SemaphoreType.DMA(()),
            pltpu.SemaphoreType.DMA((n_blocks, slots, 2)),
            pltpu.SemaphoreType.DMA((n_blocks, slots, 2)),
            pltpu.SemaphoreType.DMA((n_blocks, slots, 2)),
            pltpu.SemaphoreType.DMA((n_blocks, slots, 2)),
        ],
        compiler_params=pltpu.CompilerParams(collective_id=0, has_side_effects=True, vmem_limit_bytes=60 * 2**20),
        cost_estimate=pl.CostEstimate(flops=4 * n_blocks * n_rows * d_model * d_ff, bytes_accessed=600 * 2**20, transcendentals=0),
    )(x_flat, t_flat, w1_loc, w2_loc)


RING = 5
CHUNK = 512
PIECE = 256


def _relation(me, blk):
    own = lax.rem(blk, 4)
    a0, a1, b0, b1 = lax.rem(me, 2), me // 2, lax.rem(own, 2), own // 2
    return (a0 + b0 - 2 * a0 * b0) + 2 * (a1 + b1 - 2 * a1 * b1)


def _tile_rows(tile):
    return pl.ds(pl.multiple_of(tile * TILE, TILE), TILE)


def _gelu_grad(u):
    cube = GELU_B * (u * u)
    th = jnp.tanh(u * (GELU_A + cube))
    cdf = 0.5 + 0.5 * th
    a = u * cdf
    return a, cdf + (a * (3.0 - 3.0 * th)) * (cube + GELU_A / 3.0)


STAGE_TILE = (0, 3, 5, 8)
SENDS = 3


def backward_kernel(n_blocks, tiles, g_hbm, saved, u_hbm, w1_loc, w2_loc, wg1, wg2, local, sib, inbox, own, squares,
                    act, w1_buf, w2_buf, dw, u_buf, x_buf, x_t, g_t, acc, q_buf, k_buf, s_buf, r_buf, o_buf,
                    g_sem, w_sem, u_sem, x_sem, keep_sem, d2d_send, d2d_recv, load_sem, own_sem, ici_send, ici_recv):
    me = lax.axis_index("stage")
    core = lax.axis_index("data")
    d_model, d_ff = act.shape[1], w1_buf.shape[1]
    n_chunk = d_ff // CHUNK
    n_pair = n_chunk // 2
    n_slot = d_ff // PIECE // 2
    steps = n_blocks * tiles
    total = steps * n_chunk
    top = n_blocks - 1

    def cols_of(f):
        return pl.ds(pl.multiple_of(f * CHUNK, CHUNK), CHUNK)

    def pair_of(p):
        return pl.ds(pl.multiple_of(p * 2 * CHUNK, 2 * CHUNK), 2 * CHUNK)

    def pieces_of(f):
        return pl.ds(f * (CHUNK // PIECE), CHUNK // PIECE)

    def weight_copies(blk, pair, is_own):
        half = blk // 4
        src1, src2 = (w1_loc.at[half], w2_loc.at[half]) if is_own else (wg1.at[blk], wg2.at[blk])
        cols = pair_of(pair)
        return [pltpu.make_async_copy(src1.at[:, cols], w1_buf.at[:, cols], w_sem.at[pair, 0]),
                pltpu.make_async_copy(src2.at[cols, :], w2_buf.at[cols, :], w_sem.at[pair, 1])]

    def start_weights(blk, pair):
        rel = _relation(me, blk)

        @pl.when(rel == 0)
        def _():
            for cp in weight_copies(blk, pair, True):
                cp.start()

        @pl.when(rel != 0)
        def _():
            for cp in weight_copies(blk, pair, False):
                cp.start()

    def u_copy(step):
        blk = top - step // (tiles * n_chunk)
        tile = lax.rem(step // n_chunk, tiles)
        f = lax.rem(step, n_chunk)
        slot = lax.rem(step, RING)
        return pltpu.make_async_copy(u_hbm.at[blk, _tile_rows(tile), cols_of(f)], u_buf.at[slot], u_sem.at[slot])

    def x_copy(bt):
        par = lax.rem(bt, 2)
        return pltpu.make_async_copy(saved.at[top - bt // tiles, _tile_rows(lax.rem(bt, tiles)), :], x_buf.at[par], x_sem.at[par])

    def g_in_copy():
        return pltpu.make_async_copy(g_hbm, act, g_sem)

    def keep_copy(j, f):
        return pltpu.make_async_copy(dw.at[core, pieces_of(f)], local.at[lax.rem(j, 3), pieces_of(f)], keep_sem.at[f])

    def give_copy(j, c):
        return pltpu.make_async_remote_copy(
            src_ref=dw.at[1 - core, c], dst_ref=sib.at[j, c], send_sem=d2d_send.at[c],
            recv_sem=d2d_recv.at[j, c], device_id=(me, 1 - core), device_id_type=MESH)

    def stages_of(j):
        rel = _relation(me, top - j)
        return [jnp.where(rel == 0, 3, jnp.where(rel == 3, 1, jnp.where(rel == last, 0, 2))) for last in (2, 1)]

    def next_chip(stage, path):
        first = 1 if path == 0 else 2
        flip = jnp.where(stage == 1, 3 - first, first)
        bit0, bit1 = lax.rem(me, 2), me // 2
        return jnp.where(flip == 1, 1 - bit0 + 2 * bit1, bit0 + 2 * (1 - bit1))

    def piece_loads(j, c, buf):
        return [pltpu.make_async_copy(local.at[lax.rem(j, 3), c], k_buf.at[buf], load_sem.at[buf, 0]),
                pltpu.make_async_copy(sib.at[j, c], s_buf.at[buf], load_sem.at[buf, 1])]

    def inbox_load(j, c, buf):
        return pltpu.make_async_copy(inbox.at[j, c], r_buf.at[buf], load_sem.at[buf, 2])

    def own_copy(j, c, buf):
        return pltpu.make_async_copy(k_buf.at[buf], own.at[(top - j) // 4, c], own_sem.at[buf])

    def pass_copy(j, m, buf, stage, path):
        slot = lax.rem(m, SENDS)
        c = 2 * m + path
        return pltpu.make_async_remote_copy(
            src_ref=o_buf.at[buf, slot], dst_ref=inbox.at[j, c], send_sem=ici_send.at[buf, slot],
            recv_sem=ici_recv.at[j, c], device_id=(next_chip(stage, path), core), device_id_type=MESH)

    def first_piece(stage):
        return jnp.where(stage == 0, STAGE_TILE[0], jnp.where(stage == 1, STAGE_TILE[1], jnp.where(stage == 2, STAGE_TILE[2], STAGE_TILE[3])))

    def load_pieces(j, tile):
        live = (j >= 0) & (j < n_blocks)
        for path, (stage, before) in enumerate(zip(stages_of(j), stages_of(j - 2))):
            m = tile - first_piece(stage)

            @pl.when(live & (m >= 0) & (m < n_slot))
            def _(path=path, stage=stage, before=before, m=m):
                buf = lax.rem(j, 2) * 2 + path
                c = 2 * m + path

                @pl.when(((m >= 1) & (stage == 3)) | ((m == 0) & (j >= 2) & (before == 3)))
                def _():
                    own_copy(j, c, buf).wait()
                give_copy(j, c).wait_recv()
                for cp in piece_loads(j, c, buf):
                    cp.start()

                @pl.when(stage > 0)
                def _():
                    pass_copy(j, m, buf, stage, path).wait_recv()
                    inbox_load(j, c, buf).start()

    def sum_pieces(j, tile):
        live = (j >= 0) & (j < n_blocks)
        for path, (stage, before) in enumerate(zip(stages_of(j), stages_of(j - 2))):
            m = tile - first_piece(stage)

            @pl.when(live & (m >= 0) & (m < n_slot))
            def _(path=path, stage=stage, before=before, m=m):
                buf = lax.rem(j, 2) * 2 + path
                slot = lax.rem(m, SENDS)
                c = 2 * m + path

                @pl.when(((m >= SENDS) & (stage < 3)) | ((m < SENDS) & (j >= 2) & (before < 3)))
                def _():
                    pass_copy(j, m, buf, stage, path).wait_send()
                for cp in piece_loads(j, c, buf):
                    cp.wait()

                @pl.when(stage == 0)
                def _():
                    o_buf[buf, slot] = (k_buf[buf] + s_buf[buf]).astype(BF16)

                @pl.when(stage > 0)
                def _():
                    inbox_load(j, c, buf).wait()

                @pl.when((stage == 1) | (stage == 2))
                def _():
                    o_buf[buf, slot] = ((k_buf[buf] + s_buf[buf]) + r_buf[buf].astype(F32)).astype(BF16)

                @pl.when(stage < 3)
                def _():
                    pass_copy(j, m, buf, stage, path).start()

                @pl.when(stage == 3)
                def _():
                    val = (k_buf[buf] + s_buf[buf]) + r_buf[buf].astype(F32)
                    k_buf[buf] = val
                    part = jnp.sum((val * val).reshape(d_model // 8, 8, PIECE), axis=0)
                    squares[...] += part[:, :128] + part[:, 128:]
                    own_copy(j, c, buf).start()

    barrier = pltpu.get_barrier_semaphore()
    bit0, bit1 = lax.rem(me, 2), me // 2
    near = ((1 - bit0 + 2 * bit1, core), (bit0 + 2 * (1 - bit1), core), (me, 1 - core))
    for target in near:
        pl.semaphore_signal(barrier, inc=1, device_id=target, device_id_type=MESH)
    g_in_copy().start()
    for pair in range(n_pair):
        start_weights(jnp.int32(top), jnp.int32(pair))
    x_copy(0).start()
    x_copy(1).start()
    for step in range(RING - 2):
        u_copy(step).start()
    squares[...] = jnp.zeros_like(squares)
    pl.semaphore_wait(barrier, 3)
    g_in_copy().wait()
    x_copy(0).wait()
    x_t[0] = x_buf[0].T
    g_t[0] = act[pl.ds(0, TILE), :].T
    weight_copies(0, 0, True)[1].wait()
    q_buf[0] = _dot_t(act[pl.ds(0, TILE), :], w2_buf[pl.ds(0, CHUNK), :])

    def compute(n):
        bt = n // n_pair
        pair = lax.rem(n, n_pair)
        i = bt // tiles
        tile = lax.rem(bt, tiles)
        blk = top - i
        t_par = lax.rem(bt, 2)
        rows = _tile_rows(tile)
        next_rows = _tile_rows(lax.rem(tile + 1, tiles))

        @pl.when((pair == 0) & (bt + 1 < steps))
        def _():
            x_copy(bt + 1).wait()

        @pl.when((pair == 0) & (bt + 2 < steps))
        def _():
            x_copy(bt + 2).start()

        @pl.when(pair == 0)
        def _():
            acc[...] = act[rows, :].astype(F32)

        def chunk_prep(f, step):
            @pl.when(step + RING - 2 < total)
            def _():
                u_copy(step + RING - 2).start()
            u_copy(step).wait()

            @pl.when((tile == 0) & (i > 0))
            def _():
                keep_copy(i - 1, f).wait()
                for c in (2 * f, 2 * f + 1):
                    give_copy(i - 1, c).wait_send()

        def add_to(m, f, val):
            for part in range(CHUNK // PIECE):
                c = f * (CHUNK // PIECE) + part
                dw[m, c] = jnp.where(tile == 0, 0.0, dw[m, c]) + val[:, part * PIECE:(part + 1) * PIECE]

        def chunk_main(f, step, q_par, next_g, next_w2, with_input_grad):
            cols = cols_of(f)
            q_buf[1 - q_par] = _dot_t(next_g, next_w2)
            a, slope = _gelu_grad(u_buf[lax.rem(step, RING)])
            r = (q_buf[q_par] * slope).astype(BF16)
            add_to(0, f, _dot(x_t[t_par], r))
            add_to(1, f, _dot(g_t[t_par], a.astype(BF16)))
            if with_input_grad:
                acc[...] += _dot_t(r, w1_buf[:, cols])

        def pair_step(with_input_grad):
            f0 = pair * 2
            step = bt * n_chunk + f0
            last = pair == n_pair - 1
            chunk_prep(f0, step)
            chunk_prep(f0 + 1, step + 1)

            @pl.when(tile == 0)
            def _():
                weight_copies(0, pair, True)[0].wait()

            @pl.when((tile == 0) & (pair < n_pair - 1))
            def _():
                weight_copies(0, pair + 1, True)[1].wait()

            @pl.when(last & (tile == tiles - 1) & (bt + 1 < steps))
            def _():
                weight_copies(0, jnp.int32(0), True)[1].wait()

            q_rows = _tile_rows(jnp.where(last, lax.rem(tile + 1, tiles), tile))
            next_f = jnp.where(last, 0, f0 + 2)
            third = pl.ds(pl.multiple_of(pair * 256, 256), 256)
            x_t[1 - t_par, third, :] = x_buf[1 - t_par, :, third].T
            g_t[1 - t_par, third, :] = act[next_rows, third].T
            chunk_main(f0, step, 0, act[rows, :], w2_buf[cols_of(f0 + 1), :], with_input_grad)
            chunk_main(f0 + 1, step + 1, 1, act[q_rows, :], w2_buf[cols_of(next_f), :], with_input_grad)

            @pl.when(tile == tiles - 1)
            def _():
                for f in (f0, f0 + 1):
                    keep_copy(i, f).start()
                    for c in (2 * f, 2 * f + 1):
                        give_copy(i, c).start()

            if with_input_grad:
                @pl.when(tile == tiles - 1)
                def _():
                    start_weights(blk - 1, pair)

        @pl.when(blk > 0)
        def _():
            pair_step(True)

            @pl.when(pair == n_pair - 1)
            def _():
                act[rows, :] = acc[...].astype(BF16)

        @pl.when(blk == 0)
        def _():
            pair_step(False)

    span = tiles * n_pair
    all_steps = n_blocks * span

    @pl.loop(0, all_steps + (STAGE_TILE[3] + n_slot) * n_pair)
    def _(n):
        i = n // span
        tile = lax.rem(n, span) // n_pair
        phase = lax.rem(n, n_pair)

        @pl.when(n < all_steps)
        def _():
            compute(n)

        @pl.when(n == all_steps)
        def _():
            for f in range(n_chunk):
                keep_copy(top, f).wait()
                for c in (2 * f, 2 * f + 1):
                    give_copy(top, c).wait_send()

        @pl.when((phase == 0) & (i > 0))
        def _():
            load_pieces(i - 2, tile + tiles)
            load_pieces(i - 1, tile)

        @pl.when((phase == 1) & (i > 0))
        def _():
            sum_pieces(i - 2, tile + tiles)
            sum_pieces(i - 1, tile)

    for j in (n_blocks - 2, n_blocks - 1):
        for path, stage in enumerate(stages_of(j)):
            buf = j % 2 * 2 + path

            @pl.when(stage == 3)
            def _(j=j, path=path, buf=buf):
                own_copy(j, path, buf).wait()

            @pl.when(stage < 3)
            def _(j=j, path=path, buf=buf, stage=stage):
                for m in range(SENDS):
                    pass_copy(j, m, buf, stage, path).wait_send()


def run_backward(grad, saved, u_all, weights):
    n_rows, d_model = grad.shape
    n_half, _, d_ff = weights[0].shape
    n_blocks = 4 * n_half
    tiles = n_rows // TILE
    n_chunk = d_ff // CHUNK
    n_piece = d_ff // PIECE
    pieces = (n_piece, d_model, PIECE)
    return pl.pallas_call(
        functools.partial(backward_kernel, n_blocks, tiles),
        name="backward",
        out_shape=[
            jax.ShapeDtypeStruct((3,) + pieces, F32),
            jax.ShapeDtypeStruct((n_blocks,) + pieces, F32),
            jax.ShapeDtypeStruct((n_blocks,) + pieces, BF16),
            jax.ShapeDtypeStruct((n_half,) + pieces, F32),
            jax.ShapeDtypeStruct((8, 128), F32),
        ],
        in_specs=[ANY] * 7,
        out_specs=[ANY] * 4 + [pl.BlockSpec(memory_space=pltpu.VMEM)],
        scratch_shapes=[
            pltpu.VMEM((n_rows, d_model), BF16),
            pltpu.VMEM((d_model, d_ff), BF16),
            pltpu.VMEM((d_ff, d_model), BF16),
            pltpu.VMEM((2,) + pieces, F32),
            pltpu.VMEM((RING, TILE, CHUNK), F32),
            pltpu.VMEM((2, TILE, d_model), BF16),
            pltpu.VMEM((2, d_model, TILE), BF16),
            pltpu.VMEM((2, d_model, TILE), BF16),
            pltpu.VMEM((TILE, d_model), F32),
            pltpu.VMEM((2, TILE, CHUNK), F32),
            pltpu.VMEM((4, d_model, PIECE), F32),
            pltpu.VMEM((4, d_model, PIECE), F32),
            pltpu.VMEM((4, d_model, PIECE), BF16),
            pltpu.VMEM((4, SENDS, d_model, PIECE), BF16),
            pltpu.SemaphoreType.DMA(()),
            pltpu.SemaphoreType.DMA((n_chunk // 2, 2)),
            pltpu.SemaphoreType.DMA((RING,)),
            pltpu.SemaphoreType.DMA((2,)),
            pltpu.SemaphoreType.DMA((n_chunk,)),
            pltpu.SemaphoreType.DMA((n_piece,)),
            pltpu.SemaphoreType.DMA((n_blocks, n_piece)),
            pltpu.SemaphoreType.DMA((4, 3)),
            pltpu.SemaphoreType.DMA((4,)),
            pltpu.SemaphoreType.DMA((4, SENDS)),
            pltpu.SemaphoreType.DMA((n_blocks, n_piece)),
        ],
        compiler_params=pltpu.CompilerParams(collective_id=1, has_side_effects=True, vmem_limit_bytes=67043328),
        cost_estimate=pl.CostEstimate(flops=8 * n_blocks * n_rows * d_model * d_ff, bytes_accessed=800 * 2**20, transcendentals=0),
    )(grad, saved, u_all, *weights)


def scalars_kernel(tau_clip, squares, loss, clip_out, loss_out, mine, gathered, send_sem, recv_sem):
    stage = lax.axis_index("stage")
    core = lax.axis_index("data")
    n_dev = gathered.shape[0]
    here = stage * 2 + core
    barrier = pltpu.get_barrier_semaphore()
    for k in range(1, n_dev):
        other = lax.rem(here + k, n_dev)
        pl.semaphore_signal(barrier, inc=1, device_id=(other // 2, lax.rem(other, 2)), device_id_type=MESH)
    mine[0] = squares[...]
    mine[1] = loss[...]
    gathered[here] = mine[...]
    pl.semaphore_wait(barrier, n_dev - 1)

    def copy(k, slot):
        other = lax.rem(here + k, n_dev)
        return pltpu.make_async_remote_copy(
            src_ref=mine, dst_ref=gathered.at[slot], send_sem=send_sem.at[k], recv_sem=recv_sem.at[k],
            device_id=(other // 2, lax.rem(other, 2)), device_id_type=MESH)

    for k in range(1, n_dev):
        copy(k, here).start()
    for k in range(1, n_dev):
        copy(k, lax.rem(here + n_dev - k, n_dev)).wait_recv()
    sums = jnp.sum(gathered[...], axis=0)
    squared = jnp.sum(jnp.sum(sums[0], axis=0, keepdims=True), axis=1, keepdims=True)
    lost = jnp.sum(jnp.sum(sums[1], axis=0, keepdims=True), axis=1, keepdims=True)
    norm = jnp.sqrt(jnp.broadcast_to(squared, (8, 128)))
    clip_out[...] = jnp.minimum(1.0, tau_clip / norm)
    loss_out[...] = jnp.broadcast_to(lost, (8, 128))
    for k in range(1, n_dev):
        copy(k, here).wait_send()


def run_scalars(tau_clip, squares, loss):
    vmem = pl.BlockSpec(memory_space=pltpu.VMEM)
    return pl.pallas_call(
        functools.partial(scalars_kernel, tau_clip),
        name="scalars",
        out_shape=[jax.ShapeDtypeStruct((8, 128), F32)] * 2,
        in_specs=[vmem] * 2,
        out_specs=[vmem] * 2,
        scratch_shapes=[
            pltpu.VMEM((2, 8, 128), F32),
            pltpu.VMEM((8, 2, 8, 128), F32),
            pltpu.SemaphoreType.DMA((8,)),
            pltpu.SemaphoreType.DMA((8,)),
        ],
        compiler_params=pltpu.CompilerParams(collective_id=2, has_side_effects=True),
    )(squares, loss)


FLAT_ROWS = 3072


def update_kernel(learn_rate, grad, clip, w_old, m_old, v_old, w_new, m_new, v_new, w1_half, w2_half,
                  g_one, g_two, flat, wide, n_one, n_two, g_sem, n_sem):
    step = pl.program_id(0)
    core = lax.axis_index("data")
    d_model, d_ff = grad.shape[2], grad.shape[1] * grad.shape[3]
    rows1, rows2 = FLAT_ROWS * 128 // d_ff, FLAT_ROWS * 128 // d_model
    chunks = d_model // rows1
    steps = 2 * chunks

    def g_copy(n, of_core):
        par = lax.rem(n, 2)
        half, chunk = n // chunks, lax.rem(n, chunks)
        if of_core == 0:
            return pltpu.make_async_copy(grad.at[half, :, pl.ds(pl.multiple_of(chunk * rows1, rows1), rows1), :], g_one.at[par], g_sem.at[par])
        per_step = rows2 // PIECE
        return pltpu.make_async_copy(grad.at[half, pl.ds(chunk * per_step, per_step)], g_two.at[par], g_sem.at[par])

    def n_copy(n, of_core):
        par = lax.rem(n, 2)
        half, chunk = n // chunks, lax.rem(n, chunks)
        if of_core == 0:
            return pltpu.make_async_copy(n_one.at[par], w1_half.at[half, pl.ds(pl.multiple_of(chunk * rows1, rows1), rows1), :], n_sem.at[par])
        return pltpu.make_async_copy(n_two.at[par], w2_half.at[half, pl.ds(pl.multiple_of(chunk * rows2, rows2), rows2), :], n_sem.at[par])

    par = lax.rem(step, 2)
    for of_core in range(2):
        @pl.when(core == of_core)
        def _(of_core=of_core):
            @pl.when(step == 0)
            def _():
                g_copy(step, of_core).start()

            @pl.when(step + 1 < steps)
            def _():
                g_copy(step + 1, of_core).start()
            g_copy(step, of_core).wait()
            if of_core == 0:
                per_row = d_ff // 128
                for j in range(per_row):
                    c, lane = divmod(j * 128, PIECE)
                    flat[pl.ds(j, rows1, per_row), :] = g_one[par, c, :, lane:lane + 128]
            else:
                per_row = d_model // 128
                for c in range(rows2 // PIECE):
                    val = g_two[par, c].T
                    for j in range(per_row):
                        flat[pl.ds(c * PIECE * per_row + j, PIECE, per_row), :] = val[:, j * 128:(j + 1) * 128]

    grad_clip = jnp.broadcast_to(clip[0:1, :], (FLAT_ROWS, 128)) * flat[...]
    m_val = BETA_ONE * m_old[...] + (1.0 - BETA_ONE) * grad_clip
    v_val = BETA_TWO * v_old[...] + (1.0 - BETA_TWO) * grad_clip * grad_clip
    m_hat = m_val * (1.0 / (1.0 - BETA_ONE ** ADAM_STEP))
    v_hat = v_val * (1.0 / (1.0 - BETA_TWO ** ADAM_STEP))
    w_val = w_old[...]
    w_val = w_val - learn_rate * (m_hat / (jnp.sqrt(v_hat) + ADAM_EPS) + WEIGHT_DECAY * w_val)
    m_new[...] = m_val
    v_new[...] = v_val
    w_new[...] = w_val
    wide[...] = w_val

    for of_core in range(2):
        @pl.when(core == of_core)
        def _(of_core=of_core):
            @pl.when(step >= 2)
            def _():
                n_copy(step - 2, of_core).wait()
            buf, per_row = (n_one, d_ff // 128) if of_core == 0 else (n_two, d_model // 128)
            for j in range(per_row):
                buf[par, :, j * 128:(j + 1) * 128] = wide[pl.ds(j, buf.shape[1], per_row), :].astype(BF16)
            n_copy(step, of_core).start()

            @pl.when(step == steps - 1)
            def _():
                n_copy(step - 1, of_core).wait()
                n_copy(step, of_core).wait()


def run_update(learn_rate, grad, clip, w_old, m_old, v_old):
    d_model, d_ff = grad.shape[2], grad.shape[1] * grad.shape[3]
    rows1, rows2 = FLAT_ROWS * 128 // d_ff, FLAT_ROWS * 128 // d_model
    steps = w_old.shape[0] // FLAT_ROWS
    flat_spec = pl.BlockSpec((FLAT_ROWS, 128), lambda i: (i, 0))
    flat_shape = jax.ShapeDtypeStruct(w_old.shape, F32)
    return pl.pallas_call(
        functools.partial(update_kernel, learn_rate),
        name="update",
        grid=(steps,),
        out_shape=[flat_shape] * 3 + [jax.ShapeDtypeStruct((2, d_model, d_ff), BF16), jax.ShapeDtypeStruct((2, d_ff, d_model), BF16)],
        in_specs=[ANY, pl.BlockSpec((8, 128), lambda i: (0, 0))] + [flat_spec] * 3,
        out_specs=[flat_spec] * 3 + [ANY, ANY],
        scratch_shapes=[
            pltpu.VMEM((2, d_ff // PIECE, rows1, PIECE), F32),
            pltpu.VMEM((2, rows2 // PIECE, d_model, PIECE), F32),
            pltpu.VMEM((FLAT_ROWS, 128), F32),
            pltpu.VMEM((FLAT_ROWS, 128), F32),
            pltpu.VMEM((2, rows1, d_ff), BF16),
            pltpu.VMEM((2, rows2, d_model), BF16),
            pltpu.SemaphoreType.DMA((2,)),
            pltpu.SemaphoreType.DMA((2,)),
        ],
        compiler_params=pltpu.CompilerParams(dimension_semantics=("arbitrary",), vmem_limit_bytes=60 * 2**20),
        cost_estimate=pl.CostEstimate(flops=10**9, bytes_accessed=150 * 2**20, transcendentals=0),
    )(grad, clip, w_old, m_old, v_old)


MERGE_PARTS = 4


def merge_kernel(w1_half, w2_half, w1_got, w2_got, w1_new, w2_new, sem):
    del w1_half, w2_half
    core = lax.axis_index("data")
    for of_core, got, new in ((1, w1_got, w1_new), (0, w2_got, w2_new)):
        rows = got.shape[1] // MERGE_PARTS
        spots = [(half, pl.ds(part * rows, rows)) for half in range(2) for part in range(MERGE_PARTS)]

        @pl.when(core == of_core)
        def _(spots=spots, got=got, new=new):
            copies = [pltpu.make_async_copy(got.at[half, where, :], new.at[half, where, :], sem.at[n]) for n, (half, where) in enumerate(spots)]
            for cp in copies:
                cp.start()
            for cp in copies:
                cp.wait()


def run_merge(w1_half, w2_half, w1_got, w2_got):
    return pl.pallas_call(
        merge_kernel,
        name="merge",
        out_shape=[jax.ShapeDtypeStruct(w1_half.shape, BF16), jax.ShapeDtypeStruct(w2_half.shape, BF16)],
        in_specs=[ANY] * 4,
        out_specs=[ANY] * 2,
        input_output_aliases={0: 0, 1: 1},
        scratch_shapes=[pltpu.SemaphoreType.DMA((2 * MERGE_PARTS,))],
        compiler_params=pltpu.CompilerParams(vmem_limit_bytes=8 * 2**20),
    )(w1_half, w2_half, w1_got, w2_got)


def solution(mesh):
    n_stage = mesh.shape["stage"]
    n_data = mesh.shape["data"]
    axes = ("stage", "data")

    def device(stage, core):
        return stage * n_data + core

    def from_core(core):
        return [(device(s, core), device(s, 1 - core)) for s in range(n_stage)]

    def device_step(x_loc, t_loc, w1_loc, w2_loc, wm_loc, m_loc, v_loc):
        n_micro, n_tok, d_model = x_loc.shape
        d_ff = w1_loc.shape[4]
        n_tokens = n_micro * n_tok * n_data
        n_blocks = 2 * n_stage
        n_rows = n_micro * n_tok // n_stage
        tau_clip = 0.3 * d_model * math.sqrt(n_blocks * (3.0 / n_tokens + 0.008))
        learn_rate = 0.1 / math.sqrt(4.0 * d_model * n_blocks)
        w1 = w1_loc.reshape(2, d_model, d_ff)
        w2 = w2_loc.reshape(2, d_ff, d_model)
        flat_rows = (n_micro * n_tok, d_model)
        wg1, wg2, saved, u_all, seed, loss_acc = run_forward(n_tokens, x_loc.reshape(flat_rows), t_loc.reshape(flat_rows), w1, w2, n_rows)
        weights = (w1, w2, wg1, wg2)
        _, _, _, total, squares = run_backward(seed, saved, u_all, weights)
        clip, loss_all = run_scalars(tau_clip, squares, loss_acc)
        flat = [val.reshape(-1, 128) for val in (wm_loc, m_loc, v_loc)]
        w_new, m_new, v_new, w1_half, w2_half = run_update(learn_rate, total, clip, *flat)
        w1_got = lax.ppermute(w1_half, axes, from_core(0))
        w2_got = lax.ppermute(w2_half, axes, from_core(1))
        w1_new, w2_new = run_merge(w1_half, w2_half, w1_got, w2_got)
        mean_loss = loss_all[0, 0] / n_tokens
        return w1_new.reshape(w1_loc.shape), w2_new.reshape(w2_loc.shape), w_new.reshape(wm_loc.shape), m_new.reshape(wm_loc.shape), v_new.reshape(wm_loc.shape), mean_loss

    act_spec = P(None, "data", None)
    flat_spec = P("stage", None, None, "data")
    return jax.shard_map(device_step, mesh=mesh, in_specs=(act_spec, act_spec, P("stage"), P("stage"), flat_spec, flat_spec, flat_spec), out_specs=(P("stage"), P("stage"), flat_spec, flat_spec, flat_spec, P()), check_vma=False)
```
